8 devices in a mesh: dp: 2 (over y, z), tp: 4 (over x, core).
Axes of the slice: x: 2, y: 2, z: 1, core: 2. Of those that a mesh axis runs over, the one named last changes fastest.
Arguments:
- x: bfloat16 [8, 512, 8192], P('dp'), parts along dimension 0
- gain_a: bfloat16 [8192], replicated
- wq: bfloat16 [8192, 8192], P(None, 'tp')
- wk: bfloat16 [8192, 1024], P(None, 'tp')
- wv: bfloat16 [8192, 1024], P(None, 'tp')
- wo: bfloat16 [8192, 8192], P('tp')
- gain_m: bfloat16 [8192], replicated
- w_gate: bfloat16 [8192, 22016], P(None, 'tp')
- w_up: bfloat16 [8192, 22016], P(None, 'tp')
- w_down: bfloat16 [22016, 8192], P('tp')
Outputs:
- output: bfloat16 [8, 512, 8192], P('dp'), parts along dimension 0
There are 2 independent parts. The reference program is written for one: setup_inputs(seed, part) draws one part's arguments, and reference() takes and returns one part's arrays. A program takes and returns all parts, laid end to end along the dimension named above; an argument that names none is the same for every part.
All inputs are finite; a program needn't handle non-finite values.
Results may differ from the reference program's by a relative error of at most 0.017.
Values are sent between devices in bfloat16 or wider.
A program may use at most 2 GiB of HBM per device.

```python
import jax
import jax.numpy as jnp
from jax import lax

SEQUENCES = 4
TOKENS = 512
D = 8192
HEADS = 64
KV_HEADS = 8
HEAD = 128
FF = 22016
THETA = 10000


def setup_inputs(seed: int = 0, part: int = 0) -> dict:
    kx, ka, km, kq, kk, kv, ko, kg, ku, kd = jax.random.split(jax.random.key(seed), 10)

    def weights(key, rows, columns):
        return jax.random.normal(key, (rows, columns), jnp.float32) * rows**-0.5

    drawn = {
        "x": jax.random.normal(jax.random.fold_in(kx, part), (SEQUENCES, TOKENS, D), jnp.float32),
        "gain_a": 1 + 0.1 * jax.random.normal(ka, (D,), jnp.float32),
        "wq": 2 * weights(kq, D, HEADS * HEAD),
        "wk": 2 * weights(kk, D, KV_HEADS * HEAD),
        "wv": 4 * weights(kv, D, KV_HEADS * HEAD),
        "wo": weights(ko, HEADS * HEAD, D),
        "gain_m": 1 + 0.1 * jax.random.normal(km, (D,), jnp.float32),
        "w_gate": weights(kg, D, FF),
        "w_up": weights(ku, D, FF),
        "w_down": 3 * weights(kd, FF, D),
    }
    return {k: v.astype(jnp.bfloat16) for k, v in drawn.items()}


def normed(x, gain):
    wide = x.astype(jnp.float32)
    scale = lax.rsqrt(jnp.mean(wide * wide, -1, keepdims=True) + 1e-6)
    return (wide * scale * gain.astype(jnp.float32)).astype(jnp.bfloat16)


def turned(t, place, theta):
    half = t.shape[-1] // 2
    angle = place.astype(jnp.float32)[:, None] * theta ** (-jnp.arange(half, dtype=jnp.float32) / half)
    cos, sin = jnp.cos(angle)[:, None], jnp.sin(angle)[:, None]
    a, b = t[..., :half].astype(jnp.float32), t[..., half:].astype(jnp.float32)
    return jnp.concatenate([a * cos - b * sin, b * cos + a * sin], -1).astype(jnp.bfloat16)


def matmul(a, w):
    return jnp.dot(a, w, preferred_element_type=jnp.float32).astype(jnp.bfloat16)


def einsum(form, a, b):
    return jnp.einsum(form, a.astype(jnp.float32), b.astype(jnp.float32))


def attention(q, k, v):
    scores = einsum("tgsd,ugd->gstu", q, k) * q.shape[-1] ** -0.5
    token = jnp.arange(q.shape[0])
    scores = jnp.where(token[:, None] >= token, scores, -jnp.inf)
    weights = jax.nn.softmax(scores, -1).astype(jnp.bfloat16)
    return einsum("gstu,ugd->tgsd", weights, v).astype(jnp.bfloat16)


def one(x, gain_a, wq, wk, wv, wo, gain_m, w_gate, w_up, w_down):
    rows = x.shape[0]
    a, place = normed(x, gain_a), jnp.arange(rows)
    k = turned(matmul(a, wk).reshape(rows, -1, HEAD), place, THETA)
    q = turned(matmul(a, wq).reshape(rows, -1, HEAD), place, THETA).reshape(rows, k.shape[1], -1, HEAD)
    v = matmul(a, wv).reshape(rows, -1, HEAD)
    seen = attention(q, k, v).reshape(rows, -1)
    h = (x.astype(jnp.float32) + jnp.dot(seen, wo, preferred_element_type=jnp.float32)).astype(jnp.bfloat16)
    b = normed(h, gain_m)
    gate = jnp.dot(b, w_gate, preferred_element_type=jnp.float32)
    up = jnp.dot(b, w_up, preferred_element_type=jnp.float32)
    hidden = (jax.nn.silu(gate) * up).astype(jnp.bfloat16)
    return (h.astype(jnp.float32) + jnp.dot(hidden, w_down, preferred_element_type=jnp.float32)).astype(jnp.bfloat16)


def reference(x, gain_a, wq, wk, wv, wo, gain_m, w_gate, w_up, w_down):
    return lax.map(lambda sequence: one(sequence, gain_a, wq, wk, wv, wo, gain_m, w_gate, w_up, w_down), x)
```

```python
import functools

import jax
import jax.numpy as jnp
from jax import lax
from jax.experimental import pallas as pl
from jax.experimental.pallas import tpu as pltpu
from jax.sharding import PartitionSpec as P

HEAD = 128
THETA = 10000
LOG2E = 1.4426950408889634
HIDDEN = -2e30
MESH = pl.DeviceIdType.MESH
NB = 512
FB = 256
RING = 3
PIECE = 32
F32, BF16 = jnp.float32, jnp.bfloat16


def _dot(a, b, ca=1, cb=0):
    return lax.dot_general(a, b, (((ca,), (cb,)), ((), ())), preferred_element_type=F32)


def layer_kernel(
    x, wq, wk, wv, wo, wg, wu, wd, gain_a, gain_m, cos, sin,
    y, h_all, q_all, r_all,
    lhs, slots, qs, kvs, vts, hid, own, snd, rcv, stg, xin, qin, rin, hst, yin, yout,
    wsem, rs_send, rs_recv, st_sem, xs_sem, xr_sem, l_send, l_recv, l_free, in_sem, h_sem, yin_sem, yl_sem, ys_sem, yr_sem,
    *, seqs,
):
    tokens, depth = lhs.shape
    half = tokens // 2
    qcols, kcols, ff = wq.shape[1], wk.shape[1], wd.shape[0]
    nj = depth // NB
    nq = qcols // NB
    per = depth // qcols
    nwo = nj // per
    na = nq + 1 + nwo
    ngu = ff // FB
    tail = ff - ngu * FB
    nm = ngu + (1 if tail else 0) + nj
    first_d = nm - nj
    all_a = seqs * na
    total = all_a + seqs * nm
    heads = qcols // HEAD
    group = heads // (kcols // HEAD)

    me = lax.axis_index("tp")
    core, chip = lax.rem(me, 2), lax.div(me, 2)
    partner = {"tp": chip * 2 + (1 - core)}
    across = {"tp": (1 - chip) * 2 + core}

    barrier = pltpu.get_barrier_semaphore()
    for peer in (partner, across):
        pl.semaphore_signal(barrier, inc=1, device_id=peer, device_id_type=MESH)
    pl.semaphore_wait(barrier, 2)

    def start(g):
        slot = lax.rem(g, RING)
        sem = wsem.at[slot]
        in_a = g < all_a
        a, m = lax.rem(g, na), lax.rem(g - all_a + total, nm)
        m = lax.rem(g + (nm - all_a % nm), nm)

        @pl.when(in_a & (a < nq))
        def _():
            pltpu.make_async_copy(wq.at[:, pl.ds(pl.multiple_of(a * NB, NB), NB)], slots.at[slot], sem).start()

        @pl.when(in_a & (a == nq))
        def _():
            pltpu.make_async_copy(wk, slots.at[slot, :, pl.ds(0, kcols)], sem).start()
            pltpu.make_async_copy(wv, slots.at[slot, :, pl.ds(kcols, kcols)], sem).start()

        @pl.when(in_a & (a > nq))
        def _():
            for k in range(per):
                at = pl.multiple_of(((a - nq - 1) * per + k) * NB, NB)
                pltpu.make_async_copy(wo.at[:, pl.ds(at, NB)], slots.at[slot, pl.ds(k * qcols, qcols), :], sem).start()

        in_m = jnp.logical_not(in_a) & (g < total)

        @pl.when(in_m & (m < ngu))
        def _():
            at = pl.multiple_of(m * FB, FB)
            pltpu.make_async_copy(wg.at[:, pl.ds(at, FB)], slots.at[slot, :, pl.ds(0, FB)], sem).start()
            pltpu.make_async_copy(wu.at[:, pl.ds(at, FB)], slots.at[slot, :, pl.ds(FB, FB)], sem).start()

        if tail:

            @pl.when(in_m & (m == ngu))
            def _():
                pltpu.make_async_copy(wg.at[:, pl.ds(ngu * FB, tail)], slots.at[slot, :, pl.ds(0, tail)], sem).start()
                pltpu.make_async_copy(wu.at[:, pl.ds(ngu * FB, tail)], slots.at[slot, :, pl.ds(tail, tail)], sem).start()

        @pl.when(in_m & (m >= first_d))
        def _():
            at = pl.multiple_of((m - first_d) * NB, NB)
            pltpu.make_async_copy(wd.at[:, pl.ds(at, NB)], slots.at[slot, pl.ds(0, ff), :], sem).start()

    def ready(g, rows=None, cols=NB):
        slot = lax.rem(g, RING)
        rows = depth if rows is None else rows
        where = slots.at[slot, pl.ds(0, rows), pl.ds(0, cols)]
        pltpu.make_async_copy(where, where, wsem.at[slot]).wait()
        start(g + RING - 1)
        return slot

    def crossed(ar, j):
        return pltpu.make_async_remote_copy(q_all.at[ar, j], r_all.at[ar, j], xs_sem.at[ar], xr_sem.at[ar, j],
                                            device_id=across, device_id_type=MESH)

    def kept(ar, j):
        at = lax.rem(j, 2)
        return pltpu.make_async_copy(stg.at[at], q_all.at[ar, j], st_sem.at[at])

    def shared(j):
        at = lax.rem(j, 4)
        return pltpu.make_async_remote_copy(snd.at[at], rcv.at[at], rs_send.at[at], rs_recv.at[at],
                                            device_id=partner, device_id_type=MESH)

    def finish(ar, j):
        @pl.when(j >= 1)
        def _():
            kept(ar, j - 1).wait()
            crossed(ar, j - 1).start()

        shared(j).wait_recv()
        stg[lax.rem(j, 2)] = (own[lax.rem(j, 3)] + rcv[lax.rem(j, 4)].astype(F32)).astype(BF16)
        kept(ar, j).start()

    def block(ar, j, term):
        @pl.when(j >= 4)
        def _():
            shared(j - 4).wait_send()

        snd[lax.rem(j, 4)] = term[:half].astype(BF16)
        own[lax.rem(j, 3)] = term[half:]

        @pl.when(j >= 2)
        def _():
            finish(ar, j - 2)

        shared(j).start()

    def drain(ar):
        for j in (nj - 2, nj - 1):
            finish(ar, jnp.int32(j))
        for j in range(nj - 4, nj):
            shared(jnp.int32(j)).wait_send()
        kept(ar, jnp.int32(nj - 1)).wait()
        crossed(ar, jnp.int32(nj - 1)).start()

    def operand(c, gain, second):
        row0 = c * tokens + core * half

        def loads(p):
            at = lax.rem(p, 2)
            here = pl.ds(pl.multiple_of(p * PIECE, PIECE), PIECE)
            got = [pltpu.make_async_copy(x.at[pl.ds(pl.multiple_of(row0 + p * PIECE, PIECE), PIECE), :], xin.at[at], in_sem.at[at, 0])]
            if second:
                got.append(pltpu.make_async_copy(q_all.at[c, :, here, :], qin.at[at], in_sem.at[at, 1]))
                got.append(pltpu.make_async_copy(r_all.at[c, :, here, :], rin.at[at], in_sem.at[at, 2]))
            return got

        def put(p):
            at = lax.rem(p, 2)
            return pltpu.make_async_copy(hst.at[at], h_all.at[c, :, pl.ds(pl.multiple_of(p * PIECE, PIECE), PIECE), :], h_sem.at[at])

        def give(p):
            return pltpu.make_async_remote_copy(
                lhs.at[pl.ds(pl.multiple_of(half + p * PIECE, PIECE), PIECE), :], lhs.at[pl.ds(pl.multiple_of(p * PIECE, PIECE), PIECE), :],
                l_send, l_recv, device_id=partner, device_id_type=MESH)

        if second:

            def arrived(j, _):
                crossed(c, j).wait_recv()
                return 0

            lax.fori_loop(0, nj, arrived, 0)
        n = half // PIECE
        for copy in loads(jnp.int32(0)):
            copy.start()

        @pl.when(jnp.bool_(second) | (c > 0))
        def _():
            pl.semaphore_wait(l_free, 1)

        def piece(p, _):
            at = lax.rem(p, 2)

            @pl.when(p + 1 < n)
            def _():
                for copy in loads(p + 1):
                    copy.start()

            for copy in loads(p):
                copy.wait()
            if second:

                @pl.when(p >= 2)
                def _():
                    put(p - 2).wait()

            squares = jnp.zeros((PIECE, NB), F32)
            for j in range(nj):
                cols = slice(j * NB, (j + 1) * NB)
                v = xin[at, :, cols].astype(F32)
                if second:
                    v = (v + (qin[at, j].astype(F32) + rin[at, j].astype(F32))).astype(BF16)
                    hst[at, j] = v
                    v = v.astype(F32)
                squares += v * v
            scale = lax.rsqrt(jnp.sum(squares, axis=1, keepdims=True) * (1 / depth) + 1e-6)
            rows = pl.ds(pl.multiple_of(half + p * PIECE, PIECE), PIECE)
            for j in range(nj):
                cols = slice(j * NB, (j + 1) * NB)
                v = (hst[at, j] if second else xin[at, :, cols]).astype(F32)
                lhs[rows, cols] = (v * scale * gain[:, cols]).astype(BF16)
            if second:
                put(p).start()

            @pl.when(p >= 1)
            def _():
                give(p - 1).start()

            return 0

        lax.fori_loop(0, n, piece, 0)
        give(jnp.int32(n - 1)).start()
        if second:
            for p in (n - 2, n - 1):
                put(jnp.int32(p)).wait()
            pltpu.make_async_copy(q_all.at[c], q_all.at[c], xs_sem.at[c]).wait()
        pltpu.make_async_remote_copy(lhs.at[pl.ds(half, half), :], lhs.at[pl.ds(0, half), :], l_send, l_recv,
                                     device_id=partner, device_id_type=MESH).wait()

    def free():
        pl.semaphore_signal(l_free, inc=1, device_id=partner, device_id_type=MESH)

    early = pl.multiple_of((1 - core) * half, half)
    late = pl.multiple_of(core * half, half)

    def turned(t):
        t = t.astype(BF16).astype(F32)
        return (t * cos[...] + pltpu.roll(t, HEAD // 2, 1) * sin[...]).astype(BF16)

    def attention():
        e = HEAD**-0.5 * LOG2E
        for n in range(kcols // HEAD):
            cols = slice(kcols + n * HEAD, kcols + (n + 1) * HEAD)
            vts[n, :HEAD, :half] = kvs[pl.ds(early, half), cols].T
            vts[n, :HEAD, half:] = kvs[pl.ds(late, half), cols].T
            vts[n, HEAD:, :] = jnp.ones((vts.shape[1] - HEAD, tokens), BF16)
        seen = lax.broadcasted_iota(jnp.int32, (half, half), 0) <= lax.broadcasted_iota(jnp.int32, (half, half), 1)

        def out(o):
            return (o[:HEAD] * (1 / o[HEAD : HEAD + 1])).T.astype(BF16)

        def head(h):
            n = lax.div(h, group)
            kc = pl.ds(pl.multiple_of(n * HEAD, HEAD), HEAD)
            qc = pl.ds(pl.multiple_of(h * HEAD, HEAD), HEAD)
            k0, k1 = kvs[pl.ds(early, half), kc], kvs[pl.ds(late, half), kc]
            q0, q1 = qs[pl.ds(early, half), qc], qs[pl.ds(late, half), qc]
            s00 = jnp.where(seen, _dot(k0, q0, 1, 1), HIDDEN)
            s01 = _dot(k0, q1, 1, 1)
            s11 = jnp.where(seen, _dot(k1, q1, 1, 1), HIDDEN)
            top0 = s00.max(axis=0, keepdims=True)
            top1 = jnp.maximum(s01.max(axis=0, keepdims=True), s11.max(axis=0, keepdims=True))
            p00 = jnp.exp2((s00 - top0) * e).astype(BF16)
            p01 = jnp.exp2((s01 - top1) * e).astype(BF16)
            p11 = jnp.exp2((s11 - top1) * e).astype(BF16)
            v0, v1 = vts[n, :, :half], vts[n, :, half:]
            qs[pl.ds(early, half), qc] = out(_dot(v0, p00))
            qs[pl.ds(late, half), qc] = out(_dot(v0, p01) + _dot(v1, p11))

        def pair(i, _):
            for k in range(2):
                head(i * 2 + k)
            return 0

        lax.fori_loop(0, heads // 2, pair, 0)

    def first(c, _):
        operand(c, gain_a, False)
        g0 = c * na

        def queries(s, _):
            slot = ready(g0 + s)
            t = _dot(lhs[...], slots[slot])
            for n in range(NB // HEAD):
                qs[:, pl.ds(pl.multiple_of(s * NB + n * HEAD, HEAD), HEAD)] = turned(t[:, n * HEAD : (n + 1) * HEAD])
            return 0

        lax.fori_loop(0, nq, queries, 0)
        slot = ready(g0 + nq)
        t = _dot(lhs[...], slots[slot, :, : 2 * kcols])
        for n in range(kcols // HEAD):
            cols = slice(n * HEAD, (n + 1) * HEAD)
            kvs[:, cols] = turned(t[:, cols])
        kvs[:, kcols:] = t[:, kcols:].astype(BF16)
        free()
        attention()

        def project(j, _):
            k = lax.rem(j, per)
            g = g0 + nq + 1 + lax.div(j, per)

            @pl.when(k == 0)
            def _():
                ready(g)

            w = slots[lax.rem(g, RING), pl.ds(pl.multiple_of(k * qcols, qcols), qcols), :]
            block(c, j, _dot(qs[...], w))
            return 0

        lax.fori_loop(0, nj, project, 0)
        drain(c)
        return 0

    def gated(gate, up):
        return (gate * jax.nn.sigmoid(gate) * up).astype(BF16)

    def second(c, _):
        @pl.when(c >= 2)
        def _():
            result(c - 2)

        operand(c, gain_m, True)
        g0 = all_a + c * nm

        def gates(s, _):
            slot = ready(g0 + s)
            t = _dot(lhs[...], slots[slot])
            hid[:, pl.ds(pl.multiple_of(s * FB, FB), FB)] = gated(t[:, :FB], t[:, FB:])
            return 0

        lax.fori_loop(0, ngu, gates, 0)
        if tail:
            slot = ready(g0 + ngu, None, 2 * tail)
            t = _dot(lhs[...], slots[slot, :, : 2 * tail])
            hid[:, ngu * FB :] = gated(t[:, :tail], t[:, tail:])

        @pl.when(c + 1 < seqs)
        def _():
            free()

        def down(j, _):
            slot = ready(g0 + first_d + j, ff)
            block(seqs + c, j, _dot(hid[...], slots[slot, :ff, :]))
            return 0

        lax.fori_loop(0, nj, down, 0)
        drain(seqs + c)
        return 0

    def result(c):
        ar = seqs + c
        row0 = pl.multiple_of(c * tokens + core * half, half)

        def loads(j):
            at = lax.rem(j, 2)
            return [pltpu.make_async_copy(src, yin.at[at, i], yin_sem.at[at, i])
                    for i, src in enumerate((h_all.at[c, j], q_all.at[ar, j], r_all.at[ar, j]))]

        def puts(j):
            at = lax.rem(j, 2)
            where = y.at[pl.ds(row0, half), pl.ds(pl.multiple_of(j * NB, NB), NB)]
            return (pltpu.make_async_copy(yout.at[at], where, yl_sem.at[at]),
                    pltpu.make_async_remote_copy(yout.at[at], where, ys_sem.at[at], yr_sem.at[c], device_id=partner, device_id_type=MESH))

        def begin(j):
            crossed(ar, j).wait_recv()
            for copy in loads(j):
                copy.start()

        def left(j):
            near, far = puts(j)
            near.wait()
            far.wait_send()

        begin(jnp.int32(0))

        def piece(j, _):
            at = lax.rem(j, 2)

            @pl.when(j + 1 < nj)
            def _():
                begin(j + 1)

            for copy in loads(j):
                copy.wait()

            @pl.when(j >= 2)
            def _():
                left(j - 2)

            yout[at] = (yin[at, 0].astype(F32) + (yin[at, 1].astype(F32) + yin[at, 2].astype(F32))).astype(BF16)
            near, far = puts(j)
            near.start()
            far.start()
            return 0

        lax.fori_loop(0, nj, piece, 0)
        for j in (nj - 2, nj - 1):
            left(jnp.int32(j))
        pltpu.make_async_copy(q_all.at[ar], q_all.at[ar], xs_sem.at[ar]).wait()

    for g in range(RING - 1):
        start(jnp.int32(g))
    lax.fori_loop(0, seqs, first, 0)
    lax.fori_loop(0, seqs, second, 0)

    def end(c, _):
        result(c)
        return 0

    lax.fori_loop(max(seqs - 2, 0), seqs, end, 0)

    def arrived(c, _):
        where = y.at[pl.ds(pl.multiple_of(c * tokens + (1 - core) * half, half), half), :]
        pltpu.make_async_copy(where, where, yr_sem.at[c]).wait()
        return 0

    lax.fori_loop(0, seqs, arrived, 0)


def layer(x, gain_a, wq, wk, wv, wo, gain_m, w_gate, w_up, w_down, core):
    seqs, tokens, depth = x.shape
    half, nj = tokens // 2, depth // NB
    place = lax.rem(jnp.arange(tokens) + half * (1 - core), tokens)
    i = jnp.arange(HEAD // 2, dtype=F32)
    angle = place.astype(F32)[:, None] * THETA ** (-i / (HEAD // 2))
    cos, sin = jnp.cos(angle), jnp.sin(angle)
    cos, sin = jnp.concatenate([cos, cos], 1), jnp.concatenate([-sin, sin], 1)
    hbm, vmem = pl.BlockSpec(memory_space=pl.ANY), pl.BlockSpec(memory_space=pltpu.VMEM)
    dma = pltpu.SemaphoreType.DMA
    out = [
        jax.ShapeDtypeStruct((seqs * tokens, depth), BF16),
        jax.ShapeDtypeStruct((seqs, nj, half, NB), BF16),
        jax.ShapeDtypeStruct((2 * seqs, nj, half, NB), BF16),
        jax.ShapeDtypeStruct((2 * seqs, nj, half, NB), BF16),
    ]
    kv = wk.shape[1]
    scratch = [
        pltpu.VMEM((tokens, depth), BF16),
        pltpu.VMEM((RING, depth, NB), BF16),
        pltpu.VMEM((tokens, wq.shape[1]), BF16),
        pltpu.VMEM((tokens, 2 * kv), BF16),
        pltpu.VMEM((kv // HEAD, HEAD + 16, tokens), BF16),
        pltpu.VMEM((tokens, w_down.shape[0]), BF16),
        pltpu.VMEM((3, half, NB), F32),
        pltpu.VMEM((4, half, NB), BF16),
        pltpu.VMEM((4, half, NB), BF16),
        pltpu.VMEM((2, half, NB), BF16),
        pltpu.VMEM((2, PIECE, depth), BF16),
        pltpu.VMEM((2, nj, PIECE, NB), BF16),
        pltpu.VMEM((2, nj, PIECE, NB), BF16),
        pltpu.VMEM((2, nj, PIECE, NB), BF16),
        pltpu.VMEM((2, 3, half, NB), BF16),
        pltpu.VMEM((2, half, NB), BF16),
        dma((RING,)), dma((4,)), dma((4,)), dma((2,)), dma((2 * seqs,)), dma((2 * seqs, nj)),
        dma, dma, pltpu.SemaphoreType.REGULAR,
        dma((2, 3)), dma((2,)), dma((2, 3)), dma((2,)), dma((2,)), dma((seqs,)),
    ]
    y, *_ = pl.pallas_call(
        functools.partial(layer_kernel, seqs=seqs),
        out_shape=out,
        in_specs=[hbm] * 8 + [vmem] * 4,
        out_specs=[hbm] * 4,
        scratch_shapes=scratch,
        compiler_params=pltpu.CompilerParams(collective_id=0, has_side_effects=True, vmem_limit_bytes=67043328),
        name="layer",
    )(x.reshape(seqs * tokens, depth), wq, wk, wv, wo, w_gate, w_up, w_down,
      gain_a.astype(F32)[None], gain_m.astype(F32)[None], cos, sin)
    return y.reshape(x.shape)


def solution(mesh):
    def step(*args):
        return layer(*args, lax.rem(lax.axis_index("tp"), 2))

    tokens, whole, columns, rows_of = P("dp", None, None), P(None), P(None, "tp"), P("tp", None)
    return jax.shard_map(
        step,
        mesh=mesh,
        in_specs=(tokens, whole, columns, columns, columns, rows_of, whole, columns, columns, rows_of),
        out_specs=tokens,
        check_vma=False,
    )
```

```python
import functools

import jax
import jax.numpy as jnp
import numpy as np
from jax import lax
from jax.experimental import pallas as pl
from jax.experimental.pallas import tpu as pltpu
from jax.sharding import PartitionSpec as P

HEAD = 128
THETA = 10000
LOG2E = 1.4426950408889634
HIDDEN = -2e30
MESH = pl.DeviceIdType.MESH
NB = 512
FB = 256
RING = 3
Q, KV, O, GU, REST, DOWN = range(6)
PIECE = 32
AHEAD = 4
LAG = 3
OWN, FAR = LAG + 1, 2 * LAG
STG = 4
HEADS = 8
F32, BF16 = jnp.float32, jnp.bfloat16


def _dot(a, b, ca=1, cb=0):
    return lax.dot_general(a, b, (((ca,), (cb,)), ((), ())), preferred_element_type=F32)


def _if(cond):
    if isinstance(cond, bool):
        return (lambda act: act()) if cond else (lambda act: None)
    return pl.when(cond)


def _and(*conds):
    known = [c for c in conds if isinstance(c, bool)]
    rest = [c for c in conds if not isinstance(c, bool)]
    return functools.reduce(jnp.logical_and, rest) if all(known) and rest else all(known)


def layer_kernel(
    x, wq, wk, wv, wo, wg, wu, wd, cos_in, sin_in, gain_a, gain_m,
    y, h_all, q_all, r_all,
    lhs, slots, qs, kvs, vx, hid, own, snd, rcv, stg, xin, qin, rin, hst, yin, yout, cos, sin, gains,
    wsem, rs_send, rs_recv, st_sem, xs_sem, xr_sem, l_send, l_recv, l_free, x_free, in_sem, h_sem, yin_sem, yl_sem, ys_sem, yr_sem,
    first_sem, table_sem,
    *, seqs,
):
    tokens, depth = lhs.shape
    half = tokens // 2
    qcols, kcols, ff = wq.shape[1], wk.shape[1], wd.shape[0]
    nj = depth // NB
    nq = qcols // NB
    per = depth // qcols
    nwo = nj // per
    na = nq + 1 + nwo
    ngu = ff // FB
    tail = ff - ngu * FB
    nm = ngu + (1 if tail else 0) + nj
    first_d = nm - nj
    all_a = seqs * na
    total = all_a + seqs * nm
    heads = qcols // HEAD
    group = heads // (kcols // HEAD)
    np_ = half // PIECE
    lead = ngu - nj
    last = 2 * seqs - 1

    me = lax.axis_index("tp")
    core, chip = lax.rem(me, 2), lax.div(me, 2)
    partner = {"tp": chip * 2 + (1 - core)}
    across = {"tp": (1 - chip) * 2 + core}

    def start(g, kinds):
        slot = lax.rem(g, RING)

        def when(kind, cond):
            if kind not in kinds:
                return lambda act: None
            return (lambda act: act()) if len(kinds) == 1 else pl.when(cond)

        sem = wsem.at[slot]
        in_a = g < all_a
        a, m = lax.rem(g, na), lax.rem(g + (nm - all_a % nm), nm)

        @when(Q, in_a & (a < nq))
        def _():
            pltpu.make_async_copy(wq.at[:, pl.ds(pl.multiple_of(a * NB, NB), NB)], slots.at[slot], sem).start()

        @when(KV, in_a & (a == nq))
        def _():
            pltpu.make_async_copy(wk, slots.at[slot, :, pl.ds(0, kcols)], sem).start()
            pltpu.make_async_copy(wv, slots.at[slot, :, pl.ds(kcols, kcols)], sem).start()

        @when(O, in_a & (a > nq))
        def _():
            for k in range(per):
                at = pl.multiple_of(((a - nq - 1) * per + k) * NB, NB)
                pltpu.make_async_copy(wo.at[:, pl.ds(at, NB)], slots.at[slot, pl.ds(k * qcols, qcols), :], sem).start()

        in_m = jnp.logical_not(in_a) & (g < total)

        @when(GU, in_m & (m < ngu))
        def _():
            at = pl.multiple_of(m * FB, FB)
            pltpu.make_async_copy(wg.at[:, pl.ds(at, FB)], slots.at[slot, :, pl.ds(0, FB)], sem).start()
            pltpu.make_async_copy(wu.at[:, pl.ds(at, FB)], slots.at[slot, :, pl.ds(FB, FB)], sem).start()

        if tail:

            @when(REST, in_m & (m == ngu))
            def _():
                pltpu.make_async_copy(wg.at[:, pl.ds(ngu * FB, tail)], slots.at[slot, :, pl.ds(0, tail)], sem).start()
                pltpu.make_async_copy(wu.at[:, pl.ds(ngu * FB, tail)], slots.at[slot, :, pl.ds(tail, tail)], sem).start()

        @when(DOWN, in_m & (m >= first_d))
        def _():
            at = pl.multiple_of((m - first_d) * NB, NB)
            pltpu.make_async_copy(wd.at[:, pl.ds(at, NB)], slots.at[slot, pl.ds(0, ff), :], sem).start()

    def ready(g, kinds, rows=None, cols=NB):
        slot = lax.rem(g, RING)
        rows = depth if rows is None else rows
        where = slots.at[slot, pl.ds(0, rows), pl.ds(0, cols)]
        pltpu.make_async_copy(where, where, wsem.at[slot]).wait()
        start(g + RING - 1, kinds)
        return slot

    def crossed(ar, j):
        return pltpu.make_async_remote_copy(q_all.at[ar, j], r_all.at[ar, j], xs_sem.at[ar], xr_sem.at[ar, j],
                                            device_id=across, device_id_type=MESH)

    def kept(ar, j):
        at = lax.rem(j, STG)
        return pltpu.make_async_copy(stg.at[at], q_all.at[ar, j], st_sem.at[at])

    def shared(n):
        near, far = lax.rem(n, OWN), lax.rem(n, FAR)
        return pltpu.make_async_remote_copy(snd.at[near], rcv.at[far], rs_send.at[near], rs_recv.at[far],
                                            device_id=partner, device_id_type=MESH)

    def chip_sum(n):
        return (own[lax.rem(n, OWN)] + rcv[lax.rem(n, FAR)].astype(F32)).astype(BF16)

    def keep_term(n, t):
        snd[lax.rem(n, OWN)] = t[:half].astype(BF16)
        own[lax.rem(n, OWN)] = t[half:]

    def block(ar, j, term, side=None):
        n = ar * nj + j

        @pl.when(j >= LAG)
        def _():
            shared(n - LAG).wait_recv()

        @pl.when(j >= OWN)
        def _():
            shared(n - OWN).wait_send()

        if side:
            side.before(j)
            side.work(j)
        stg[lax.rem(j + 12 - LAG, STG)] = chip_sum(n + 12 - LAG)
        keep_term(n, term())

        @pl.when(j > LAG)
        def _():
            kept(ar, j - LAG - 1).wait()
            crossed(ar, j - LAG - 1).start()

        @pl.when(j >= LAG)
        def _():
            kept(ar, j - LAG).start()

        shared(n).start()
        if side:
            side.after(j)

    def drain(ar):
        for j in range(nj - LAG, nj):
            shared(ar * nj + j).wait_recv()
            stg[j % STG] = chip_sum(ar * nj + j)
            kept(ar, jnp.int32(j)).start()

    def drained(ar):
        for j in range(nj - LAG - 1, nj):
            kept(ar, jnp.int32(j)).wait()
            crossed(ar, jnp.int32(j)).start()
        for j in range(nj - OWN, nj):
            shared(ar * nj + j).wait_send()

    def block_cols(j):
        return pl.ds(pl.multiple_of(j * NB, NB), NB)

    def crossed_last(j):
        return pltpu.make_async_remote_copy(lhs.at[pl.ds(0, half), block_cols(j)], lhs.at[pl.ds(half, half), block_cols(j)],
                                            xs_sem.at[last], xr_sem.at[last, j], device_id=across, device_id_type=MESH)

    def finish_last(j):
        n = last * nj + j
        shared(n).wait_recv()
        lhs[:half, block_cols(j)] = chip_sum(n)
        crossed_last(j).start()

    def block_last(j, term):
        n = last * nj + j

        @pl.when(j >= 1)
        def _():
            finish_last(j - 1)

        @pl.when(j >= OWN)
        def _():
            shared(n - OWN).wait_send()

        keep_term(n, term())
        shared(n).start()

    def give(p):
        here = pl.ds(pl.multiple_of(half + p * PIECE, PIECE), PIECE)
        there = pl.ds(pl.multiple_of(p * PIECE, PIECE), PIECE)
        return pltpu.make_async_remote_copy(lhs.at[here, :], lhs.at[there, :], l_send, l_recv, device_id=partner, device_id_type=MESH)

    def exchanged():
        pltpu.make_async_remote_copy(lhs.at[pl.ds(half, half), :], lhs.at[pl.ds(0, half), :], l_send, l_recv,
                                     device_id=partner, device_id_type=MESH).wait()

    def free():
        pl.semaphore_signal(l_free, inc=1, device_id=partner, device_id_type=MESH)

    def scaled(rows, which, part):
        squares = jnp.zeros((PIECE, NB), F32)
        for j in range(nj):
            v = part(j, True)
            squares += v * v
        scale = lax.rsqrt(jnp.sum(squares, axis=1, keepdims=True) * (1 / depth) + 1e-6)
        for j in range(nj):
            cols = slice(j * NB, (j + 1) * NB)
            lhs[rows, cols] = (part(j, False) * scale * gains[pl.ds(which, 1), cols]).astype(BF16)

    class Operand:
        def __init__(self, c, second):
            self.c, self.second = c, second

        def loads(self, p):
            at = lax.rem(p, AHEAD)
            here = pl.ds(pl.multiple_of(p * PIECE, PIECE), PIECE)
            rows = pl.ds(pl.multiple_of(self.c * tokens + core * half + p * PIECE, PIECE), PIECE)
            return (pltpu.make_async_copy(x.at[rows, :], xin.at[at], in_sem.at[at, 0]),
                    pltpu.make_async_copy(q_all.at[self.c, :, here, :], qin.at[at], in_sem.at[at, 1]),
                    pltpu.make_async_copy(r_all.at[self.c, :, here, :], rin.at[at], in_sem.at[at, 2]))

        def each(self, p, act):
            got = self.loads(p)

            act(got[0])

            @_if(self.second)
            def _():
                act(got[1])
                act(got[2])

        def put(self, p):
            at = lax.rem(p, 2)
            here = pl.ds(pl.multiple_of(p * PIECE, PIECE), PIECE)
            return pltpu.make_async_copy(hst.at[at], h_all.at[self.c, :, here, :], h_sem.at[at])

        def begin(self):
            @_if(self.second)
            def _():
                def arrived(j, _):
                    crossed(self.c, j).wait_recv()
                    return 0

                lax.fori_loop(0, nj, arrived, 0)
                pltpu.make_async_copy(q_all.at[self.c], q_all.at[self.c], xs_sem.at[self.c]).wait()

            for p in range(min(AHEAD - 1, np_)):
                self.each(jnp.int32(p), lambda copy: copy.start())

            pl.semaphore_wait(l_free, 1)

        def before(self, p):
            @pl.when(p + AHEAD - 1 < np_)
            def _():
                self.each(p + AHEAD - 1, lambda copy: copy.start())

            self.each(p, lambda copy: copy.wait())

            @_if(_and(p >= 2, self.second))
            def _():
                self.put(p - 2).wait()

            @pl.when(p >= 1)
            def _():
                give(p - 1).start()

        def work(self, p):
            at, to = lax.rem(p, AHEAD), lax.rem(p, 2)
            rows = pl.ds(pl.multiple_of(half + p * PIECE, PIECE), PIECE)

            def part(j, new):
                if new:
                    v = xin[at, :, j * NB : (j + 1) * NB].astype(F32) + (qin[at, j].astype(F32) + rin[at, j].astype(F32))
                    hst[to, j] = v.astype(BF16)
                return hst[to, j].astype(F32)

            scaled(rows, 1 if self.second is True else jnp.where(self.second, 1, 0), part)

        def after(self, p):
            @_if(self.second)
            def _():
                self.put(p).start()

        def end(self):
            exchanged()

            @_if(self.second)
            def _():
                for p in (np_ - 2, np_ - 1):
                    self.put(jnp.int32(p)).wait()

        def last(self):
            give(jnp.int32(np_ - 1)).start()

    def with_operand(c, second, step):
        side = Operand(c, second)
        side.begin()
        lax.fori_loop(0, np_, lambda j, _: step(j, side), 0)
        side.last()
        lax.fori_loop(np_, nj, lambda j, _: step(j, None), 0)
        side.end()

    early = pl.multiple_of((1 - core) * half, half)
    late = pl.multiple_of(core * half, half)

    def turned(t):
        t = t.astype(BF16).astype(F32)
        r = pltpu.roll(t, HEAD // 2, 1)
        out = []
        for rows, place in ((slice(0, half), (1 - core) * half), (slice(half, tokens), core * half)):
            place = pl.ds(pl.multiple_of(place, half), half)
            out.append((t[rows] * cos[place, :] + r[rows] * sin[place, :]).astype(BF16))
        return jnp.concatenate(out, 0)

    def attention():
        e = HEAD**-0.5 * LOG2E
        for n in range(kcols // HEAD):
            vx[n, :, :HEAD] = kvs[:, kcols + n * HEAD : kcols + (n + 1) * HEAD]
            vx[n, :, HEAD:] = jnp.ones((tokens, HEAD), BF16)
        seen = lax.broadcasted_iota(jnp.int32, (half, half), 1) <= lax.broadcasted_iota(jnp.int32, (half, half), 0)
        many = min(HEADS, group)

        def weights(*scores):
            top = scores[0].max(axis=1, keepdims=True)
            for s in scores[1:]:
                top = jnp.maximum(top, s.max(axis=1, keepdims=True))
            return [jnp.exp2((s - top) * e).astype(BF16) for s in scores]

        def out(o):
            return (o[:, :HEAD] / o[:, HEAD:]).astype(BF16)

        def some(i, _):
            n = lax.div(i * many, group)
            kc = pl.ds(pl.multiple_of(n * HEAD, HEAD), HEAD)
            k0, k1 = kvs[pl.ds(early, half), kc], kvs[pl.ds(late, half), kc]
            v0, v1 = vx[n, pl.ds(early, half), :], vx[n, pl.ds(late, half), :]
            cols = [pl.ds(pl.multiple_of((i * many + t) * HEAD, HEAD), HEAD) for t in range(many)]
            q0 = jnp.concatenate([qs[pl.ds(early, half), c] for c in cols], 0)
            q1 = jnp.concatenate([qs[pl.ds(late, half), c] for c in cols], 0)
            s0 = _dot(jnp.concatenate([q0, q1], 0), k0, 1, 1)
            s1 = _dot(q1, k1, 1, 1)

            def of(s, t):
                return s[t * half : (t + 1) * half]

            p00, p01, p11 = [], [], []
            for t in range(many):
                p00 += weights(jnp.where(seen, of(s0, t), HIDDEN))
            for t in range(many):
                a, b = weights(of(s0, many + t), jnp.where(seen, of(s1, t), HIDDEN))
                p01.append(a)
                p11.append(b)
            o0 = _dot(jnp.concatenate(p00 + p01, 0), v0)
            o1 = _dot(jnp.concatenate(p11, 0), v1)
            for t, c in enumerate(cols):
                qs[pl.ds(early, half), c] = out(of(o0, t))
                qs[pl.ds(late, half), c] = out(of(o0, many + t) + of(o1, t))
            return 0

        lax.fori_loop(0, heads // many, some, 0)

    def first(c, _):
        g0 = c * na

        def queries(s, _):
            slot = ready(g0 + s, (Q, KV, O))
            t = _dot(lhs[...], slots[slot])
            for n in range(NB // HEAD):
                qs[:, pl.ds(pl.multiple_of(s * NB + n * HEAD, HEAD), HEAD)] = turned(t[:, n * HEAD : (n + 1) * HEAD])

            @pl.when((c >= 1) & (s == min(1, nq - 1)))
            def _():
                drain(c - 1)

            return 0

        lax.fori_loop(0, nq, queries, 0)

        slot = ready(g0 + nq, (O,) if nwo > 1 else (O, Q, GU))
        t = _dot(lhs[...], slots[slot, :, : 2 * kcols])
        for n in range(kcols // HEAD):
            cols = slice(n * HEAD, (n + 1) * HEAD)
            kvs[:, cols] = turned(t[:, cols])
        kvs[:, kcols:] = t[:, kcols:].astype(BF16)
        free()

        @pl.when(c >= 1)
        def _():
            drained(c - 1)

        attention()

        def project(j, side):
            k = lax.rem(j, per)
            g = g0 + nq + 1 + lax.div(j, per)

            @pl.when(k == 0)
            def _():
                ready(g, (O, Q, KV, GU, DOWN))

            w = slots.at[lax.rem(g, RING), pl.ds(pl.multiple_of(k * qcols, qcols), qcols), :]
            block(c, j, lambda: _dot(qs[...], w[...]), side)
            return 0

        over = c == seqs - 1
        with_operand(jnp.where(over, 0, c + 1), over, project)
        return 0

    class Result:
        def __init__(self, c):
            self.c = c

        def loads(self, j):
            at = lax.rem(j, 2)
            ar = seqs + self.c
            return [pltpu.make_async_copy(src, yin.at[at, i], yin_sem.at[at, i])
                    for i, src in enumerate((h_all.at[self.c, j], q_all.at[ar, j], r_all.at[ar, j]))]

        def puts(self, j):
            at = lax.rem(j, 2)
            row0 = pl.multiple_of(self.c * tokens + core * half, half)
            where = y.at[pl.ds(row0, half), pl.ds(pl.multiple_of(j * NB, NB), NB)]
            return (pltpu.make_async_copy(yout.at[at], where, yl_sem.at[at]),
                    pltpu.make_async_remote_copy(yout.at[at], where, ys_sem.at[at], yr_sem.at[self.c],
                                                 device_id=partner, device_id_type=MESH))

        def begin(self, j):
            crossed(seqs + self.c, j).wait_recv()
            for copy in self.loads(j):
                copy.start()

        def left(self, j):
            near, far = self.puts(j)
            near.wait()
            far.wait_send()

        def before(self, j):
            @pl.when(j + 1 < nj)
            def _():
                self.begin(j + 1)

            for copy in self.loads(j):
                copy.wait()

            @pl.when(j >= 2)
            def _():
                self.left(j - 2)

        def work(self, j):
            at = lax.rem(j, 2)
            yout[at] = (yin[at, 0].astype(F32) + (yin[at, 1].astype(F32) + yin[at, 2].astype(F32))).astype(BF16)

        def after(self, j):
            near, far = self.puts(j)
            near.start()
            far.start()

        def end(self):
            for j in (nj - 2, nj - 1):
                self.left(jnp.int32(j))
            ar = seqs + self.c
            pltpu.make_async_copy(q_all.at[ar], q_all.at[ar], xs_sem.at[ar]).wait()

    def gated(gate, up):
        return (gate * jax.nn.sigmoid(gate) * up).astype(BF16)

    def second(c, _):
        g0 = all_a + c * nm

        def gates(s, side):
            slot = ready(g0 + s, (GU, REST, DOWN))
            if side:
                side.before(s - lead)
                side.work(s - lead)
            t = _dot(lhs[...], slots[slot])
            hid[:, pl.ds(pl.multiple_of(s * FB, FB), FB)] = gated(t[:, :FB], t[:, FB:])
            if side:
                side.after(s - lead)
            else:

                @pl.when(s == 1)
                def _():
                    drain(seqs - 1 + c)

                @pl.when(s == 3)
                def _():
                    drained(seqs - 1 + c)

            return 0

        side = Result(c - 2)
        bare = jnp.where(c >= 2, lead, ngu)
        lax.fori_loop(0, bare, lambda s, _: gates(s, None), 0)

        @pl.when(c >= 2)
        def _():
            side.begin(jnp.int32(0))

        lax.fori_loop(bare, ngu, lambda s, _: gates(s, side), 0)
        if tail:
            slot = ready(g0 + ngu, (DOWN,), None, 2 * tail)
            t = _dot(lhs[...], slots[slot, :, : 2 * tail])
            hid[:, ngu * FB :] = gated(t[:, :tail], t[:, tail:])

        @pl.when(c >= 2)
        def _():
            side.end()

        more = c + 1 < seqs

        @pl.when(more)
        def _():
            free()

        def down(j, side):
            slot = ready(g0 + first_d + j, (GU, DOWN), ff)
            block(seqs + c, j, lambda: _dot(hid[...], slots[slot, :ff, :]), side)
            return 0

        @pl.when(more)
        def _():
            with_operand(c + 1, True, down)

        def down_last(j, _):
            slot = ready(g0 + first_d + j, (GU, DOWN), ff)
            block_last(j, lambda: _dot(hid[...], slots[slot, :ff, :]))
            return 0

        @pl.when(jnp.logical_not(more))
        def _():
            pl.semaphore_signal(x_free, inc=1, device_id=across, device_id_type=MESH)
            pl.semaphore_wait(x_free, 1)
            lax.fori_loop(0, nj, down_last, 0)

        return 0

    for g in range(RING - 1):
        start(jnp.int32(g), (Q, KV))
    tables = [pltpu.make_async_copy(src, dst, table_sem.at[i]) for i, (src, dst) in enumerate(((cos_in, cos), (sin_in, sin)))]

    def fetched(p):
        return pltpu.make_async_copy(x.at[pl.ds(pl.multiple_of(core * half + p * PIECE, PIECE), PIECE), :],
                                     lhs.at[pl.ds(half + p * PIECE, PIECE), :], first_sem.at[p])

    for p in range(np_):
        fetched(p).start()
    for copy in tables:
        copy.start()
    gains[0:1, :] = gain_a[...].astype(F32)
    gains[1:2, :] = gain_m[...].astype(F32)
    for ref in (qin, rin):
        ref[...] = jnp.zeros(ref.shape, BF16)
    barrier = pltpu.get_barrier_semaphore()
    for peer in (partner, across):
        pl.semaphore_signal(barrier, inc=1, device_id=peer, device_id_type=MESH)
    pl.semaphore_wait(barrier, 2)

    def normed(p, _):
        rows = pl.ds(pl.multiple_of(half + p * PIECE, PIECE), PIECE)
        fetched(p).wait()
        scaled(rows, 0, lambda j, new: lhs[rows, j * NB : (j + 1) * NB].astype(F32))

        @pl.when(p >= 1)
        def _():
            give(p - 1).start()

        return 0

    lax.fori_loop(0, np_, normed, 0)
    give(jnp.int32(np_ - 1)).start()
    for copy in tables:
        copy.wait()
    exchanged()
    lax.fori_loop(0, seqs, first, 0)
    lax.fori_loop(0, seqs, second, 0)
    finish_last(jnp.int32(nj - 1))
    for j in range(nj - OWN, nj):
        shared(jnp.int32(last * nj + j)).wait_send()

    def beside(j, side):
        side.before(j)
        side.work(j)
        side.after(j)
        return 0

    rest = Result(jnp.int32(seqs - 2))
    rest.begin(jnp.int32(0))
    lax.fori_loop(0, nj, lambda j, _: beside(j, rest), 0)
    rest.end()
    rest = Result(jnp.int32(seqs - 1))

    def h_block(j):
        at = lax.rem(j, 2)
        return pltpu.make_async_copy(h_all.at[seqs - 1, j], yin.at[at, 0], yin_sem.at[at, 0])

    h_block(jnp.int32(0)).start()

    def piece(j, _):
        at = lax.rem(j, 2)

        @pl.when(j + 1 < nj)
        def _():
            h_block(j + 1).start()

        @pl.when(j >= 2)
        def _():
            rest.left(j - 2)

        h_block(j).wait()
        crossed_last(j).wait_recv()
        here, there = lhs[:half, block_cols(j)].astype(F32), lhs[half:, block_cols(j)].astype(F32)
        yout[at] = (yin[at, 0].astype(F32) + (here + there)).astype(BF16)
        rest.after(j)
        return 0

    lax.fori_loop(0, nj, piece, 0)
    for j in (nj - 2, nj - 1):
        rest.left(jnp.int32(j))
    pltpu.make_async_copy(q_all.at[last], q_all.at[last], xs_sem.at[last]).wait()

    def arrived(c, _):
        where = y.at[pl.ds(pl.multiple_of(c * tokens + (1 - core) * half, half), half), :]
        pltpu.make_async_copy(where, where, yr_sem.at[c]).wait()
        return 0

    lax.fori_loop(0, seqs, arrived, 0)


def layer(x, gain_a, wq, wk, wv, wo, gain_m, w_gate, w_up, w_down):
    seqs, tokens, depth = x.shape
    half, nj = tokens // 2, depth // NB
    i = np.arange(HEAD // 2, dtype=np.float32)
    angle = np.arange(tokens, dtype=np.float32)[:, None] * np.float32(THETA) ** (-i / np.float32(HEAD // 2))
    cos, sin = np.cos(angle), np.sin(angle)
    cos, sin = np.concatenate([cos, cos], 1).astype(np.float32), np.concatenate([-sin, sin], 1).astype(np.float32)
    hbm, vmem = pl.BlockSpec(memory_space=pl.ANY), pl.BlockSpec(memory_space=pltpu.VMEM)
    dma, regular = pltpu.SemaphoreType.DMA, pltpu.SemaphoreType.REGULAR
    out = [
        jax.ShapeDtypeStruct((seqs * tokens, depth), BF16),
        jax.ShapeDtypeStruct((seqs, nj, half, NB), BF16),
        jax.ShapeDtypeStruct((2 * seqs, nj, half, NB), BF16),
        jax.ShapeDtypeStruct((2 * seqs, nj, half, NB), BF16),
    ]
    kv = wk.shape[1]
    scratch = [
        pltpu.VMEM((tokens, depth), BF16),
        pltpu.VMEM((RING, depth, NB), BF16),
        pltpu.VMEM((tokens, wq.shape[1]), BF16),
        pltpu.VMEM((tokens, 2 * kv), BF16),
        pltpu.VMEM((kv // HEAD, tokens, 2 * HEAD), BF16),
        pltpu.VMEM((tokens, w_down.shape[0]), BF16),
        pltpu.VMEM((OWN, half, NB), F32),
        pltpu.VMEM((OWN, half, NB), BF16),
        pltpu.VMEM((FAR, half, NB), BF16),
        pltpu.VMEM((STG, half, NB), BF16),
        pltpu.VMEM((AHEAD, PIECE, depth), BF16),
        pltpu.VMEM((AHEAD, nj, PIECE, NB), BF16),
        pltpu.VMEM((AHEAD, nj, PIECE, NB), BF16),
        pltpu.VMEM((2, nj, PIECE, NB), BF16),
        pltpu.VMEM((2, 3, half, NB), BF16),
        pltpu.VMEM((2, half, NB), BF16),
        pltpu.VMEM((tokens, HEAD), F32),
        pltpu.VMEM((tokens, HEAD), F32),
        pltpu.VMEM((2, depth), F32),
        dma((RING,)), dma((OWN,)), dma((FAR,)), dma((STG,)), dma((2 * seqs,)), dma((2 * seqs, nj)),
        dma, dma, regular, regular,
        dma((AHEAD, 3)), dma((2,)), dma((2, 3)), dma((2,)), dma((2,)), dma((seqs,)),
        dma((half // PIECE,)), dma((2,)),
    ]
    y, *_ = pl.pallas_call(
        functools.partial(layer_kernel, seqs=seqs),
        out_shape=out,
        in_specs=[hbm] * 10 + [vmem] * 2,
        out_specs=[hbm] * 4,
        scratch_shapes=scratch,
        compiler_params=pltpu.CompilerParams(collective_id=0, has_side_effects=True, vmem_limit_bytes=67043328),
        name="layer",
    )(x.reshape(seqs * tokens, depth), wq, wk, wv, wo, w_gate, w_up, w_down, cos, sin, gain_a[None], gain_m[None])
    return y.reshape(x.shape)


def solution(mesh):
    def step(*args):
        return layer(*args)

    tokens, whole, columns, rows_of = P("dp", None, None), P(None), P(None, "tp"), P("tp", None)
    return jax.shard_map(
        step,
        mesh=mesh,
        in_specs=(tokens, whole, columns, columns, columns, rows_of, whole, columns, columns, rows_of),
        out_specs=tokens,
        check_vma=False,
    )
```

```python
import functools

import jax
import jax.numpy as jnp
import numpy as np
from jax import lax
from jax.experimental import pallas as pl
from jax.experimental.pallas import tpu as pltpu
from jax.sharding import PartitionSpec as P

HEAD = 128
THETA = 10000
LOG2E = 1.4426950408889634
HIDDEN = -2e30
MESH = pl.DeviceIdType.MESH
NB = 512
FB = 256
EARLY = 1
RING = 3
Q, KV, O, GU, REST, DOWN = range(6)
LANES = 128
PIECE = 32
AHEAD = 4
LAG = 3
OWN, FAR = LAG + 1, 2 * LAG
STG = 4
YB = 3
QB = 128
HEADS = 8
F32, BF16 = jnp.float32, jnp.bfloat16


def _dot(a, b, ca=1, cb=0):
    return lax.dot_general(a, b, (((ca,), (cb,)), ((), ())), preferred_element_type=F32)


def _if(cond):
    if isinstance(cond, bool):
        return (lambda act: act()) if cond else (lambda act: None)
    return pl.when(cond)


def _and(*conds):
    known = [c for c in conds if isinstance(c, bool)]
    rest = [c for c in conds if not isinstance(c, bool)]
    return functools.reduce(jnp.logical_and, rest) if all(known) and rest else all(known)


def _shares(seqs, half):
    big = half + PIECE
    return big, seqs * half - (seqs - 1) * big


def layer_kernel(
    x, wq, wk, wv, wo, wg, wu, wd, cos_in, sin_in, gain_a, gain_m,
    y, h_all, q_all, r_all,
    lhs, slots, qs, kvs, vx, hid, own, snd, rcv, stg, xin, qin, rin, hst, yin, yout, cos, sin, gain_in, gains,
    wsem, rs_send, rs_recv, st_sem, xs_sem, xr_sem, l_send, l_recv, l_free, x_free, in_sem, h_sem, yin_sem, yl_sem, ys_sem, yr_sem,
    first_sem, table_sem, xh_sem,
    *, seqs,
):
    tokens, depth = qs.shape[0], x.shape[1]
    half = tokens // 2
    big, small = _shares(seqs, half)
    qcols, kcols, ff = wq.shape[1], wk.shape[1], wd.shape[0]
    nj = depth // NB
    nq = qcols // NB
    per = depth // qcols
    nwo = nj // per
    na = nq + 1 + nwo
    ngu = ff // FB
    tail = ff - ngu * FB
    nm = ngu + (1 if tail else 0) + nj
    first_d = nm - nj
    all_a = seqs * na
    total = all_a + seqs * nm
    heads = qcols // HEAD
    group = heads // (kcols // HEAD)
    np_ = half // PIECE
    last = 2 * seqs - 1

    me = lax.axis_index("tp")
    core, chip = lax.rem(me, 2), lax.div(me, 2)
    partner = {"tp": chip * 2 + (1 - core)}
    across = {"tp": (1 - chip) * 2 + core}

    def start(g, kinds):
        slot = lax.rem(g, RING)

        def when(kind, cond):
            if kind not in kinds:
                return lambda act: None
            return (lambda act: act()) if len(kinds) == 1 else pl.when(cond)

        sem = wsem.at[slot]
        in_a = g < all_a
        a, m = lax.rem(g, na), lax.rem(g + (nm - all_a % nm), nm)

        @when(Q, in_a & (a < nq))
        def _():
            pltpu.make_async_copy(wq.at[:, pl.ds(pl.multiple_of(a * NB, NB), NB)], slots.at[slot], sem).start()

        @when(KV, in_a & (a == nq))
        def _():
            pltpu.make_async_copy(wk, slots.at[slot, :, pl.ds(0, kcols)], sem).start()
            pltpu.make_async_copy(wv, slots.at[slot, :, pl.ds(kcols, kcols)], sem).start()

        @when(O, in_a & (a > nq))
        def _():
            for k in range(per):
                at = pl.multiple_of(((a - nq - 1) * per + k) * NB, NB)
                pltpu.make_async_copy(wo.at[:, pl.ds(at, NB)], slots.at[slot, pl.ds(k * qcols, qcols), :], sem).start()

        in_m = jnp.logical_not(in_a) & (g < total)

        @when(GU, in_m & (m < ngu))
        def _():
            at = pl.multiple_of(m * FB, FB)
            pltpu.make_async_copy(wg.at[:, pl.ds(at, FB)], slots.at[slot, :, pl.ds(0, FB)], sem).start()
            pltpu.make_async_copy(wu.at[:, pl.ds(at, FB)], slots.at[slot, :, pl.ds(FB, FB)], sem).start()

        if tail:

            @when(REST, in_m & (m == ngu))
            def _():
                pltpu.make_async_copy(wg.at[:, pl.ds(ngu * FB, tail)], slots.at[slot, :, pl.ds(0, tail)], sem).start()
                pltpu.make_async_copy(wu.at[:, pl.ds(ngu * FB, tail)], slots.at[slot, :, pl.ds(tail, tail)], sem).start()

        @when(DOWN, in_m & (m >= first_d))
        def _():
            at = pl.multiple_of((m - first_d) * NB, NB)
            pltpu.make_async_copy(wd.at[:, pl.ds(at, NB)], slots.at[slot, pl.ds(0, ff), :], sem).start()

    def ready(g, kinds, rows=None, cols=NB):
        slot = lax.rem(g, RING)
        rows = depth if rows is None else rows
        where = slots.at[slot, pl.ds(0, rows), pl.ds(0, cols)]
        pltpu.make_async_copy(where, where, wsem.at[slot]).wait()
        start(g + RING - 1, kinds)
        return slot

    class Sum:
        def __init__(self, ar, which, row0, n):
            self.ar, self.which, self.row0, self.n = ar, which, row0, n

        def far(self, j, at, n, sem):
            rows = pl.ds(pl.multiple_of(self.row0 + at, PIECE), n)
            return pltpu.make_async_remote_copy(q_all.at[self.which, j, rows, :], r_all.at[self.which, j, rows, :], xs_sem.at[self.ar], sem,
                                                device_id=across, device_id_type=MESH)

        def crossed(self, j):
            return self.far(j, 0, self.n, xr_sem.at[self.ar, j])

        def head(self, j):
            return self.far(j, 0, PIECE, xh_sem.at[j])

        def rest(self, j):
            return self.far(j, PIECE, self.n - PIECE, xr_sem.at[self.ar, j])

        def cross(self, j):
            if self.which:
                self.crossed(j).start()
            else:

                @pl.when(self.ar == EARLY)
                def _():
                    self.head(j).start()

                @pl.when(self.ar != EARLY)
                def _():
                    self.crossed(j).start()

        def each(self, act):
            def one(j, _):
                act(j)
                return 0

            lax.fori_loop(0, nj, one, 0)

        def sent(self):
            whole = q_all.at[self.which, :, pl.ds(pl.multiple_of(self.row0, PIECE), self.n), :]
            pltpu.make_async_copy(whole, whole, xs_sem.at[self.ar]).wait()

        def kept(self, j):
            at = lax.rem(j, STG)
            rows = pl.ds(pl.multiple_of(self.row0, PIECE), self.n)
            return pltpu.make_async_copy(stg.at[at, pl.ds(0, self.n), :], q_all.at[self.which, j, rows, :], st_sem.at[at])

        def shared(self, j):
            i = self.ar * nj + j
            near, far = lax.rem(i, OWN), lax.rem(i, FAR)
            return pltpu.make_async_remote_copy(snd.at[near, pl.ds(0, self.n), :], rcv.at[far, pl.ds(0, self.n), :], rs_send.at[near],
                                                rs_recv.at[far], device_id=partner, device_id_type=MESH)

        def of_chip(self, j):
            i = self.ar * nj + j
            return (own[lax.rem(i, OWN), : self.n] + rcv[lax.rem(i, FAR), : self.n].astype(F32)).astype(BF16)

        def keep_term(self, j, t):
            i = self.ar * nj + j
            snd[lax.rem(i, OWN), : self.n] = t[: self.n].astype(BF16)
            own[lax.rem(i, OWN), : self.n] = t[self.n :]

    def sum_a(c):
        return Sum(c, 0, c * half, half)

    def sum_m(m):
        return Sum(seqs + m, 1, m * big, big)

    final = Sum(jnp.int32(last), 1, (seqs - 1) * big, small)

    def block(s, j, term, *sides):
        @pl.when(j >= LAG)
        def _():
            s.shared(j - LAG).wait_recv()

        @pl.when(j >= OWN)
        def _():
            s.shared(j - OWN).wait_send()

        for side in sides:
            side.before(j)
        for side in sides:
            side.work(j)
        stg[lax.rem(j + 12 - LAG, STG), : s.n] = s.of_chip(j + 12 - LAG)
        s.keep_term(j, term())

        @pl.when(j > LAG)
        def _():
            s.kept(j - LAG - 1).wait()
            s.cross(j - LAG - 1)

        @pl.when(j >= LAG)
        def _():
            s.kept(j - LAG).start()

        s.shared(j).start()
        for side in sides:
            side.after(j)

    def drain(s):
        for j in range(nj - LAG, nj):
            s.shared(jnp.int32(j)).wait_recv()
            stg[j % STG, : s.n] = s.of_chip(jnp.int32(j))
            s.kept(jnp.int32(j)).start()

    def drained(s):
        for j in range(nj - LAG - 1, nj):
            s.kept(jnp.int32(j)).wait()
            s.cross(jnp.int32(j))
        for j in range(nj - OWN, nj):
            s.shared(jnp.int32(j)).wait_send()
        if not s.which:

            @pl.when(s.ar == EARLY)
            def _():
                s.each(lambda j: s.rest(j).start())

    def block_cols(j):
        return pl.ds(pl.multiple_of(j * NB, NB), NB)

    def crossed_last(j):
        return pltpu.make_async_remote_copy(lhs.at[pl.ds(0, small), block_cols(j)], lhs.at[pl.ds(small, small), block_cols(j)],
                                            xs_sem.at[last], xr_sem.at[last, j], device_id=across, device_id_type=MESH)

    def finish_last(j):
        final.shared(j).wait_recv()
        lhs[:small, block_cols(j)] = final.of_chip(j)
        crossed_last(j).start()

    def block_last(j, term, side):
        side.before(j)
        side.work(j)
        side.after(j)

        @pl.when(j >= 1)
        def _():
            finish_last(j - 1)

        @pl.when(j >= OWN)
        def _():
            final.shared(j - OWN).wait_send()

        final.keep_term(j, term())
        final.shared(j).start()

    def exchanged(n):
        pltpu.make_async_remote_copy(lhs.at[pl.ds(n, n), :], lhs.at[pl.ds(0, n), :], l_send, l_recv,
                                     device_id=partner, device_id_type=MESH).wait()

    def free():
        pl.semaphore_signal(l_free, inc=1, device_id=partner, device_id_type=MESH)

    def scaled(rows, which, part):
        squares = jnp.zeros((PIECE, NB), F32)
        for j in range(nj):
            v = part(j, True)
            squares += v * v
        scale = lax.rsqrt(jnp.sum(squares, axis=1, keepdims=True) * (1 / depth) + 1e-6)
        for j in range(nj):
            cols = slice(j * NB, (j + 1) * NB)
            lhs[rows, cols] = (part(j, False) * scale * gains[pl.ds(which, 1), cols]).astype(BF16)

    class Operand:
        def __init__(self, piece0, pieces, base, second):
            self.piece0, self.pieces, self.base, self.second = piece0, pieces, base, second

        def here(self, p):
            return pl.ds(pl.multiple_of((self.piece0 + p) * PIECE, PIECE), PIECE)

        def loads(self, p):
            at, i = lax.rem(p, AHEAD), self.piece0 + p
            row = lax.div(i, np_) * tokens + core * half + lax.rem(i, np_) * PIECE
            return (pltpu.make_async_copy(x.at[pl.ds(pl.multiple_of(row, PIECE), PIECE), :], xin.at[at], in_sem.at[at, 0]),
                    pltpu.make_async_copy(q_all.at[0, :, self.here(p), :], qin.at[at], in_sem.at[at, 1]),
                    pltpu.make_async_copy(r_all.at[0, :, self.here(p), :], rin.at[at], in_sem.at[at, 2]))[: 3 if self.second else 1]

        def put(self, p):
            at = lax.rem(p, 2)
            return pltpu.make_async_copy(hst.at[at], h_all.at[:, self.here(p), :], h_sem.at[at])

        def give(self, p):
            here = pl.ds(pl.multiple_of(self.base + p * PIECE, PIECE), PIECE)
            there = pl.ds(pl.multiple_of(p * PIECE, PIECE), PIECE)
            return pltpu.make_async_remote_copy(lhs.at[here, :], lhs.at[there, :], l_send, l_recv, device_id=partner, device_id_type=MESH)

        def begin(self):
            for p in range(AHEAD - 1):
                for copy in self.loads(jnp.int32(p)):
                    copy.start()
            pl.semaphore_wait(l_free, 1)

        def before(self, p):
            @pl.when(p + AHEAD - 1 < self.pieces)
            def _():
                for copy in self.loads(p + AHEAD - 1):
                    copy.start()

            for copy in self.loads(p):
                copy.wait()

            @_if(_and(p >= 2, self.second))
            def _():
                self.put(p - 2).wait()

            @pl.when(p >= 1)
            def _():
                self.give(p - 1).start()

        def work(self, p):
            at, to = lax.rem(p, AHEAD), lax.rem(p, 2)
            rows = pl.ds(pl.multiple_of(self.base + p * PIECE, PIECE), PIECE)

            def plain(j, new):
                return xin[at, :, j * NB : (j + 1) * NB].astype(F32)

            def part(j, new):
                if new:
                    v = xin[at, :, j * NB : (j + 1) * NB].astype(F32) + (qin[at, j].astype(F32) + rin[at, j].astype(F32))
                    hst[to, j] = v.astype(BF16)
                return hst[to, j].astype(F32)

            scaled(rows, int(self.second), part if self.second else plain)

        def after(self, p):
            if self.second:
                self.put(p).start()

        def last(self):
            self.give(jnp.int32(self.pieces - 1)).start()

        def end(self):
            if self.second:
                for p in (2, 1):
                    self.put(jnp.int32(self.pieces - p)).wait()

    def with_operand(side, step):
        side.begin()
        lax.fori_loop(0, side.pieces, lambda j, _: step(j, side), 0)
        side.last()
        lax.fori_loop(side.pieces, nj, lambda j, _: step(j), 0)
        side.end()

    def have(s, what):
        s.each(lambda j: what(j).wait_recv())

    early = pl.multiple_of((1 - core) * half, half)
    late = pl.multiple_of(core * half, half)

    def turned(t):
        t = t.astype(F32)
        r = pltpu.roll(t, HEAD // 2, 1)
        out = []
        for rows, place in ((slice(0, half), (1 - core) * half), (slice(half, tokens), core * half)):
            place = pl.ds(pl.multiple_of(place, half), half)
            out.append((t[rows] * cos[place, :] + r[rows] * sin[place, :]).astype(BF16))
        return jnp.concatenate(out, 0)

    def turn(s):
        for n in range(NB // HEAD):
            cols = pl.ds(pl.multiple_of(s * NB + n * HEAD, HEAD), HEAD)
            qs[:, cols] = turned(qs[:, cols])

    def attention():
        e = HEAD**-0.5 * LOG2E
        for n in range(kcols // HEAD):
            vx[n, :, :HEAD] = kvs[:, kcols + n * HEAD : kcols + (n + 1) * HEAD]
            vx[n, :, HEAD:] = jnp.ones((tokens, HEAD), BF16)
        seen = lax.broadcasted_iota(jnp.int32, (QB, QB), 1) <= lax.broadcasted_iota(jnp.int32, (QB, QB), 0)
        many = min(HEADS, group)

        def rows(b):
            at = b * QB
            return pl.ds(pl.multiple_of(early + at if at < half else late + at - half, QB), QB)

        def some(i, _):
            n = lax.div(i * many, group)
            kc = pl.ds(pl.multiple_of(n * HEAD, HEAD), HEAD)
            cols = [pl.ds(pl.multiple_of((i * many + t) * HEAD, HEAD), HEAD) for t in range(many)]
            keys = [kvs[rows(b), kc] for b in range(tokens // QB)]
            values = [vx[n, rows(b), :] for b in range(tokens // QB)]
            for b in range(tokens // QB):
                q = jnp.concatenate([qs[rows(b), c] for c in cols], 0)
                scores = _dot(q, jnp.concatenate(keys[: b + 1], 0), 1, 1)
                weights = []
                for t in range(many):
                    of = scores[t * QB : (t + 1) * QB]
                    parts = [of[:, u * QB : (u + 1) * QB] for u in range(b)] + [jnp.where(seen, of[:, b * QB :], HIDDEN)]
                    top = functools.reduce(jnp.maximum, parts).max(axis=1, keepdims=True)
                    weights.append(jnp.concatenate([jnp.exp2((u - top) * e).astype(BF16) for u in parts], 1))
                o = _dot(jnp.concatenate(weights, 0), jnp.concatenate(values[: b + 1], 0))
                for t, c in enumerate(cols):
                    of = o[t * QB : (t + 1) * QB]
                    hid[rows(b), c] = (of[:, :HEAD] / of[:, HEAD:]).astype(BF16)
            return 0

        lax.fori_loop(0, heads // many, some, 0)

    def first(c, _):
        g0 = c * na

        def queries(s, _):
            slot = ready(g0 + s, (Q, KV, O))
            turn(jnp.maximum(s - 1, 0))
            qs[:, pl.ds(pl.multiple_of(s * NB, NB), NB)] = _dot(lhs[:tokens], slots[slot]).astype(BF16)

            @pl.when((c >= 1) & (s == min(1, nq - 1)))
            def _():
                drain(sum_a(c - 1))

            return 0

        lax.fori_loop(0, nq, queries, 0)

        slot = ready(g0 + nq, (O,) if nwo > 1 else (O, Q, GU))
        turn(nq - 1)
        t = _dot(lhs[:tokens], slots[slot, :, : 2 * kcols])
        for n in range(kcols // HEAD):
            cols = slice(n * HEAD, (n + 1) * HEAD)
            kvs[:, cols] = turned(t[:, cols].astype(BF16))
        kvs[:, kcols:] = t[:, kcols:].astype(BF16)
        free()

        @pl.when(c >= 1)
        def _():
            drained(sum_a(c - 1))

        attention()

        def project(j, *sides):
            k = lax.rem(j, per)
            g = g0 + nq + 1 + lax.div(j, per)

            @pl.when(k == 0)
            def _():
                ready(g, (O, Q, KV, GU, DOWN))

            w = slots.at[lax.rem(g, RING), pl.ds(pl.multiple_of(k * qcols, qcols), qcols), :]
            block(sum_a(c), j, lambda: _dot(hid[:tokens, :qcols], w[...]), *sides)
            return 0

        @pl.when(c + 1 < seqs)
        def _():
            with_operand(Operand((c + 1) * np_, np_, half, False), project)
            exchanged(half)

        @pl.when(c + 1 == seqs)
        def _():
            s = sum_a(jnp.int32(0))
            have(s, s.crossed)
            s.sent()
            s = sum_a(jnp.int32(EARLY))
            have(s, s.head)
            with_operand(Operand(jnp.int32(0), big // PIECE, big, True), project)
            exchanged(big)

        return 0

    class Result:
        def __init__(self, c, valid=True):
            self.c, self.valid = c, valid

        def loads(self, j):
            at = lax.rem(j, YB)
            rows = pl.ds(pl.multiple_of(self.c * half, half), half)
            return [pltpu.make_async_copy(src, yin.at[at, i], yin_sem.at[at, i])
                    for i, src in enumerate((h_all.at[j, rows, :], q_all.at[1, j, rows, :], r_all.at[1, j, rows, :]))]

        def puts(self, j):
            at = lax.rem(j, YB)
            row0 = pl.multiple_of(self.c * tokens + core * half, half)
            where = y.at[pl.ds(row0, half), block_cols(j)]
            return (pltpu.make_async_copy(yout.at[at], where, yl_sem.at[at]),
                    pltpu.make_async_remote_copy(yout.at[at], where, ys_sem.at[at], yr_sem.at[self.c],
                                                 device_id=partner, device_id_type=MESH))

        def fetch(self, j):
            sum_m(self.c).crossed(j).wait_recv()
            for copy in self.loads(j):
                copy.start()

        def begin(self):
            @_if(self.valid)
            def _():
                for j in range(YB - 1):
                    self.fetch(jnp.int32(j))

        def left(self, j):
            near, far = self.puts(j)
            near.wait()
            far.wait_send()

        def before(self, j):
            @_if(_and(self.valid, j + YB - 1 < nj))
            def _():
                self.fetch(j + YB - 1)

            @_if(self.valid)
            def _():
                for copy in self.loads(j):
                    copy.wait()

            @_if(_and(self.valid, j >= YB))
            def _():
                self.left(j - YB)

        def work(self, j):
            at = lax.rem(j, YB)
            yout[at] = (yin[at, 0].astype(F32) + (yin[at, 1].astype(F32) + yin[at, 2].astype(F32))).astype(BF16)

        def after(self, j):
            @_if(self.valid)
            def _():
                near, far = self.puts(j)
                near.start()
                far.start()

        def end(self):
            @_if(self.valid)
            def _():
                for j in range(nj - YB, nj):
                    self.left(jnp.int32(j))
                sum_m(self.c).sent()

    def gated(gate, up):
        return (gate * jax.nn.sigmoid(gate) * up).astype(BF16)

    def second(m, n):
        g0 = all_a + m * nm

        def before(act):
            if n == small:
                act(sum_m(m - 1))
            else:

                @pl.when(m == 0)
                def _():
                    act(sum_a(jnp.int32(seqs - 1)))

                @pl.when(m > 0)
                def _():
                    act(sum_m(m - 1))

        def gates(s, _):
            slot = ready(g0 + s, (GU, REST, DOWN))
            t = _dot(lhs[: 2 * n], slots[slot])
            hid[: 2 * n, pl.ds(pl.multiple_of(s * FB, FB), FB)] = gated(t[:, :FB], t[:, FB:])

            @pl.when(s == 1)
            def _():
                before(drain)

            @pl.when(s == 3)
            def _():
                before(drained)
                Result(m - 2, m >= 2).end()

            return 0

        lax.fori_loop(0, ngu, gates, 0)
        if tail:
            slot = ready(g0 + ngu, (DOWN,), None, 2 * tail)
            t = _dot(lhs[: 2 * n], slots[slot, :, : 2 * tail])
            hid[: 2 * n, ngu * FB :] = gated(t[:, :tail], t[:, tail:])

        def down(j):
            slot = ready(g0 + first_d + j, (GU, DOWN), ff)
            return lambda: _dot(hid[: 2 * n], slots[slot, :ff, :])

        return down

    def share(m, _):
        down = second(m, big)
        free()

        @pl.when(m == 0)
        def _():
            s = sum_a(jnp.int32(EARLY))
            have(s, s.rest)
            s.sent()

        @pl.when(m + 2 < seqs)
        def _():
            s = sum_a(m + 2)
            have(s, s.crossed)
            s.sent()

        done = Result(m - 1, m >= 1)
        done.begin()

        def step(j, *sides):
            block(sum_m(m), j, down(j), *sides, done)
            return 0

        ends = m == seqs - 2
        next_n = jnp.where(ends, small, big)
        with_operand(Operand((m + 1) * (big // PIECE), lax.div(next_n, PIECE), next_n, True), step)

        @pl.when(ends)
        def _():
            exchanged(small)

        @pl.when(jnp.logical_not(ends))
        def _():
            exchanged(big)

        return 0

    def last_share():
        down = second(seqs - 1, small)
        pl.semaphore_signal(x_free, inc=1, device_id=across, device_id_type=MESH)
        pl.semaphore_wait(x_free, 1)
        done = Result(jnp.int32(seqs - 2))
        done.begin()

        def step(j, _):
            block_last(j, down(j), done)
            return 0

        lax.fori_loop(0, nj, step, 0)
        finish_last(jnp.int32(nj - 1))
        for j in range(nj - OWN, nj):
            final.shared(jnp.int32(j)).wait_send()
        done.end()

    def fetched(p):
        owner = jnp.where(p < np_, 1 - core, core)
        rows = pl.ds(pl.multiple_of(owner * half + lax.rem(p, np_) * PIECE, PIECE), PIECE)
        return pltpu.make_async_copy(x.at[rows, :], lhs.at[pl.ds(pl.multiple_of(p * PIECE, PIECE), PIECE), :], first_sem.at[p])

    tables = [pltpu.make_async_copy(src, dst, table_sem.at[i]) for i, (src, dst) in
              enumerate(((gain_a, gain_in.at[0]), (gain_m, gain_in.at[1]), (cos_in, cos), (sin_in, sin)))]
    for p in range(2 * np_):
        fetched(jnp.int32(p)).start()
    for copy in tables:
        copy.start()
    for g in range(RING - 1):
        start(jnp.int32(g), (Q, KV))
    barrier = pltpu.get_barrier_semaphore()
    for peer in (partner, across):
        pl.semaphore_signal(barrier, inc=1, device_id=peer, device_id_type=MESH)
    for i in range(2):
        tables[i].wait()
        wide = gain_in[i].astype(F32)
        for r in range(depth // LANES):
            gains[i : i + 1, r * LANES : (r + 1) * LANES] = wide[r : r + 1]
    pl.semaphore_wait(barrier, 2)

    def normed(p, _):
        rows = pl.ds(pl.multiple_of(p * PIECE, PIECE), PIECE)
        fetched(p).wait()
        scaled(rows, 0, lambda j, new: lhs[rows, j * NB : (j + 1) * NB].astype(F32))
        return 0

    lax.fori_loop(0, 2 * np_, normed, 0)
    for copy in tables[2:]:
        copy.wait()
    lax.fori_loop(0, seqs, first, 0)
    lax.fori_loop(0, seqs - 1, share, 0)
    last_share()

    rest = Result(jnp.int32(seqs - 1))
    over = (seqs - 1) * (big - half)

    def blocks(j):
        at, row0 = lax.rem(j, YB), (seqs - 1) * half
        return [pltpu.make_async_copy(src.at[j, pl.ds(row0, n), :], yin.at[at, i, pl.ds(0, n), :], yin_sem.at[at, i])
                for i, (src, n) in enumerate(((h_all, half), (q_all.at[1], over), (r_all.at[1], over)))]

    for j in range(YB - 1):
        for copy in blocks(jnp.int32(j)):
            copy.start()

    def piece(j, _):
        at = lax.rem(j, YB)

        @pl.when(j + YB - 1 < nj)
        def _():
            for copy in blocks(j + YB - 1):
                copy.start()

        @pl.when(j >= YB)
        def _():
            rest.left(j - YB)

        for copy in blocks(j):
            copy.wait()
        crossed_last(j).wait_recv()
        here, there = lhs[:small, block_cols(j)].astype(F32), lhs[small : 2 * small, block_cols(j)].astype(F32)
        yout[at, :over] = (yin[at, 0, :over].astype(F32) + (yin[at, 1, :over].astype(F32) + yin[at, 2, :over].astype(F32))).astype(BF16)
        yout[at, over:] = (yin[at, 0, over:].astype(F32) + (here + there)).astype(BF16)
        rest.after(j)
        return 0

    lax.fori_loop(0, nj, piece, 0)
    for j in range(nj - YB, nj):
        rest.left(jnp.int32(j))
    final.sent()

    def arrived(c, _):
        where = y.at[pl.ds(pl.multiple_of(c * tokens + (1 - core) * half, half), half), :]
        pltpu.make_async_copy(where, where, yr_sem.at[c]).wait()
        return 0

    lax.fori_loop(0, seqs, arrived, 0)


def layer(x, gain_a, wq, wk, wv, wo, gain_m, w_gate, w_up, w_down):
    seqs, tokens, depth = x.shape
    half, nj = tokens // 2, depth // NB
    big, _ = _shares(seqs, half)
    i = np.arange(HEAD // 2, dtype=np.float32)
    angle = np.arange(tokens, dtype=np.float32)[:, None] * np.float32(THETA) ** (-i / np.float32(HEAD // 2))
    cos, sin = np.cos(angle), np.sin(angle)
    cos, sin = np.concatenate([cos, cos], 1).astype(np.float32), np.concatenate([-sin, sin], 1).astype(np.float32)
    hbm = pl.BlockSpec(memory_space=pl.ANY)
    dma, regular = pltpu.SemaphoreType.DMA, pltpu.SemaphoreType.REGULAR
    out = [
        jax.ShapeDtypeStruct((seqs * tokens, depth), BF16),
        jax.ShapeDtypeStruct((nj, seqs * half, NB), BF16),
        jax.ShapeDtypeStruct((2, nj, seqs * half, NB), BF16),
        jax.ShapeDtypeStruct((2, nj, seqs * half, NB), BF16),
    ]
    kv = wk.shape[1]
    scratch = [
        pltpu.VMEM((2 * big, depth), BF16),
        pltpu.VMEM((RING, depth, NB), BF16),
        pltpu.VMEM((tokens, wq.shape[1]), BF16),
        pltpu.VMEM((tokens, 2 * kv), BF16),
        pltpu.VMEM((kv // HEAD, tokens, 2 * HEAD), BF16),
        pltpu.VMEM((2 * big, w_down.shape[0]), BF16),
        pltpu.VMEM((OWN, big, NB), F32),
        pltpu.VMEM((OWN, big, NB), BF16),
        pltpu.VMEM((FAR, big, NB), BF16),
        pltpu.VMEM((STG, big, NB), BF16),
        pltpu.VMEM((AHEAD, PIECE, depth), BF16),
        pltpu.VMEM((AHEAD, nj, PIECE, NB), BF16),
        pltpu.VMEM((AHEAD, nj, PIECE, NB), BF16),
        pltpu.VMEM((2, nj, PIECE, NB), BF16),
        pltpu.VMEM((YB, 3, half, NB), BF16),
        pltpu.VMEM((YB, half, NB), BF16),
        pltpu.VMEM((tokens, HEAD), F32),
        pltpu.VMEM((tokens, HEAD), F32),
        pltpu.VMEM((2, depth // LANES, LANES), BF16),
        pltpu.VMEM((2, depth), F32),
        dma((RING,)), dma((OWN,)), dma((FAR,)), dma((STG,)), dma((2 * seqs,)), dma((2 * seqs, nj)),
        dma, dma, regular, regular,
        dma((AHEAD, 3)), dma((2,)), dma((YB, 3)), dma((YB,)), dma((YB,)), dma((seqs,)),
        dma((tokens // PIECE,)), dma((4,)), dma((nj,)),
    ]
    y, *_ = pl.pallas_call(
        functools.partial(layer_kernel, seqs=seqs),
        out_shape=out,
        in_specs=[hbm] * 12,
        out_specs=[hbm] * 4,
        scratch_shapes=scratch,
        compiler_params=pltpu.CompilerParams(collective_id=0, has_side_effects=True, vmem_limit_bytes=67043328),
        name="layer",
    )(x.reshape(seqs * tokens, depth), wq, wk, wv, wo, w_gate, w_up, w_down, cos, sin,
      gain_a.reshape(-1, LANES), gain_m.reshape(-1, LANES))
    return y.reshape(x.shape)


def solution(mesh):
    def step(*args):
        return layer(*args)

    tokens, whole, columns, rows_of = P("dp", None, None), P(None), P(None, "tp"), P("tp", None)
    return jax.shard_map(
        step,
        mesh=mesh,
        in_specs=(tokens, whole, columns, columns, columns, rows_of, whole, columns, columns, rows_of),
        out_specs=tokens,
        check_vma=False,
    )
```

```python
import functools

import jax
import jax.numpy as jnp
import numpy as np
from jax import lax
from jax.experimental import pallas as pl
from jax.experimental.pallas import tpu as pltpu
from jax.sharding import PartitionSpec as P

HEAD = 128
THETA = 10000
LOG2E = 1.4426950408889634
HIDDEN = -2e30
MESH = pl.DeviceIdType.MESH
NB = 512
FB = 256
EARLY = 1
RING = 3
Q, KV, O, GU, REST, DOWN = range(6)
LANES = 128
PIECE = 32
AHEAD = 4
LAG = 3
OWN, FAR = LAG + 1, 2 * LAG
STG = 4
YB = 4
QB = 128
HEADS = 8
F32, BF16 = jnp.float32, jnp.bfloat16


def _dot(a, b, ca=1, cb=0):
    return lax.dot_general(a, b, (((ca,), (cb,)), ((), ())), preferred_element_type=F32)


def _if(cond):
    if isinstance(cond, bool):
        return (lambda act: act()) if cond else (lambda act: None)
    return pl.when(cond)


def _and(*conds):
    known = [c for c in conds if isinstance(c, bool)]
    rest = [c for c in conds if not isinstance(c, bool)]
    return functools.reduce(jnp.logical_and, rest) if all(known) and rest else all(known)


def _shares(seqs, half):
    big = half + PIECE
    return big, seqs * half - (seqs - 1) * big


def layer_kernel(
    x, wq, wk, wv, wo, wg, wu, wd, cos_in, sin_in, gain_a, gain_m,
    y, h_all, q_all, r_all,
    lhs, slots, qs, kvs, vx, hid, own, snd, rcv, stg, xin, qin, rin, hst, yin, yout, cos, sin, gain_in, gains,
    wsem, rs_send, rs_recv, st_sem, xs_sem, xr_sem, l_send, l_recv, l_free, x_free, in_sem, h_sem, yin_sem, yl_sem, ys_sem, yr_sem,
    first_sem, table_sem, xh_sem,
    *, seqs,
):
    tokens, depth = qs.shape[0], x.shape[1]
    half = tokens // 2
    big, small = _shares(seqs, half)
    qcols, kcols, ff = wq.shape[1], wk.shape[1], wd.shape[0]
    nj = depth // NB
    nq = qcols // NB
    per = depth // qcols
    nwo = nj // per
    na = nq + 1 + nwo
    ngu = ff // FB
    tail = ff - ngu * FB
    nm = ngu + (1 if tail else 0) + nj
    first_d = nm - nj
    all_a = seqs * na
    total = all_a + seqs * nm
    heads = qcols // HEAD
    group = heads // (kcols // HEAD)
    np_ = half // PIECE
    last = 2 * seqs - 1

    me = lax.axis_index("tp")
    core, chip = lax.rem(me, 2), lax.div(me, 2)
    partner = {"tp": chip * 2 + (1 - core)}
    across = {"tp": (1 - chip) * 2 + core}

    def start(g, kinds):
        slot = lax.rem(g, RING)

        def when(kind, cond):
            if kind not in kinds:
                return lambda act: None
            return (lambda act: act()) if len(kinds) == 1 else pl.when(cond)

        sem = wsem.at[slot]
        in_a = g < all_a
        a, m = lax.rem(g, na), lax.rem(g + (nm - all_a % nm), nm)

        @when(Q, in_a & (a < nq))
        def _():
            pltpu.make_async_copy(wq.at[:, pl.ds(pl.multiple_of(a * NB, NB), NB)], slots.at[slot], sem).start()

        @when(KV, in_a & (a == nq))
        def _():
            pltpu.make_async_copy(wk, slots.at[slot, :, pl.ds(0, kcols)], sem).start()
            pltpu.make_async_copy(wv, slots.at[slot, :, pl.ds(kcols, kcols)], sem).start()

        @when(O, in_a & (a > nq))
        def _():
            for k in range(per):
                at = pl.multiple_of(((a - nq - 1) * per + k) * NB, NB)
                pltpu.make_async_copy(wo.at[:, pl.ds(at, NB)], slots.at[slot, pl.ds(k * qcols, qcols), :], sem).start()

        in_m = jnp.logical_not(in_a) & (g < total)

        @when(GU, in_m & (m < ngu))
        def _():
            at = pl.multiple_of(m * FB, FB)
            pltpu.make_async_copy(wg.at[:, pl.ds(at, FB)], slots.at[slot, :, pl.ds(0, FB)], sem).start()
            pltpu.make_async_copy(wu.at[:, pl.ds(at, FB)], slots.at[slot, :, pl.ds(FB, FB)], sem).start()

        if tail:

            @when(REST, in_m & (m == ngu))
            def _():
                pltpu.make_async_copy(wg.at[:, pl.ds(ngu * FB, tail)], slots.at[slot, :, pl.ds(0, tail)], sem).start()
                pltpu.make_async_copy(wu.at[:, pl.ds(ngu * FB, tail)], slots.at[slot, :, pl.ds(tail, tail)], sem).start()

        @when(DOWN, in_m & (m >= first_d))
        def _():
            at = pl.multiple_of((m - first_d) * NB, NB)
            pltpu.make_async_copy(wd.at[:, pl.ds(at, NB)], slots.at[slot, pl.ds(0, ff), :], sem).start()

    def ready(g, kinds, rows=None, cols=NB):
        slot = lax.rem(g, RING)
        rows = depth if rows is None else rows
        where = slots.at[slot, pl.ds(0, rows), pl.ds(0, cols)]
        pltpu.make_async_copy(where, where, wsem.at[slot]).wait()
        start(g + RING - 1, kinds)
        return slot

    class Sum:
        def __init__(self, ar, which, row0, n):
            self.ar, self.which, self.row0, self.n = ar, which, row0, n

        def far(self, j, at, n, sem):
            rows = pl.ds(pl.multiple_of(self.row0 + at, PIECE), n)
            return pltpu.make_async_remote_copy(q_all.at[self.which, j, rows, :], r_all.at[self.which, j, rows, :], xs_sem.at[self.ar], sem,
                                                device_id=across, device_id_type=MESH)

        def crossed(self, j):
            return self.far(j, 0, self.n, xr_sem.at[self.ar, j])

        def head(self, j):
            return self.far(j, 0, PIECE, xh_sem.at[j])

        def rest(self, j):
            return self.far(j, PIECE, self.n - PIECE, xr_sem.at[self.ar, j])

        def cross(self, j):
            if self.which:
                self.crossed(j).start()
            else:

                @pl.when(self.ar == EARLY)
                def _():
                    self.head(j).start()

                @pl.when(self.ar != EARLY)
                def _():
                    self.crossed(j).start()

        def each(self, act):
            def one(j, _):
                act(j)
                return 0

            lax.fori_loop(0, nj, one, 0)

        def sent(self):
            whole = q_all.at[self.which, :, pl.ds(pl.multiple_of(self.row0, PIECE), self.n), :]
            pltpu.make_async_copy(whole, whole, xs_sem.at[self.ar]).wait()

        def kept(self, j):
            at = lax.rem(j, STG)
            rows = pl.ds(pl.multiple_of(self.row0, PIECE), self.n)
            return pltpu.make_async_copy(stg.at[at, pl.ds(0, self.n), :], q_all.at[self.which, j, rows, :], st_sem.at[at])

        def shared(self, j):
            i = self.ar * nj + j
            near, far = lax.rem(i, OWN), lax.rem(i, FAR)
            return pltpu.make_async_remote_copy(snd.at[near, pl.ds(0, self.n), :], rcv.at[far, pl.ds(0, self.n), :], rs_send.at[near],
                                                rs_recv.at[far], device_id=partner, device_id_type=MESH)

        def of_chip(self, j):
            i = self.ar * nj + j
            return (own[lax.rem(i, OWN), : self.n] + rcv[lax.rem(i, FAR), : self.n].astype(F32)).astype(BF16)

        def keep_term(self, j, t):
            i = self.ar * nj + j
            snd[lax.rem(i, OWN), : self.n] = t[: self.n].astype(BF16)
            own[lax.rem(i, OWN), : self.n] = t[self.n :]

    def sum_a(c):
        return Sum(c, 0, c * half, half)

    def sum_m(m):
        return Sum(seqs + m, 1, m * big, big)

    final = Sum(jnp.int32(last), 1, (seqs - 1) * big, small)

    def block(s, j, term, *sides):
        @pl.when(j >= LAG)
        def _():
            s.shared(j - LAG).wait_recv()

        @pl.when(j >= OWN)
        def _():
            s.shared(j - OWN).wait_send()

        for side in sides:
            side.before(j)
        for side in sides:
            side.work(j)
        stg[lax.rem(j + 12 - LAG, STG), : s.n] = s.of_chip(j + 12 - LAG)
        s.keep_term(j, term())

        @pl.when(j > LAG)
        def _():
            s.kept(j - LAG - 1).wait()
            s.cross(j - LAG - 1)

        @pl.when(j >= LAG)
        def _():
            s.kept(j - LAG).start()

        s.shared(j).start()
        for side in sides:
            side.after(j)

    def drain(s):
        for j in range(nj - LAG, nj):
            s.shared(jnp.int32(j)).wait_recv()
            stg[j % STG, : s.n] = s.of_chip(jnp.int32(j))
            s.kept(jnp.int32(j)).start()

    def drained(s):
        for j in range(nj - LAG - 1, nj):
            s.kept(jnp.int32(j)).wait()
            s.cross(jnp.int32(j))
        for j in range(nj - OWN, nj):
            s.shared(jnp.int32(j)).wait_send()
        if not s.which:

            @pl.when(s.ar == EARLY)
            def _():
                s.each(lambda j: s.rest(j).start())

    def block_cols(j):
        return pl.ds(pl.multiple_of(j * NB, NB), NB)

    def crossed_last(j):
        return pltpu.make_async_remote_copy(lhs.at[pl.ds(0, small), block_cols(j)], lhs.at[pl.ds(small, small), block_cols(j)],
                                            xs_sem.at[last], xr_sem.at[last, j], device_id=across, device_id_type=MESH)

    def finish_last(j):
        final.shared(j).wait_recv()
        lhs[:small, block_cols(j)] = final.of_chip(j)
        crossed_last(j).start()

    def block_last(j, term, side):
        side.beside(j)

        @pl.when(j >= 1)
        def _():
            finish_last(j - 1)

        @pl.when(j >= OWN)
        def _():
            final.shared(j - OWN).wait_send()

        final.keep_term(j, term())
        final.shared(j).start()

    def exchanged(n):
        pltpu.make_async_remote_copy(lhs.at[pl.ds(n, n), :], lhs.at[pl.ds(0, n), :], l_send, l_recv,
                                     device_id=partner, device_id_type=MESH).wait()

    def free():
        pl.semaphore_signal(l_free, inc=1, device_id=partner, device_id_type=MESH)

    def scaled(rows, which, part):
        squares = jnp.zeros((PIECE, NB), F32)
        for j in range(nj):
            v = part(j, True)
            squares += v * v
        scale = lax.rsqrt(jnp.sum(squares, axis=1, keepdims=True) * (1 / depth) + 1e-6)
        for j in range(nj):
            cols = slice(j * NB, (j + 1) * NB)
            lhs[rows, cols] = (part(j, False) * scale * gains[pl.ds(which, 1), cols]).astype(BF16)

    class Operand:
        def __init__(self, piece0, pieces, base, second):
            self.piece0, self.pieces, self.base, self.second = piece0, pieces, base, second

        def here(self, p):
            return pl.ds(pl.multiple_of((self.piece0 + p) * PIECE, PIECE), PIECE)

        def loads(self, p):
            at, i = lax.rem(p, AHEAD), self.piece0 + p
            row = lax.div(i, np_) * tokens + core * half + lax.rem(i, np_) * PIECE
            return (pltpu.make_async_copy(x.at[pl.ds(pl.multiple_of(row, PIECE), PIECE), :], xin.at[at], in_sem.at[at, 0]),
                    pltpu.make_async_copy(q_all.at[0, :, self.here(p), :], qin.at[at], in_sem.at[at, 1]),
                    pltpu.make_async_copy(r_all.at[0, :, self.here(p), :], rin.at[at], in_sem.at[at, 2]))[: 3 if self.second else 1]

        def put(self, p):
            at = lax.rem(p, 2)
            return pltpu.make_async_copy(hst.at[at], h_all.at[:, self.here(p), :], h_sem.at[at])

        def give(self, p):
            here = pl.ds(pl.multiple_of(self.base + p * PIECE, PIECE), PIECE)
            there = pl.ds(pl.multiple_of(p * PIECE, PIECE), PIECE)
            return pltpu.make_async_remote_copy(lhs.at[here, :], lhs.at[there, :], l_send, l_recv, device_id=partner, device_id_type=MESH)

        def begin(self):
            for p in range(AHEAD - 1):
                for copy in self.loads(jnp.int32(p)):
                    copy.start()
            pl.semaphore_wait(l_free, 1)

        def before(self, p):
            @pl.when(p + AHEAD - 1 < self.pieces)
            def _():
                for copy in self.loads(p + AHEAD - 1):
                    copy.start()

            for copy in self.loads(p):
                copy.wait()

            @_if(_and(p >= 2, self.second))
            def _():
                self.put(p - 2).wait()

            @pl.when(p >= 1)
            def _():
                self.give(p - 1).start()

        def work(self, p):
            at, to = lax.rem(p, AHEAD), lax.rem(p, 2)
            rows = pl.ds(pl.multiple_of(self.base + p * PIECE, PIECE), PIECE)

            def plain(j, new):
                return xin[at, :, j * NB : (j + 1) * NB].astype(F32)

            def part(j, new):
                if new:
                    v = xin[at, :, j * NB : (j + 1) * NB].astype(F32) + (qin[at, j].astype(F32) + rin[at, j].astype(F32))
                    hst[to, j] = v.astype(BF16)
                return hst[to, j].astype(F32)

            scaled(rows, int(self.second), part if self.second else plain)

        def after(self, p):
            if self.second:
                self.put(p).start()

        def last(self):
            self.give(jnp.int32(self.pieces - 1)).start()

        def end(self):
            if self.second:
                for p in (2, 1):
                    self.put(jnp.int32(self.pieces - p)).wait()

    def with_operand(side, step):
        side.begin()
        lax.fori_loop(0, side.pieces, lambda j, _: step(j, side), 0)
        side.last()
        lax.fori_loop(side.pieces, nj, lambda j, _: step(j), 0)
        side.end()

    def have(s, what):
        s.each(lambda j: what(j).wait_recv())

    early = pl.multiple_of((1 - core) * half, half)
    late = pl.multiple_of(core * half, half)

    def turned(t):
        t = t.astype(F32)
        r = pltpu.roll(t, HEAD // 2, 1)
        out = []
        for rows, place in ((slice(0, half), (1 - core) * half), (slice(half, tokens), core * half)):
            place = pl.ds(pl.multiple_of(place, half), half)
            out.append((t[rows] * cos[place, :] + r[rows] * sin[place, :]).astype(BF16))
        return jnp.concatenate(out, 0)

    def turn(s):
        for n in range(NB // HEAD):
            cols = pl.ds(pl.multiple_of(s * NB + n * HEAD, HEAD), HEAD)
            qs[:, cols] = turned(qs[:, cols])

    def attention():
        e = HEAD**-0.5 * LOG2E
        for n in range(kcols // HEAD):
            vx[n, :, :HEAD] = kvs[:, kcols + n * HEAD : kcols + (n + 1) * HEAD]
            vx[n, :, HEAD:] = jnp.ones((tokens, HEAD), BF16)
        seen = lax.broadcasted_iota(jnp.int32, (QB, QB), 1) <= lax.broadcasted_iota(jnp.int32, (QB, QB), 0)
        many = min(HEADS, group)

        def rows(b):
            at = b * QB
            return pl.ds(pl.multiple_of(early + at if at < half else late + at - half, QB), QB)

        def some(i, _):
            n = lax.div(i * many, group)
            kc = pl.ds(pl.multiple_of(n * HEAD, HEAD), HEAD)
            cols = [pl.ds(pl.multiple_of((i * many + t) * HEAD, HEAD), HEAD) for t in range(many)]
            keys = [kvs[rows(b), kc] for b in range(tokens // QB)]
            values = [vx[n, rows(b), :] for b in range(tokens // QB)]
            for b in range(tokens // QB):
                q = jnp.concatenate([qs[rows(b), c] for c in cols], 0)
                scores = _dot(q, jnp.concatenate(keys[: b + 1], 0), 1, 1)
                weights = []
                for t in range(many):
                    of = scores[t * QB : (t + 1) * QB]
                    parts = [of[:, u * QB : (u + 1) * QB] for u in range(b)] + [jnp.where(seen, of[:, b * QB :], HIDDEN)]
                    top = functools.reduce(jnp.maximum, parts).max(axis=1, keepdims=True)
                    weights.append(jnp.concatenate([jnp.exp2((u - top) * e).astype(BF16) for u in parts], 1))
                o = _dot(jnp.concatenate(weights, 0), jnp.concatenate(values[: b + 1], 0))
                for t, c in enumerate(cols):
                    of = o[t * QB : (t + 1) * QB]
                    hid[rows(b), c] = (of[:, :HEAD] / of[:, HEAD:]).astype(BF16)
            return 0

        lax.fori_loop(0, heads // many, some, 0)

    def first(c, _):
        g0 = c * na

        def queries(s, _):
            slot = ready(g0 + s, (Q, KV, O))
            turn(jnp.maximum(s - 1, 0))
            qs[:, pl.ds(pl.multiple_of(s * NB, NB), NB)] = _dot(lhs[:tokens], slots[slot]).astype(BF16)

            @pl.when((c >= 1) & (s == min(1, nq - 1)))
            def _():
                drain(sum_a(c - 1))

            return 0

        lax.fori_loop(0, nq, queries, 0)

        slot = ready(g0 + nq, (O,) if nwo > 1 else (O, Q, GU))
        turn(nq - 1)
        t = _dot(lhs[:tokens], slots[slot, :, : 2 * kcols])
        for n in range(kcols // HEAD):
            cols = slice(n * HEAD, (n + 1) * HEAD)
            kvs[:, cols] = turned(t[:, cols].astype(BF16))
        kvs[:, kcols:] = t[:, kcols:].astype(BF16)
        free()

        @pl.when(c >= 1)
        def _():
            drained(sum_a(c - 1))

        attention()

        def project(j, *sides):
            k = lax.rem(j, per)
            g = g0 + nq + 1 + lax.div(j, per)

            @pl.when(k == 0)
            def _():
                ready(g, (O, Q, KV, GU, DOWN))

            w = slots.at[lax.rem(g, RING), pl.ds(pl.multiple_of(k * qcols, qcols), qcols), :]
            block(sum_a(c), j, lambda: _dot(hid[:tokens, :qcols], w[...]), *sides)
            return 0

        @pl.when(c + 1 < seqs)
        def _():
            with_operand(Operand((c + 1) * np_, np_, half, False), project)
            exchanged(half)

        @pl.when(c + 1 == seqs)
        def _():
            s = sum_a(jnp.int32(0))
            have(s, s.crossed)
            s.sent()
            s = sum_a(jnp.int32(EARLY))
            have(s, s.head)
            with_operand(Operand(jnp.int32(0), big // PIECE, big, True), project)
            exchanged(big)

        return 0

    def puts(c, j, t):
        at = lax.rem(t, YB)
        where = y.at[pl.ds(pl.multiple_of(c * tokens + core * half, half), half), block_cols(j)]
        return (pltpu.make_async_copy(yout.at[at], where, yl_sem.at[at]),
                pltpu.make_async_remote_copy(yout.at[at], where, ys_sem.at[at], yr_sem.at[c], device_id=partner, device_id_type=MESH))

    class Results:
        def __init__(self):
            self.count = seqs - 1

        def of(self, t):
            return lax.rem(t, self.count), lax.div(t, self.count)

        def loads(self, t):
            c, j = self.of(t)
            at = lax.rem(t, YB)
            rows = pl.ds(pl.multiple_of(c * half, half), half)
            return [pltpu.make_async_copy(src, yin.at[at, i], yin_sem.at[at, i])
                    for i, src in enumerate((h_all.at[j, rows, :], q_all.at[1, j, rows, :], r_all.at[1, j, rows, :]))]

        def fetch(self, t):
            c, j = self.of(t)
            sum_m(c).crossed(j).wait_recv()
            for copy in self.loads(t):
                copy.start()

        def begin(self):
            for t in range(YB - 1):
                self.fetch(jnp.int32(t))

        def left(self, t):
            near, far = puts(*self.of(t), t)
            near.wait()
            far.wait_send()

        def item(self, t):
            at = lax.rem(t, YB)

            @pl.when(t + YB - 1 < self.count * nj)
            def _():
                self.fetch(t + YB - 1)

            for copy in self.loads(t):
                copy.wait()

            @pl.when(t >= YB)
            def _():
                self.left(t - YB)

            yout[at] = (yin[at, 0].astype(F32) + (yin[at, 1].astype(F32) + yin[at, 2].astype(F32))).astype(BF16)
            for copy in puts(*self.of(t), t):
                copy.start()

        def beside(self, j):
            for k in range(self.count):
                self.item(j * self.count + k)

        def end(self):
            for t in range(self.count * nj - YB, self.count * nj):
                self.left(jnp.int32(t))
            for c in range(self.count):
                sum_m(jnp.int32(c)).sent()

    def gated(gate, up):
        return (gate * jax.nn.sigmoid(gate) * up).astype(BF16)

    def second(m, n):
        g0 = all_a + m * nm

        def before(act):
            if n == small:
                act(sum_m(m - 1))
            else:

                @pl.when(m == 0)
                def _():
                    act(sum_a(jnp.int32(seqs - 1)))

                @pl.when(m > 0)
                def _():
                    act(sum_m(m - 1))

        def gates(s, _):
            slot = ready(g0 + s, (GU, REST, DOWN))
            t = _dot(lhs[: 2 * n], slots[slot])
            hid[: 2 * n, pl.ds(pl.multiple_of(s * FB, FB), FB)] = gated(t[:, :FB], t[:, FB:])

            @pl.when(s == 1)
            def _():
                before(drain)

            @pl.when(s == 3)
            def _():
                before(drained)

            return 0

        lax.fori_loop(0, ngu, gates, 0)
        if tail:
            slot = ready(g0 + ngu, (DOWN,), None, 2 * tail)
            t = _dot(lhs[: 2 * n], slots[slot, :, : 2 * tail])
            hid[: 2 * n, ngu * FB :] = gated(t[:, :tail], t[:, tail:])

        def down(j):
            slot = ready(g0 + first_d + j, (GU, DOWN), ff)
            return lambda: _dot(hid[: 2 * n], slots[slot, :ff, :])

        return down

    def share(m, _):
        down = second(m, big)
        free()

        @pl.when(m == 0)
        def _():
            s = sum_a(jnp.int32(EARLY))
            have(s, s.rest)
            s.sent()

        @pl.when(m + 2 < seqs)
        def _():
            s = sum_a(m + 2)
            have(s, s.crossed)
            s.sent()

        def step(j, *sides):
            block(sum_m(m), j, down(j), *sides)
            return 0

        ends = m == seqs - 2
        next_n = jnp.where(ends, small, big)
        with_operand(Operand((m + 1) * (big // PIECE), lax.div(next_n, PIECE), next_n, True), step)

        @pl.when(ends)
        def _():
            exchanged(small)

        @pl.when(jnp.logical_not(ends))
        def _():
            exchanged(big)

        return 0

    def last_share():
        down = second(seqs - 1, small)
        pl.semaphore_signal(x_free, inc=1, device_id=across, device_id_type=MESH)
        pl.semaphore_wait(x_free, 1)
        done = Results()
        done.begin()

        def step(j, _):
            block_last(j, down(j), done)
            return 0

        lax.fori_loop(0, nj, step, 0)
        finish_last(jnp.int32(nj - 1))
        for j in range(nj - OWN, nj):
            final.shared(jnp.int32(j)).wait_send()
        done.end()

    def fetched(p):
        owner = jnp.where(p < np_, 1 - core, core)
        rows = pl.ds(pl.multiple_of(owner * half + lax.rem(p, np_) * PIECE, PIECE), PIECE)
        return pltpu.make_async_copy(x.at[rows, :], lhs.at[pl.ds(pl.multiple_of(p * PIECE, PIECE), PIECE), :], first_sem.at[p])

    tables = [pltpu.make_async_copy(src, dst, table_sem.at[i]) for i, (src, dst) in
              enumerate(((gain_a, gain_in.at[0]), (gain_m, gain_in.at[1]), (cos_in, cos), (sin_in, sin)))]
    for p in range(2 * np_):
        fetched(jnp.int32(p)).start()
    for copy in tables:
        copy.start()
    barrier = pltpu.get_barrier_semaphore()
    for peer in (partner, across):
        pl.semaphore_signal(barrier, inc=1, device_id=peer, device_id_type=MESH)
    for i in range(2):
        tables[i].wait()
        wide = gain_in[i].astype(F32)
        for r in range(depth // LANES):
            gains[i : i + 1, r * LANES : (r + 1) * LANES] = wide[r : r + 1]

    def normed(p, _):
        rows = pl.ds(pl.multiple_of(p * PIECE, PIECE), PIECE)
        fetched(p).wait()
        scaled(rows, 0, lambda j, new: lhs[rows, j * NB : (j + 1) * NB].astype(F32))

        for g in range(RING - 1):

            @pl.when(p == 3 + 4 * g)
            def _():
                start(jnp.int32(g), (Q, KV))

        return 0

    lax.fori_loop(0, 2 * np_, normed, 0)
    pl.semaphore_wait(barrier, 2)
    for copy in tables[2:]:
        copy.wait()
    lax.fori_loop(0, seqs, first, 0)
    lax.fori_loop(0, seqs - 1, share, 0)
    last_share()

    def left(j):
        near, far = puts(seqs - 1, j, j)
        near.wait()
        far.wait_send()

    over = (seqs - 1) * (big - half)

    def blocks(j):
        at, row0 = lax.rem(j, YB), (seqs - 1) * half
        return [pltpu.make_async_copy(src.at[j, pl.ds(row0, n), :], yin.at[at, i, pl.ds(0, n), :], yin_sem.at[at, i])
                for i, (src, n) in enumerate(((h_all, half), (q_all.at[1], over), (r_all.at[1], over)))]

    for j in range(YB - 1):
        for copy in blocks(jnp.int32(j)):
            copy.start()

    def piece(j, _):
        at = lax.rem(j, YB)

        @pl.when(j + YB - 1 < nj)
        def _():
            for copy in blocks(j + YB - 1):
                copy.start()

        @pl.when(j >= YB)
        def _():
            left(j - YB)

        for copy in blocks(j):
            copy.wait()
        crossed_last(j).wait_recv()
        here, there = lhs[:small, block_cols(j)].astype(F32), lhs[small : 2 * small, block_cols(j)].astype(F32)
        yout[at, :over] = (yin[at, 0, :over].astype(F32) + (yin[at, 1, :over].astype(F32) + yin[at, 2, :over].astype(F32))).astype(BF16)
        yout[at, over:] = (yin[at, 0, over:].astype(F32) + (here + there)).astype(BF16)
        for copy in puts(seqs - 1, j, j):
            copy.start()
        return 0

    lax.fori_loop(0, nj, piece, 0)
    for j in range(nj - YB, nj):
        left(jnp.int32(j))
    final.sent()

    def arrived(c, _):
        where = y.at[pl.ds(pl.multiple_of(c * tokens + (1 - core) * half, half), half), :]
        pltpu.make_async_copy(where, where, yr_sem.at[c]).wait()
        return 0

    lax.fori_loop(0, seqs, arrived, 0)


def layer(x, gain_a, wq, wk, wv, wo, gain_m, w_gate, w_up, w_down):
    seqs, tokens, depth = x.shape
    half, nj = tokens // 2, depth // NB
    big, _ = _shares(seqs, half)
    i = np.arange(HEAD // 2, dtype=np.float32)
    angle = np.arange(tokens, dtype=np.float32)[:, None] * np.float32(THETA) ** (-i / np.float32(HEAD // 2))
    cos, sin = np.cos(angle), np.sin(angle)
    cos, sin = np.concatenate([cos, cos], 1).astype(np.float32), np.concatenate([-sin, sin], 1).astype(np.float32)
    hbm = pl.BlockSpec(memory_space=pl.ANY)
    dma, regular = pltpu.SemaphoreType.DMA, pltpu.SemaphoreType.REGULAR
    out = [
        jax.ShapeDtypeStruct((seqs * tokens, depth), BF16),
        jax.ShapeDtypeStruct((nj, seqs * half, NB), BF16),
        jax.ShapeDtypeStruct((2, nj, seqs * half, NB), BF16),
        jax.ShapeDtypeStruct((2, nj, seqs * half, NB), BF16),
    ]
    kv = wk.shape[1]
    scratch = [
        pltpu.VMEM((2 * big, depth), BF16),
        pltpu.VMEM((RING, depth, NB), BF16),
        pltpu.VMEM((tokens, wq.shape[1]), BF16),
        pltpu.VMEM((tokens, 2 * kv), BF16),
        pltpu.VMEM((kv // HEAD, tokens, 2 * HEAD), BF16),
        pltpu.VMEM((2 * big, w_down.shape[0]), BF16),
        pltpu.VMEM((OWN, big, NB), F32),
        pltpu.VMEM((OWN, big, NB), BF16),
        pltpu.VMEM((FAR, big, NB), BF16),
        pltpu.VMEM((STG, big, NB), BF16),
        pltpu.VMEM((AHEAD, PIECE, depth), BF16),
        pltpu.VMEM((AHEAD, nj, PIECE, NB), BF16),
        pltpu.VMEM((AHEAD, nj, PIECE, NB), BF16),
        pltpu.VMEM((2, nj, PIECE, NB), BF16),
        pltpu.VMEM((YB, 3, half, NB), BF16),
        pltpu.VMEM((YB, half, NB), BF16),
        pltpu.VMEM((tokens, HEAD), F32),
        pltpu.VMEM((tokens, HEAD), F32),
        pltpu.VMEM((2, depth // LANES, LANES), BF16),
        pltpu.VMEM((2, depth), F32),
        dma((RING,)), dma((OWN,)), dma((FAR,)), dma((STG,)), dma((2 * seqs,)), dma((2 * seqs, nj)),
        dma, dma, regular, regular,
        dma((AHEAD, 3)), dma((2,)), dma((YB, 3)), dma((YB,)), dma((YB,)), dma((seqs,)),
        dma((tokens // PIECE,)), dma((4,)), dma((nj,)),
    ]
    y, *_ = pl.pallas_call(
        functools.partial(layer_kernel, seqs=seqs),
        out_shape=out,
        in_specs=[hbm] * 12,
        out_specs=[hbm] * 4,
        scratch_shapes=scratch,
        compiler_params=pltpu.CompilerParams(collective_id=0, has_side_effects=True, vmem_limit_bytes=67043328),
        name="layer",
    )(x.reshape(seqs * tokens, depth), wq, wk, wv, wo, w_gate, w_up, w_down, cos, sin,
      gain_a.reshape(-1, LANES), gain_m.reshape(-1, LANES))
    return y.reshape(x.shape)


def solution(mesh):
    def step(*args):
        return layer(*args)

    tokens, whole, columns, rows_of = P("dp", None, None), P(None), P(None, "tp"), P("tp", None)
    return jax.shard_map(
        step,
        mesh=mesh,
        in_specs=(tokens, whole, columns, columns, columns, rows_of, whole, columns, columns, rows_of),
        out_specs=tokens,
        check_vma=False,
    )
```

```python
import functools

import jax
import jax.numpy as jnp
import numpy as np
from jax import lax
from jax.experimental import pallas as pl
from jax.experimental.pallas import tpu as pltpu
from jax.sharding import PartitionSpec as P

HEAD = 128
THETA = 10000
LOG2E = 1.4426950408889634
HIDDEN = -2e30
MESH = pl.DeviceIdType.MESH
NB = 512
FB = 256
NEXT = 3
EARLY = 1
RING = 3
Q, KV, O, GU, REST, DOWN = range(6)
LANES = 128
PIECE = 32
AHEAD = 4
LAG = 3
OWN, FAR = LAG + 1, 2 * LAG
STG = 4
YB = 4
QB = 128
HEADS = 8
F32, BF16 = jnp.float32, jnp.bfloat16


def _dot(a, b, ca=1, cb=0):
    return lax.dot_general(a, b, (((ca,), (cb,)), ((), ())), preferred_element_type=F32)


def _if(cond):
    if isinstance(cond, bool):
        return (lambda act: act()) if cond else (lambda act: None)
    return pl.when(cond)


def _and(*conds):
    known = [c for c in conds if isinstance(c, bool)]
    rest = [c for c in conds if not isinstance(c, bool)]
    return functools.reduce(jnp.logical_and, rest) if all(known) and rest else all(known)


def _shares(seqs, half):
    big = half + PIECE
    return big, seqs * half - (seqs - 1) * big


def layer_kernel(
    x, wq, wk, wv, wo, wg, wu, wd, cos_in, sin_in, gain_a, gain_m,
    y, h_all, q_all, r_all,
    lhs, slots, qs, kvs, vx, hid, own, snd, rcv, stg, xin, qin, rin, hst, yin, yout, cos, sin, gain_in, gains,
    wsem, rs_send, rs_recv, st_sem, xs_sem, xr_sem, l_send, l_recv, l_free, x_free, in_sem, h_sem, yin_sem, yl_sem, ys_sem, yr_sem,
    first_sem, table_sem, xh_sem, xl_sem,
    *, seqs,
):
    tokens, depth = qs.shape[0], x.shape[1]
    half = tokens // 2
    big, small = _shares(seqs, half)
    qcols, kcols, ff = wq.shape[1], wk.shape[1], wd.shape[0]
    nj = depth // NB
    nq = qcols // NB
    per = depth // qcols
    nwo = nj // per
    na = nq + 1 + nwo
    ngu = ff // FB
    tail = ff - ngu * FB
    nm = ngu + (1 if tail else 0) + nj
    first_d = nm - nj
    all_a = seqs * na
    total = all_a + seqs * nm
    heads = qcols // HEAD
    group = heads // (kcols // HEAD)
    np_ = half // PIECE
    last = 2 * seqs - 1

    me = lax.axis_index("tp")
    core, chip = lax.rem(me, 2), lax.div(me, 2)
    partner = {"tp": chip * 2 + (1 - core)}
    across = {"tp": (1 - chip) * 2 + core}

    def start(g, kinds):
        slot = lax.rem(g, RING)

        def when(kind, cond):
            if kind not in kinds:
                return lambda act: None
            return (lambda act: act()) if len(kinds) == 1 else pl.when(cond)

        sem = wsem.at[slot]
        in_a = g < all_a
        a, m = lax.rem(g, na), lax.rem(g + (nm - all_a % nm), nm)

        @when(Q, in_a & (a < nq))
        def _():
            pltpu.make_async_copy(wq.at[:, pl.ds(pl.multiple_of(a * NB, NB), NB)], slots.at[slot], sem).start()

        @when(KV, in_a & (a == nq))
        def _():
            pltpu.make_async_copy(wk, slots.at[slot, :, pl.ds(0, kcols)], sem).start()
            pltpu.make_async_copy(wv, slots.at[slot, :, pl.ds(kcols, kcols)], sem).start()

        @when(O, in_a & (a > nq))
        def _():
            for k in range(per):
                at = pl.multiple_of(((a - nq - 1) * per + k) * NB, NB)
                pltpu.make_async_copy(wo.at[:, pl.ds(at, NB)], slots.at[slot, pl.ds(k * qcols, qcols), :], sem).start()

        in_m = jnp.logical_not(in_a) & (g < total)

        @when(GU, in_m & (m < ngu))
        def _():
            at = pl.multiple_of(m * FB, FB)
            pltpu.make_async_copy(wg.at[:, pl.ds(at, FB)], slots.at[slot, :, pl.ds(0, FB)], sem).start()
            pltpu.make_async_copy(wu.at[:, pl.ds(at, FB)], slots.at[slot, :, pl.ds(FB, FB)], sem).start()

        if tail:

            @when(REST, in_m & (m == ngu))
            def _():
                pltpu.make_async_copy(wg.at[:, pl.ds(ngu * FB, tail)], slots.at[slot, :, pl.ds(0, tail)], sem).start()
                pltpu.make_async_copy(wu.at[:, pl.ds(ngu * FB, tail)], slots.at[slot, :, pl.ds(tail, tail)], sem).start()

        @when(DOWN, in_m & (m >= first_d))
        def _():
            at = pl.multiple_of((m - first_d) * NB, NB)
            pltpu.make_async_copy(wd.at[:, pl.ds(at, NB)], slots.at[slot, pl.ds(0, ff), :], sem).start()

    def ready(g, kinds, rows=None, cols=NB):
        slot = lax.rem(g, RING)
        rows = depth if rows is None else rows
        where = slots.at[slot, pl.ds(0, rows), pl.ds(0, cols)]
        pltpu.make_async_copy(where, where, wsem.at[slot]).wait()
        start(g + RING - 1, kinds)
        return slot

    class Sum:
        def __init__(self, ar, which, row0, n):
            self.ar, self.which, self.row0, self.n = ar, which, row0, n

        def far(self, j, at, n, sem):
            rows = pl.ds(pl.multiple_of(self.row0 + at, PIECE), n)
            return pltpu.make_async_remote_copy(q_all.at[self.which, j, rows, :], r_all.at[self.which, j, rows, :], xs_sem.at[self.ar], sem,
                                                device_id=across, device_id_type=MESH)

        def crossed(self, j):
            return self.far(j, 0, self.n, xr_sem.at[self.ar])

        def head(self, j):
            return self.far(j, 0, PIECE, xh_sem)

        def rest(self, j):
            return self.far(j, PIECE, self.n - PIECE, xr_sem.at[self.ar])

        def cross(self, j):
            if self.which:
                self.crossed(j).start()
            else:

                @pl.when(self.ar == EARLY)
                def _():
                    self.head(j).start()

                @pl.when(self.ar != EARLY)
                def _():
                    self.crossed(j).start()

        def each(self, act):
            def one(j, _):
                act(j)
                return 0

            lax.fori_loop(0, nj, one, 0)

        def all_blocks(self, sem, at=0, n=None):
            rows = pl.ds(pl.multiple_of(self.row0 + at, PIECE), n or self.n)
            whole = r_all.at[self.which, :, rows, :]
            pltpu.make_async_copy(whole, whole, sem).wait()

        def sent(self):
            self.all_blocks(xs_sem.at[self.ar])

        def have(self):
            self.all_blocks(xr_sem.at[self.ar])

        def have_head(self):
            self.all_blocks(xh_sem, 0, PIECE)

        def have_rest(self):
            self.all_blocks(xr_sem.at[self.ar], PIECE, self.n - PIECE)

        def kept(self, j):
            at = lax.rem(j, STG)
            rows = pl.ds(pl.multiple_of(self.row0, PIECE), self.n)
            return pltpu.make_async_copy(stg.at[at, pl.ds(0, self.n), :], q_all.at[self.which, j, rows, :], st_sem.at[at])

        def shared(self, j):
            i = self.ar * nj + j
            near, far = lax.rem(i, OWN), lax.rem(i, FAR)
            return pltpu.make_async_remote_copy(snd.at[near, pl.ds(0, self.n), :], rcv.at[far, pl.ds(0, self.n), :], rs_send.at[near],
                                                rs_recv.at[far], device_id=partner, device_id_type=MESH)

        def of_chip(self, j):
            i = self.ar * nj + j
            return (own[lax.rem(i, OWN), : self.n] + rcv[lax.rem(i, FAR), : self.n].astype(F32)).astype(BF16)

        def keep_term(self, j, t):
            i = self.ar * nj + j
            snd[lax.rem(i, OWN), : self.n] = t[: self.n].astype(BF16)
            own[lax.rem(i, OWN), : self.n] = t[self.n :]

    def sum_a(c):
        return Sum(c, 0, c * half, half)

    def sum_m(m):
        return Sum(seqs + m, 1, m * big, big)

    final = Sum(jnp.int32(last), 1, (seqs - 1) * big, small)

    def block(s, j, term, *sides):
        @pl.when(j >= LAG)
        def _():
            s.shared(j - LAG).wait_recv()

        @pl.when(j >= OWN)
        def _():
            s.shared(j - OWN).wait_send()

        for side in sides:
            side.before(j)
        for side in sides:
            side.work(j)
        stg[lax.rem(j + 12 - LAG, STG), : s.n] = s.of_chip(j + 12 - LAG)
        s.keep_term(j, term())

        @pl.when(j > LAG)
        def _():
            s.kept(j - LAG - 1).wait()
            s.cross(j - LAG - 1)

        @pl.when(j >= LAG)
        def _():
            s.kept(j - LAG).start()

        s.shared(j).start()
        for side in sides:
            side.after(j)

    def drain(s):
        for j in range(nj - LAG, nj):
            s.shared(jnp.int32(j)).wait_recv()
            stg[j % STG, : s.n] = s.of_chip(jnp.int32(j))
            s.kept(jnp.int32(j)).start()

    def drained(s):
        for j in range(nj - LAG - 1, nj):
            s.kept(jnp.int32(j)).wait()
            s.cross(jnp.int32(j))
        for j in range(nj - OWN, nj):
            s.shared(jnp.int32(j)).wait_send()
        if not s.which:

            @pl.when(s.ar == EARLY)
            def _():
                s.each(lambda j: s.rest(j).start())

    def block_cols(j):
        return pl.ds(pl.multiple_of(j * NB, NB), NB)

    def crossed_last(j):
        return pltpu.make_async_remote_copy(lhs.at[pl.ds(0, small), block_cols(j)], lhs.at[pl.ds(small, small), block_cols(j)],
                                            xs_sem.at[last], xl_sem.at[j], device_id=across, device_id_type=MESH)

    def finish_last(j):
        final.shared(j).wait_recv()
        lhs[:small, block_cols(j)] = final.of_chip(j)
        crossed_last(j).start()

    def block_last(j, term, side):
        side.beside(j)

        @pl.when(j == 1)
        def _():
            pl.semaphore_wait(x_free, 1)

        @pl.when(j >= 1)
        def _():
            finish_last(j - 1)

        @pl.when(j >= OWN)
        def _():
            final.shared(j - OWN).wait_send()

        final.keep_term(j, term())
        final.shared(j).start()

    def exchanged(n):
        pltpu.make_async_remote_copy(lhs.at[pl.ds(n, n), :], lhs.at[pl.ds(0, n), :], l_send, l_recv,
                                     device_id=partner, device_id_type=MESH).wait()

    def free():
        pl.semaphore_signal(l_free, inc=1, device_id=partner, device_id_type=MESH)

    def scaled(rows, which, part):
        squares = jnp.zeros((PIECE, NB), F32)
        for j in range(nj):
            v = part(j, True)
            squares += v * v
        scale = lax.rsqrt(jnp.sum(squares, axis=1, keepdims=True) * (1 / depth) + 1e-6)
        for j in range(nj):
            cols = slice(j * NB, (j + 1) * NB)
            lhs[rows, cols] = (part(j, False) * scale * gains[pl.ds(which, 1), cols]).astype(BF16)

    class Operand:
        def __init__(self, piece0, pieces, base, second):
            self.piece0, self.pieces, self.base, self.second = piece0, pieces, base, second

        def here(self, p):
            return pl.ds(pl.multiple_of((self.piece0 + p) * PIECE, PIECE), PIECE)

        def loads(self, p):
            at, i = lax.rem(p, AHEAD), self.piece0 + p
            row = lax.div(i, np_) * tokens + core * half + lax.rem(i, np_) * PIECE
            return (pltpu.make_async_copy(x.at[pl.ds(pl.multiple_of(row, PIECE), PIECE), :], xin.at[at], in_sem.at[at, 0]),
                    pltpu.make_async_copy(q_all.at[0, :, self.here(p), :], qin.at[at], in_sem.at[at, 1]),
                    pltpu.make_async_copy(r_all.at[0, :, self.here(p), :], rin.at[at], in_sem.at[at, 2]))[: 3 if self.second else 1]

        def put(self, p):
            at = lax.rem(p, 2)
            return pltpu.make_async_copy(hst.at[at], h_all.at[:, self.here(p), :], h_sem.at[at])

        def give(self, p):
            here = pl.ds(pl.multiple_of(self.base + p * PIECE, PIECE), PIECE)
            there = pl.ds(pl.multiple_of(p * PIECE, PIECE), PIECE)
            return pltpu.make_async_remote_copy(lhs.at[here, :], lhs.at[there, :], l_send, l_recv, device_id=partner, device_id_type=MESH)

        def begin(self):
            for p in range(AHEAD - 1):
                for copy in self.loads(jnp.int32(p)):
                    copy.start()

        def before(self, p):
            @pl.when(p + AHEAD - 1 < self.pieces)
            def _():
                for copy in self.loads(p + AHEAD - 1):
                    copy.start()

            for copy in self.loads(p):
                copy.wait()

            @_if(_and(p >= 2, self.second))
            def _():
                self.put(p - 2).wait()

            @pl.when(p == 1)
            def _():
                pl.semaphore_wait(l_free, 1)

            @pl.when(p >= 1)
            def _():
                self.give(p - 1).start()

        def work(self, p):
            at, to = lax.rem(p, AHEAD), lax.rem(p, 2)
            rows = pl.ds(pl.multiple_of(self.base + p * PIECE, PIECE), PIECE)

            def plain(j, new):
                return xin[at, :, j * NB : (j + 1) * NB].astype(F32)

            def part(j, new):
                if new:
                    v = xin[at, :, j * NB : (j + 1) * NB].astype(F32) + (qin[at, j].astype(F32) + rin[at, j].astype(F32))
                    hst[to, j] = v.astype(BF16)
                return hst[to, j].astype(F32)

            scaled(rows, int(self.second), part if self.second else plain)

        def after(self, p):
            if self.second:
                self.put(p).start()

        def last(self):
            self.give(jnp.int32(self.pieces - 1)).start()

        def end(self):
            if self.second:
                for p in (2, 1):
                    self.put(jnp.int32(self.pieces - p)).wait()

    def with_operand(side, step):
        lax.fori_loop(0, side.pieces, lambda j, _: step(j, side), 0)
        side.last()
        lax.fori_loop(side.pieces, nj, lambda j, _: step(j), 0)
        side.end()

    early = pl.multiple_of((1 - core) * half, half)
    late = pl.multiple_of(core * half, half)

    def turned(t):
        t = t.astype(F32)
        r = pltpu.roll(t, HEAD // 2, 1)
        out = []
        for rows, place in ((slice(0, half), (1 - core) * half), (slice(half, tokens), core * half)):
            place = pl.ds(pl.multiple_of(place, half), half)
            out.append((t[rows] * cos[place, :] + r[rows] * sin[place, :]).astype(BF16))
        return jnp.concatenate(out, 0)

    def turn(s):
        for n in range(NB // HEAD):
            cols = pl.ds(pl.multiple_of(s * NB + n * HEAD, HEAD), HEAD)
            qs[:, cols] = turned(qs[:, cols])

    def attention():
        e = HEAD**-0.5 * LOG2E
        for n in range(kcols // HEAD):
            vx[n, :, :HEAD] = kvs[:, kcols + n * HEAD : kcols + (n + 1) * HEAD]
            vx[n, :, HEAD:] = jnp.ones((tokens, HEAD), BF16)
        seen = lax.broadcasted_iota(jnp.int32, (QB, QB), 1) <= lax.broadcasted_iota(jnp.int32, (QB, QB), 0)
        many = min(HEADS, group)

        def rows(b):
            at = b * QB
            return pl.ds(pl.multiple_of(early + at if at < half else late + at - half, QB), QB)

        def some(i, _):
            n = lax.div(i * many, group)
            kc = pl.ds(pl.multiple_of(n * HEAD, HEAD), HEAD)
            cols = [pl.ds(pl.multiple_of((i * many + t) * HEAD, HEAD), HEAD) for t in range(many)]
            keys = [kvs[rows(b), kc] for b in range(tokens // QB)]
            values = [vx[n, rows(b), :] for b in range(tokens // QB)]
            for b in range(tokens // QB):
                q = jnp.concatenate([qs[rows(b), c] for c in cols], 0)
                scores = _dot(q, jnp.concatenate(keys[: b + 1], 0), 1, 1)
                weights = []
                for t in range(many):
                    of = scores[t * QB : (t + 1) * QB]
                    parts = [of[:, u * QB : (u + 1) * QB] for u in range(b)] + [jnp.where(seen, of[:, b * QB :], HIDDEN)]
                    top = functools.reduce(jnp.maximum, parts).max(axis=1, keepdims=True)
                    weights.append(jnp.concatenate([jnp.exp2((u - top) * e).astype(BF16) for u in parts], 1))
                o = _dot(jnp.concatenate(weights, 0), jnp.concatenate(values[: b + 1], 0))
                for t, c in enumerate(cols):
                    of = o[t * QB : (t + 1) * QB]
                    hid[rows(b), c] = (of[:, :HEAD] / of[:, HEAD:]).astype(BF16)
            return 0

        lax.fori_loop(0, heads // many, some, 0)

    def first(c, _):
        g0 = c * na

        def queries(s, _):
            slot = ready(g0 + s, (Q, KV, O))
            turn(jnp.maximum(s - 1, 0))
            qs[:, pl.ds(pl.multiple_of(s * NB, NB), NB)] = _dot(lhs[:tokens], slots[slot]).astype(BF16)

            @pl.when((c >= 1) & (s == min(1, nq - 1)))
            def _():
                drain(sum_a(c - 1))

            return 0

        lax.fori_loop(0, nq, queries, 0)

        slot = ready(g0 + nq, (O,) if nwo > 1 else (O, Q, GU))
        turn(nq - 1)
        t = _dot(lhs[:tokens], slots[slot, :, : 2 * kcols])
        for n in range(kcols // HEAD):
            cols = slice(n * HEAD, (n + 1) * HEAD)
            kvs[:, cols] = turned(t[:, cols].astype(BF16))
        kvs[:, kcols:] = t[:, kcols:].astype(BF16)
        free()

        @pl.when(c >= 1)
        def _():
            drained(sum_a(c - 1))

        rows = Operand((c + 1) * np_, np_, half, False)
        shares = Operand(jnp.int32(0), big // PIECE, big, True)

        @pl.when(c + 1 < seqs)
        def _():
            rows.begin()

        @pl.when(c + 1 == seqs)
        def _():
            s = sum_a(jnp.int32(0))
            s.have()
            s.sent()
            sum_a(jnp.int32(EARLY)).have_head()
            shares.begin()

        attention()

        def project(j, *sides):
            k = lax.rem(j, per)
            g = g0 + nq + 1 + lax.div(j, per)

            @pl.when(k == 0)
            def _():
                ready(g, (O, Q, KV, GU, DOWN))

            w = slots.at[lax.rem(g, RING), pl.ds(pl.multiple_of(k * qcols, qcols), qcols), :]
            block(sum_a(c), j, lambda: _dot(hid[:tokens, :qcols], w[...]), *sides)
            return 0

        @pl.when(c + 1 < seqs)
        def _():
            with_operand(rows, project)
            exchanged(half)

        @pl.when(c + 1 == seqs)
        def _():
            with_operand(shares, project)
            exchanged(big)

        return 0

    def puts(c, j, t):
        at = lax.rem(t, YB)
        where = y.at[pl.ds(pl.multiple_of(c * tokens + core * half, half), half), block_cols(j)]
        return (pltpu.make_async_copy(yout.at[at], where, yl_sem.at[at]),
                pltpu.make_async_remote_copy(yout.at[at], where, ys_sem.at[at], yr_sem.at[c], device_id=partner, device_id_type=MESH))

    class Results:
        def __init__(self):
            self.count = seqs - 1

        def of(self, t):
            return lax.div(t, nj), lax.rem(t, nj)

        def loads(self, t):
            c, j = self.of(t)
            at = lax.rem(t, YB)
            rows = pl.ds(pl.multiple_of(c * half, half), half)
            return [pltpu.make_async_copy(src, yin.at[at, i], yin_sem.at[at, i])
                    for i, src in enumerate((h_all.at[j, rows, :], q_all.at[1, j, rows, :], r_all.at[1, j, rows, :]))]

        def fetch(self, t):
            c, j = self.of(t)

            @pl.when(j == 0)
            def _():
                sum_m(c).have()

            for copy in self.loads(t):
                copy.start()

        def begin(self):
            for t in range(YB - 1):
                self.fetch(jnp.int32(t))

        def left(self, t):
            near, far = puts(*self.of(t), t)
            near.wait()
            far.wait_send()

        def item(self, t):
            at = lax.rem(t, YB)

            @pl.when(t + YB - 1 < self.count * nj)
            def _():
                self.fetch(t + YB - 1)

            for copy in self.loads(t):
                copy.wait()

            @pl.when(t >= YB)
            def _():
                self.left(t - YB)

            yout[at] = (yin[at, 0].astype(F32) + (yin[at, 1].astype(F32) + yin[at, 2].astype(F32))).astype(BF16)
            for copy in puts(*self.of(t), t):
                copy.start()

        def beside(self, j):
            for k in range(self.count):
                self.item(j * self.count + k)

        def end(self):
            for t in range(self.count * nj - YB, self.count * nj):
                self.left(jnp.int32(t))
            for c in range(self.count):
                sum_m(jnp.int32(c)).sent()

    def gated(gate, up):
        return (gate * jax.nn.sigmoid(gate) * up).astype(BF16)

    def second(m, n, ahead):
        g0 = all_a + m * nm

        def before(act):
            if n == small:
                act(sum_m(m - 1))
            else:

                @pl.when(m == 0)
                def _():
                    act(sum_a(jnp.int32(seqs - 1)))

                @pl.when(m > 0)
                def _():
                    act(sum_m(m - 1))

        def gates(s, _):
            slot = ready(g0 + s, (GU, REST, DOWN))
            t = _dot(lhs[: 2 * n], slots[slot])
            hid[: 2 * n, pl.ds(pl.multiple_of(s * FB, FB), FB)] = gated(t[:, :FB], t[:, FB:])

            @pl.when(s == 1)
            def _():
                before(drain)

            @pl.when(s == 3)
            def _():
                before(drained)

            return 0

        lax.fori_loop(0, ngu, gates, 0)
        ahead()
        if tail:
            slot = ready(g0 + ngu, (DOWN,), None, 2 * tail)
            t = _dot(lhs[: 2 * n], slots[slot, :, : 2 * tail])
            hid[: 2 * n, ngu * FB :] = gated(t[:, :tail], t[:, tail:])

        def down(j):
            slot = ready(g0 + first_d + j, (GU, DOWN), ff)
            return lambda: _dot(hid[: 2 * n], slots[slot, :ff, :])

        return down

    def share(m, _):
        ends = m == seqs - 2
        next_n = jnp.where(ends, small, big)
        side = Operand((m + 1) * (big // PIECE), lax.div(next_n, PIECE), next_n, True)

        def ahead():
            @pl.when(m == 0)
            def _():
                s = sum_a(jnp.int32(EARLY))
                s.have_rest()
                s.sent()

            side.begin()

        down = second(m, big, ahead)
        free()

        def step(j, *sides):
            if sides:

                @pl.when((j == NEXT) & (m + 2 < seqs))
                def _():
                    s = sum_a(m + 2)
                    s.have()
                    s.sent()

            block(sum_m(m), j, down(j), *sides)
            return 0

        with_operand(side, step)

        @pl.when(ends)
        def _():
            exchanged(small)

        @pl.when(jnp.logical_not(ends))
        def _():
            exchanged(big)

        return 0

    def last_share():
        done = Results()
        down = second(seqs - 1, small, done.begin)
        pl.semaphore_signal(x_free, inc=1, device_id=across, device_id_type=MESH)

        def step(j, _):
            block_last(j, down(j), done)
            return 0

        lax.fori_loop(0, nj, step, 0)
        finish_last(jnp.int32(nj - 1))
        for j in range(nj - OWN, nj):
            final.shared(jnp.int32(j)).wait_send()
        done.end()

    def fetched(p):
        owner = jnp.where(p < np_, 1 - core, core)
        rows = pl.ds(pl.multiple_of(owner * half + lax.rem(p, np_) * PIECE, PIECE), PIECE)
        return pltpu.make_async_copy(x.at[rows, :], lhs.at[pl.ds(pl.multiple_of(p * PIECE, PIECE), PIECE), :], first_sem.at[p])

    tables = [pltpu.make_async_copy(src, dst, table_sem.at[i]) for i, (src, dst) in
              enumerate(((gain_a, gain_in.at[0]), (gain_m, gain_in.at[1]), (cos_in, cos), (sin_in, sin)))]
    for p in range(2 * np_):
        fetched(jnp.int32(p)).start()
    for copy in tables:
        copy.start()
    barrier = pltpu.get_barrier_semaphore()
    for peer in (partner, across):
        pl.semaphore_signal(barrier, inc=1, device_id=peer, device_id_type=MESH)
    for i in range(2):
        tables[i].wait()
        wide = gain_in[i].astype(F32)
        for r in range(depth // LANES):
            gains[i : i + 1, r * LANES : (r + 1) * LANES] = wide[r : r + 1]

    def normed(p, _):
        rows = pl.ds(pl.multiple_of(p * PIECE, PIECE), PIECE)
        fetched(p).wait()
        scaled(rows, 0, lambda j, new: lhs[rows, j * NB : (j + 1) * NB].astype(F32))

        for g in range(RING - 1):

            @pl.when(p == 3 + 4 * g)
            def _():
                start(jnp.int32(g), (Q, KV))

        return 0

    lax.fori_loop(0, 2 * np_, normed, 0)
    pl.semaphore_wait(barrier, 2)
    for copy in tables[2:]:
        copy.wait()
    lax.fori_loop(0, seqs, first, 0)
    lax.fori_loop(0, seqs - 1, share, 0)
    last_share()

    def left(j):
        near, far = puts(seqs - 1, j, j)
        near.wait()
        far.wait_send()

    over = (seqs - 1) * (big - half)

    def blocks(j):
        at, row0 = lax.rem(j, YB), (seqs - 1) * half
        return [pltpu.make_async_copy(src.at[j, pl.ds(row0, n), :], yin.at[at, i, pl.ds(0, n), :], yin_sem.at[at, i])
                for i, (src, n) in enumerate(((h_all, half), (q_all.at[1], over), (r_all.at[1], over)))]

    for j in range(YB - 1):
        for copy in blocks(jnp.int32(j)):
            copy.start()

    def piece(j, _):
        at = lax.rem(j, YB)

        @pl.when(j + YB - 1 < nj)
        def _():
            for copy in blocks(j + YB - 1):
                copy.start()

        @pl.when(j >= YB)
        def _():
            left(j - YB)

        for copy in blocks(j):
            copy.wait()
        crossed_last(j).wait_recv()
        here, there = lhs[:small, block_cols(j)].astype(F32), lhs[small : 2 * small, block_cols(j)].astype(F32)
        yout[at, :over] = (yin[at, 0, :over].astype(F32) + (yin[at, 1, :over].astype(F32) + yin[at, 2, :over].astype(F32))).astype(BF16)
        yout[at, over:] = (yin[at, 0, over:].astype(F32) + (here + there)).astype(BF16)
        for copy in puts(seqs - 1, j, j):
            copy.start()
        return 0

    lax.fori_loop(0, nj, piece, 0)
    for j in range(nj - YB, nj):
        left(jnp.int32(j))
    final.sent()

    def arrived(c, _):
        where = y.at[pl.ds(pl.multiple_of(c * tokens + (1 - core) * half, half), half), :]
        pltpu.make_async_copy(where, where, yr_sem.at[c]).wait()
        return 0

    lax.fori_loop(0, seqs, arrived, 0)


def layer(x, gain_a, wq, wk, wv, wo, gain_m, w_gate, w_up, w_down):
    seqs, tokens, depth = x.shape
    half, nj = tokens // 2, depth // NB
    big, _ = _shares(seqs, half)
    i = np.arange(HEAD // 2, dtype=np.float32)
    angle = np.arange(tokens, dtype=np.float32)[:, None] * np.float32(THETA) ** (-i / np.float32(HEAD // 2))
    cos, sin = np.cos(angle), np.sin(angle)
    cos, sin = np.concatenate([cos, cos], 1).astype(np.float32), np.concatenate([-sin, sin], 1).astype(np.float32)
    hbm = pl.BlockSpec(memory_space=pl.ANY)
    dma, regular = pltpu.SemaphoreType.DMA, pltpu.SemaphoreType.REGULAR
    out = [
        jax.ShapeDtypeStruct((seqs * tokens, depth), BF16),
        jax.ShapeDtypeStruct((nj, seqs * half, NB), BF16),
        jax.ShapeDtypeStruct((2, nj, seqs * half, NB), BF16),
        jax.ShapeDtypeStruct((2, nj, seqs * half, NB), BF16),
    ]
    kv = wk.shape[1]
    scratch = [
        pltpu.VMEM((2 * big, depth), BF16),
        pltpu.VMEM((RING, depth, NB), BF16),
        pltpu.VMEM((tokens, wq.shape[1]), BF16),
        pltpu.VMEM((tokens, 2 * kv), BF16),
        pltpu.VMEM((kv // HEAD, tokens, 2 * HEAD), BF16),
        pltpu.VMEM((2 * big, w_down.shape[0]), BF16),
        pltpu.VMEM((OWN, big, NB), F32),
        pltpu.VMEM((OWN, big, NB), BF16),
        pltpu.VMEM((FAR, big, NB), BF16),
        pltpu.VMEM((STG, big, NB), BF16),
        pltpu.VMEM((AHEAD, PIECE, depth), BF16),
        pltpu.VMEM((AHEAD, nj, PIECE, NB), BF16),
        pltpu.VMEM((AHEAD, nj, PIECE, NB), BF16),
        pltpu.VMEM((2, nj, PIECE, NB), BF16),
        pltpu.VMEM((YB, 3, half, NB), BF16),
        pltpu.VMEM((YB, half, NB), BF16),
        pltpu.VMEM((tokens, HEAD), F32),
        pltpu.VMEM((tokens, HEAD), F32),
        pltpu.VMEM((2, depth // LANES, LANES), BF16),
        pltpu.VMEM((2, depth), F32),
        dma((RING,)), dma((OWN,)), dma((FAR,)), dma((STG,)), dma((2 * seqs,)), dma((2 * seqs - 1,)),
        dma, dma, regular, regular,
        dma((AHEAD, 3)), dma((2,)), dma((YB, 3)), dma((YB,)), dma((YB,)), dma((seqs,)),
        dma((tokens // PIECE,)), dma((4,)), dma, dma((nj,)),
    ]
    y, *_ = pl.pallas_call(
        functools.partial(layer_kernel, seqs=seqs),
        out_shape=out,
        in_specs=[hbm] * 12,
        out_specs=[hbm] * 4,
        scratch_shapes=scratch,
        compiler_params=pltpu.CompilerParams(collective_id=0, has_side_effects=True, vmem_limit_bytes=67043328),
        name="layer",
    )(x.reshape(seqs * tokens, depth), wq, wk, wv, wo, w_gate, w_up, w_down, cos, sin,
      gain_a.reshape(-1, LANES), gain_m.reshape(-1, LANES))
    return y.reshape(x.shape)


def solution(mesh):
    def step(*args):
        return layer(*args)

    tokens, whole, columns, rows_of = P("dp", None, None), P(None), P(None, "tp"), P("tp", None)
    return jax.shard_map(
        step,
        mesh=mesh,
        in_specs=(tokens, whole, columns, columns, columns, rows_of, whole, columns, columns, rows_of),
        out_specs=tokens,
        check_vma=False,
    )
```

```python
import functools

import jax
import jax.numpy as jnp
import numpy as np
from jax import lax
from jax.experimental import pallas as pl
from jax.experimental.pallas import tpu as pltpu
from jax.sharding import PartitionSpec as P

HEAD = 128
THETA = 10000
LOG2E = 1.4426950408889634
HIDDEN = -2e30
MESH = pl.DeviceIdType.MESH
NB = 512
FB = 256
NEXT = 3
EARLY = 1
RING = 3
Q, KV, O, GU, REST, DOWN = range(6)
LANES = 128
PIECE = 32
AHEAD = 4
LAG = 3
OWN, FAR = LAG + 1, 2 * LAG
STG = 4
YB = 4
QB = 128
HEADS = 8
F32, BF16 = jnp.float32, jnp.bfloat16


def _dot(a, b, ca=1, cb=0):
    return lax.dot_general(a, b, (((ca,), (cb,)), ((), ())), preferred_element_type=F32)


def _if(cond):
    if isinstance(cond, bool):
        return (lambda act: act()) if cond else (lambda act: None)
    return pl.when(cond)


def _either(cond, yes, no):
    def run(act):
        def branch():
            act()
            return 0

        return branch

    lax.cond(cond, run(yes), run(no))


def _and(*conds):
    known = [c for c in conds if isinstance(c, bool)]
    rest = [c for c in conds if not isinstance(c, bool)]
    return functools.reduce(jnp.logical_and, rest) if all(known) and rest else all(known)


def _shares(seqs, half):
    big = half + PIECE
    return big, seqs * half - (seqs - 1) * big


def layer_kernel(
    x, wq, wk, wv, wo, wg, wu, wd, cos_in, sin_in, gain_a, gain_m,
    y, h_all, q_all, r_all,
    lhs, slots, qs, kvs, vx, hid, own, snd, rcv, stg, xin, qin, rin, hst, yin, yout, cos, sin, gain_in, gains,
    wsem, rs_send, rs_recv, st_sem, xs_sem, xr_sem, l_send, l_recv, l_free, x_free, in_sem, h_sem, yin_sem, yl_sem, ys_sem, yr_sem,
    first_sem, table_sem, xh_sem, xl_sem,
    *, seqs,
):
    tokens, depth = qs.shape[0], x.shape[1]
    half = tokens // 2
    big, small = _shares(seqs, half)
    qcols, kcols, ff = wq.shape[1], wk.shape[1], wd.shape[0]
    nj = depth // NB
    nq = qcols // NB
    per = depth // qcols
    nwo = nj // per
    na = nq + 1 + nwo
    ngu = ff // FB
    tail = ff - ngu * FB
    nm = ngu + (1 if tail else 0) + nj
    first_d = nm - nj
    all_a = seqs * na
    total = all_a + seqs * nm
    heads = qcols // HEAD
    group = heads // (kcols // HEAD)
    np_ = half // PIECE
    last = 2 * seqs - 1

    me = lax.axis_index("tp")
    core, chip = lax.rem(me, 2), lax.div(me, 2)
    partner = {"tp": chip * 2 + (1 - core)}
    across = {"tp": (1 - chip) * 2 + core}

    def start(g, kinds):
        slot = lax.rem(g, RING)

        def when(kind, cond):
            if kind not in kinds:
                return lambda act: None
            return (lambda act: act()) if len(kinds) == 1 else pl.when(cond)

        sem = wsem.at[slot]
        in_a = g < all_a
        a, m = lax.rem(g, na), lax.rem(g + (nm - all_a % nm), nm)

        @when(Q, in_a & (a < nq))
        def _():
            pltpu.make_async_copy(wq.at[:, pl.ds(pl.multiple_of(a * NB, NB), NB)], slots.at[slot], sem).start()

        @when(KV, in_a & (a == nq))
        def _():
            pltpu.make_async_copy(wk, slots.at[slot, :, pl.ds(0, kcols)], sem).start()
            pltpu.make_async_copy(wv, slots.at[slot, :, pl.ds(kcols, kcols)], sem).start()

        @when(O, in_a & (a > nq))
        def _():
            for k in range(per):
                at = pl.multiple_of(((a - nq - 1) * per + k) * NB, NB)
                pltpu.make_async_copy(wo.at[:, pl.ds(at, NB)], slots.at[slot, pl.ds(k * qcols, qcols), :], sem).start()

        in_m = jnp.logical_not(in_a) & (g < total)

        @when(GU, in_m & (m < ngu))
        def _():
            at = pl.multiple_of(m * FB, FB)
            pltpu.make_async_copy(wg.at[:, pl.ds(at, FB)], slots.at[slot, :, pl.ds(0, FB)], sem).start()
            pltpu.make_async_copy(wu.at[:, pl.ds(at, FB)], slots.at[slot, :, pl.ds(FB, FB)], sem).start()

        if tail:

            @when(REST, in_m & (m == ngu))
            def _():
                pltpu.make_async_copy(wg.at[:, pl.ds(ngu * FB, tail)], slots.at[slot, :, pl.ds(0, tail)], sem).start()
                pltpu.make_async_copy(wu.at[:, pl.ds(ngu * FB, tail)], slots.at[slot, :, pl.ds(tail, tail)], sem).start()

        @when(DOWN, in_m & (m >= first_d))
        def _():
            at = pl.multiple_of((m - first_d) * NB, NB)
            pltpu.make_async_copy(wd.at[:, pl.ds(at, NB)], slots.at[slot, pl.ds(0, ff), :], sem).start()

    def ready(g, kinds, rows=None, cols=NB):
        to = g + RING - 1
        a, m = lax.rem(to, na), lax.rem(to + (nm - all_a % nm), nm)

        def follow():
            if kinds == (GU, REST, DOWN):
                _either(m < ngu, lambda: start(to, (GU,)), lambda: start(to, (REST, DOWN)))
            elif kinds == (GU, DOWN):

                def gates():
                    @pl.when(to < total)
                    def _():
                        start(to, (GU,))

                _either(m >= first_d, lambda: start(to, (DOWN,)), gates)
            elif kinds == (Q, KV, O):
                _either(a < nq, lambda: start(to, (Q,)), lambda: start(to, (KV, O)))
            else:
                start(to, kinds)

        slot = lax.rem(g, RING)
        rows = depth if rows is None else rows
        where = slots.at[slot, pl.ds(0, rows), pl.ds(0, cols)]
        pltpu.make_async_copy(where, where, wsem.at[slot]).wait()
        follow()
        return slot

    class Sum:
        def __init__(self, ar, which, row0, n):
            self.ar, self.which, self.row0, self.n = ar, which, row0, n

        def far(self, j, at, n, sem):
            rows = pl.ds(pl.multiple_of(self.row0 + at, PIECE), n)
            return pltpu.make_async_remote_copy(q_all.at[self.which, j, rows, :], r_all.at[self.which, j, rows, :], xs_sem.at[self.ar], sem,
                                                device_id=across, device_id_type=MESH)

        def crossed(self, j):
            return self.far(j, 0, self.n, xr_sem.at[self.ar])

        def head(self, j):
            return self.far(j, 0, PIECE, xh_sem)

        def rest(self, j):
            return self.far(j, PIECE, self.n - PIECE, xr_sem.at[self.ar])

        def cross(self, j):
            if self.which:
                self.crossed(j).start()
            else:

                _either(self.ar == EARLY, lambda: self.head(j).start(), lambda: self.crossed(j).start())

        def each(self, act):
            def one(j, _):
                act(j)
                return 0

            lax.fori_loop(0, nj, one, 0)

        def all_blocks(self, sem, at=0, n=None):
            rows = pl.ds(pl.multiple_of(self.row0 + at, PIECE), n or self.n)
            whole = r_all.at[self.which, :, rows, :]
            pltpu.make_async_copy(whole, whole, sem).wait()

        def sent(self):
            self.all_blocks(xs_sem.at[self.ar])

        def have(self):
            self.all_blocks(xr_sem.at[self.ar])

        def have_head(self):
            self.all_blocks(xh_sem, 0, PIECE)

        def have_rest(self):
            self.all_blocks(xr_sem.at[self.ar], PIECE, self.n - PIECE)

        def kept(self, j):
            at = lax.rem(j, STG)
            rows = pl.ds(pl.multiple_of(self.row0, PIECE), self.n)
            return pltpu.make_async_copy(stg.at[at, pl.ds(0, self.n), :], q_all.at[self.which, j, rows, :], st_sem.at[at])

        def shared(self, j):
            i = self.ar * nj + j
            near, far = lax.rem(i, OWN), lax.rem(i, FAR)
            return pltpu.make_async_remote_copy(snd.at[near, pl.ds(0, self.n), :], rcv.at[far, pl.ds(0, self.n), :], rs_send.at[near],
                                                rs_recv.at[far], device_id=partner, device_id_type=MESH)

        def of_chip(self, j):
            i = self.ar * nj + j
            return (own[lax.rem(i, OWN), : self.n] + rcv[lax.rem(i, FAR), : self.n].astype(F32)).astype(BF16)

        def keep_term(self, j, t):
            i = self.ar * nj + j
            snd[lax.rem(i, OWN), : self.n] = t[: self.n].astype(BF16)
            own[lax.rem(i, OWN), : self.n] = t[self.n :]

    def sum_a(c):
        return Sum(c, 0, c * half, half)

    def sum_m(m):
        return Sum(seqs + m, 1, m * big, big)

    final = Sum(jnp.int32(last), 1, (seqs - 1) * big, small)

    def block(s, j, term, *sides):
        @pl.when(j >= LAG)
        def _():
            s.shared(j - LAG).wait()

        for side in sides:
            side.before(j)
        for side in sides:
            side.work(j)
        stg[lax.rem(j + 12 - LAG, STG), : s.n] = s.of_chip(j + 12 - LAG)
        s.keep_term(j, term())

        @pl.when(j >= LAG)
        def _():
            @pl.when(j > LAG)
            def _():
                s.kept(j - LAG - 1).wait()
                s.cross(j - LAG - 1)

            s.kept(j - LAG).start()

        s.shared(j).start()
        for side in sides:
            side.after(j)

    def drain(s):
        for j in range(nj - LAG, nj):
            s.shared(jnp.int32(j)).wait_recv()
            stg[j % STG, : s.n] = s.of_chip(jnp.int32(j))
            s.kept(jnp.int32(j)).start()

    def drained(s):
        for j in range(nj - LAG - 1, nj):
            s.kept(jnp.int32(j)).wait()
            s.cross(jnp.int32(j))
        for j in range(nj - LAG, nj):
            s.shared(jnp.int32(j)).wait_send()
        if not s.which:

            @pl.when(s.ar == EARLY)
            def _():
                s.each(lambda j: s.rest(j).start())

    def block_cols(j):
        return pl.ds(pl.multiple_of(j * NB, NB), NB)

    def crossed_last(j):
        return pltpu.make_async_remote_copy(lhs.at[pl.ds(0, small), block_cols(j)], lhs.at[pl.ds(small, small), block_cols(j)],
                                            xs_sem.at[last], xl_sem.at[j], device_id=across, device_id_type=MESH)

    def finish_last(j):
        final.shared(j).wait_recv()
        lhs[:small, block_cols(j)] = final.of_chip(j)
        crossed_last(j).start()

    def block_last(j, term, side):
        @pl.when(j >= OWN)
        def _():
            final.shared(j - OWN).wait_send()

        final.keep_term(j, term())
        final.shared(j).start()
        side.beside(j)

        @pl.when(j == 0)
        def _():
            pl.semaphore_wait(x_free, 1)

        finish_last(j)

    def exchanged(n):
        pltpu.make_async_remote_copy(lhs.at[pl.ds(n, n), :], lhs.at[pl.ds(0, n), :], l_send, l_recv,
                                     device_id=partner, device_id_type=MESH).wait()

    def free():
        pl.semaphore_signal(l_free, inc=1, device_id=partner, device_id_type=MESH)

    def scaled(rows, which, part):
        squares = jnp.zeros((PIECE, NB), F32)
        for j in range(nj):
            v = part(j, True)
            squares += v * v
        scale = lax.rsqrt(jnp.sum(squares, axis=1, keepdims=True) * (1 / depth) + 1e-6)
        for j in range(nj):
            cols = slice(j * NB, (j + 1) * NB)
            lhs[rows, cols] = (part(j, False) * scale * gains[pl.ds(which, 1), cols]).astype(BF16)

    class Operand:
        def __init__(self, piece0, pieces, base, second):
            self.piece0, self.pieces, self.base, self.second = piece0, pieces, base, second

        def here(self, p):
            return pl.ds(pl.multiple_of((self.piece0 + p) * PIECE, PIECE), PIECE)

        def loads(self, p):
            at, i = lax.rem(p, AHEAD), self.piece0 + p
            row = lax.div(i, np_) * tokens + core * half + lax.rem(i, np_) * PIECE
            return (pltpu.make_async_copy(x.at[pl.ds(pl.multiple_of(row, PIECE), PIECE), :], xin.at[at], in_sem.at[at, 0]),
                    pltpu.make_async_copy(q_all.at[0, :, self.here(p), :], qin.at[at], in_sem.at[at, 1]),
                    pltpu.make_async_copy(r_all.at[0, :, self.here(p), :], rin.at[at], in_sem.at[at, 2]))[: 3 if self.second else 1]

        def put(self, p):
            at = lax.rem(p, 2)
            return pltpu.make_async_copy(hst.at[at], h_all.at[:, self.here(p), :], h_sem.at[at])

        def give(self, p):
            here = pl.ds(pl.multiple_of(self.base + p * PIECE, PIECE), PIECE)
            there = pl.ds(pl.multiple_of(p * PIECE, PIECE), PIECE)
            return pltpu.make_async_remote_copy(lhs.at[here, :], lhs.at[there, :], l_send, l_recv, device_id=partner, device_id_type=MESH)

        def begin(self):
            for p in range(AHEAD - 1):
                for copy in self.loads(jnp.int32(p)):
                    copy.start()

        def before(self, p):
            @pl.when(p + AHEAD - 1 < self.pieces)
            def _():
                for copy in self.loads(p + AHEAD - 1):
                    copy.start()

            for copy in self.loads(p):
                copy.wait()

            @pl.when(p == 1)
            def _():
                pl.semaphore_wait(l_free, 1)
                self.give(jnp.int32(0)).start()

            @pl.when(p >= 2)
            def _():
                if self.second:
                    self.put(p - 2).wait()
                self.give(p - 1).start()

        def work(self, p):
            at, to = lax.rem(p, AHEAD), lax.rem(p, 2)
            rows = pl.ds(pl.multiple_of(self.base + p * PIECE, PIECE), PIECE)

            def plain(j, new):
                return xin[at, :, j * NB : (j + 1) * NB].astype(F32)

            def part(j, new):
                if new:
                    v = xin[at, :, j * NB : (j + 1) * NB].astype(F32) + (qin[at, j].astype(F32) + rin[at, j].astype(F32))
                    hst[to, j] = v.astype(BF16)
                return hst[to, j].astype(F32)

            scaled(rows, int(self.second), part if self.second else plain)

        def after(self, p):
            if self.second:
                self.put(p).start()

        def last(self):
            self.give(jnp.int32(self.pieces - 1)).start()

        def end(self):
            if self.second:
                for p in (2, 1):
                    self.put(jnp.int32(self.pieces - p)).wait()

    def with_operand(side, step):
        lax.fori_loop(0, side.pieces, lambda j, _: step(j, side), 0)
        side.last()
        lax.fori_loop(side.pieces, nj, lambda j, _: step(j), 0)
        side.end()

    early = pl.multiple_of((1 - core) * half, half)
    late = pl.multiple_of(core * half, half)

    def turned(t):
        t = t.astype(F32)
        r = pltpu.roll(t, HEAD // 2, 1)
        out = []
        for rows, place in ((slice(0, half), (1 - core) * half), (slice(half, tokens), core * half)):
            place = pl.ds(pl.multiple_of(place, half), half)
            out.append((t[rows] * cos[place, :] + r[rows] * sin[place, :]).astype(BF16))
        return jnp.concatenate(out, 0)

    def turn(s):
        for n in range(NB // HEAD):
            cols = pl.ds(pl.multiple_of(s * NB + n * HEAD, HEAD), HEAD)
            qs[:, cols] = turned(qs[:, cols])

    def attention():
        e = HEAD**-0.5 * LOG2E
        for n in range(kcols // HEAD):
            vx[n, :, :HEAD] = kvs[:, kcols + n * HEAD : kcols + (n + 1) * HEAD]
        seen = lax.broadcasted_iota(jnp.int32, (QB, QB), 1) <= lax.broadcasted_iota(jnp.int32, (QB, QB), 0)
        many = min(HEADS, group)

        def rows(b):
            at = b * QB
            return pl.ds(pl.multiple_of(early + at if at < half else late + at - half, QB), QB)

        def some(i, _):
            n = lax.div(i * many, group)
            kc = pl.ds(pl.multiple_of(n * HEAD, HEAD), HEAD)
            cols = [pl.ds(pl.multiple_of((i * many + t) * HEAD, HEAD), HEAD) for t in range(many)]
            keys = [kvs[rows(b), kc] for b in range(tokens // QB)]
            values = [vx[n, rows(b), :] for b in range(tokens // QB)]
            for b in range(tokens // QB):
                q = jnp.concatenate([qs[rows(b), c] for c in cols], 0)
                scores = _dot(q, jnp.concatenate(keys[: b + 1], 0), 1, 1)
                weights = []
                for t in range(many):
                    of = scores[t * QB : (t + 1) * QB]
                    parts = [of[:, u * QB : (u + 1) * QB] for u in range(b)] + [jnp.where(seen, of[:, b * QB :], HIDDEN)]
                    top = functools.reduce(jnp.maximum, parts).max(axis=1, keepdims=True)
                    weights.append(jnp.concatenate([jnp.exp2((u - top) * e).astype(BF16) for u in parts], 1))
                o = _dot(jnp.concatenate(weights, 0), jnp.concatenate(values[: b + 1], 0))
                for t, c in enumerate(cols):
                    of = o[t * QB : (t + 1) * QB]
                    hid[rows(b), c] = (of[:, :HEAD] / of[:, HEAD:]).astype(BF16)
            return 0

        lax.fori_loop(0, heads // many, some, 0)

    def first(c, _):
        g0 = c * na

        def queries(s, _):
            slot = ready(g0 + s, (Q, KV, O))
            turn(jnp.maximum(s - 1, 0))
            qs[:, pl.ds(pl.multiple_of(s * NB, NB), NB)] = _dot(lhs[:tokens], slots[slot]).astype(BF16)

            @pl.when((c >= 1) & (s == min(1, nq - 1)))
            def _():
                drain(sum_a(c - 1))

            return 0

        lax.fori_loop(0, nq, queries, 0)

        slot = ready(g0 + nq, (O,) if nwo > 1 else (O, Q, GU))
        turn(nq - 1)
        t = _dot(lhs[:tokens], slots[slot, :, : 2 * kcols])
        for n in range(kcols // HEAD):
            cols = slice(n * HEAD, (n + 1) * HEAD)
            kvs[:, cols] = turned(t[:, cols].astype(BF16))
        kvs[:, kcols:] = t[:, kcols:].astype(BF16)
        free()

        @pl.when(c >= 1)
        def _():
            drained(sum_a(c - 1))

        rows = Operand((c + 1) * np_, np_, half, False)
        shares = Operand(jnp.int32(0), big // PIECE, big, True)

        @pl.when(c + 1 < seqs)
        def _():
            rows.begin()

        @pl.when(c + 1 == seqs)
        def _():
            s = sum_a(jnp.int32(0))
            s.have()
            s.sent()
            sum_a(jnp.int32(EARLY)).have_head()
            shares.begin()

        attention()

        def project(j, *sides):
            k = lax.rem(j, per)
            g = g0 + nq + 1 + lax.div(j, per)

            @pl.when(k == 0)
            def _():
                ready(g, (O, Q, KV, GU, DOWN))

            w = slots.at[lax.rem(g, RING), pl.ds(pl.multiple_of(k * qcols, qcols), qcols), :]
            block(sum_a(c), j, lambda: _dot(hid[:tokens, :qcols], w[...]), *sides)
            return 0

        @pl.when(c + 1 < seqs)
        def _():
            with_operand(rows, project)
            exchanged(half)

        @pl.when(c + 1 == seqs)
        def _():
            with_operand(shares, project)
            exchanged(big)

        return 0

    def puts(c, j, t):
        at = lax.rem(t, YB)
        where = y.at[pl.ds(pl.multiple_of(c * tokens + core * half, half), half), block_cols(j)]
        return (pltpu.make_async_copy(yout.at[at], where, yl_sem.at[at]),
                pltpu.make_async_remote_copy(yout.at[at], where, ys_sem.at[at], yr_sem.at[c], device_id=partner, device_id_type=MESH))

    class Results:
        def __init__(self):
            self.count = seqs - 1

        def of(self, t):
            return lax.div(t, nj), lax.rem(t, nj)

        def loads(self, t):
            c, j = self.of(t)
            at = lax.rem(t, YB)
            rows = pl.ds(pl.multiple_of(c * half, half), half)
            return [pltpu.make_async_copy(src, yin.at[at, i], yin_sem.at[at, i])
                    for i, src in enumerate((h_all.at[j, rows, :], q_all.at[1, j, rows, :], r_all.at[1, j, rows, :]))]

        def fetch(self, t):
            c, j = self.of(t)

            @pl.when(j == 0)
            def _():
                sum_m(c).have()

            for copy in self.loads(t):
                copy.start()

        def begin(self):
            for t in range(YB - 1):
                self.fetch(jnp.int32(t))

        def left(self, t):
            near, far = puts(*self.of(t), t)
            near.wait()
            far.wait_send()

        def item(self, t):
            at = lax.rem(t, YB)

            @pl.when(t + YB - 1 < self.count * nj)
            def _():
                self.fetch(t + YB - 1)

            for copy in self.loads(t):
                copy.wait()

            @pl.when(t >= YB)
            def _():
                self.left(t - YB)

            yout[at] = (yin[at, 0].astype(F32) + (yin[at, 1].astype(F32) + yin[at, 2].astype(F32))).astype(BF16)
            for copy in puts(*self.of(t), t):
                copy.start()

        def beside(self, j):
            for k in range(self.count):
                self.item(j * self.count + k)

        def end(self):
            for t in range(self.count * nj - YB, self.count * nj):
                self.left(jnp.int32(t))
            for c in range(self.count):
                sum_m(jnp.int32(c)).sent()

    def gated(gate, up):
        return (gate * jax.nn.sigmoid(gate) * up).astype(BF16)

    def second(m, n, ahead):
        g0 = all_a + m * nm

        def before(act):
            if n == small:
                act(sum_m(m - 1))
            else:

                @pl.when(m == 0)
                def _():
                    act(sum_a(jnp.int32(seqs - 1)))

                @pl.when(m > 0)
                def _():
                    act(sum_m(m - 1))

        def gates(s, _):
            slot = ready(g0 + s, (GU, REST, DOWN))
            t = _dot(lhs[: 2 * n], slots[slot])
            hid[: 2 * n, pl.ds(pl.multiple_of(s * FB, FB), FB)] = gated(t[:, :FB], t[:, FB:])

            @pl.when((s == 1) | (s == 3))
            def _():
                @pl.when(s == 1)
                def _():
                    before(drain)

                @pl.when(s == 3)
                def _():
                    before(drained)

            return 0

        lax.fori_loop(0, ngu, gates, 0)
        ahead()
        if tail:
            slot = ready(g0 + ngu, (DOWN,), None, 2 * tail)
            t = _dot(lhs[: 2 * n], slots[slot, :, : 2 * tail])
            hid[: 2 * n, ngu * FB :] = gated(t[:, :tail], t[:, tail:])

        def down(j):
            slot = ready(g0 + first_d + j, (GU, DOWN), ff)
            return lambda: _dot(hid[: 2 * n], slots[slot, :ff, :])

        return down

    def share(m, _):
        ends = m == seqs - 2
        next_n = jnp.where(ends, small, big)
        side = Operand((m + 1) * (big // PIECE), lax.div(next_n, PIECE), next_n, True)

        def ahead():
            @pl.when(m == 0)
            def _():
                s = sum_a(jnp.int32(EARLY))
                s.have_rest()
                s.sent()

            side.begin()

        down = second(m, big, ahead)
        free()

        def step(j, *sides):
            if sides:

                @pl.when((j == NEXT) & (m + 2 < seqs))
                def _():
                    s = sum_a(m + 2)
                    s.have()
                    s.sent()

            block(sum_m(m), j, down(j), *sides)
            return 0

        with_operand(side, step)

        @pl.when(ends)
        def _():
            exchanged(small)

        @pl.when(jnp.logical_not(ends))
        def _():
            exchanged(big)

        return 0

    def last_share():
        done = Results()
        down = second(seqs - 1, small, done.begin)
        pl.semaphore_signal(x_free, inc=1, device_id=across, device_id_type=MESH)

        def step(j, _):
            block_last(j, down(j), done)
            return 0

        lax.fori_loop(0, nj, step, 0)
        for j in range(nj - OWN, nj):
            final.shared(jnp.int32(j)).wait_send()
        done.end()

    def fetched(p):
        owner = jnp.where(p < np_, 1 - core, core)
        rows = pl.ds(pl.multiple_of(owner * half + lax.rem(p, np_) * PIECE, PIECE), PIECE)
        return pltpu.make_async_copy(x.at[rows, :], lhs.at[pl.ds(pl.multiple_of(p * PIECE, PIECE), PIECE), :], first_sem.at[p])

    tables = [pltpu.make_async_copy(src, dst, table_sem.at[i]) for i, (src, dst) in
              enumerate(((gain_a, gain_in.at[0]), (gain_m, gain_in.at[1]), (cos_in, cos), (sin_in, sin)))]
    for p in range(2 * np_):
        fetched(jnp.int32(p)).start()
    for copy in tables:
        copy.start()
    barrier = pltpu.get_barrier_semaphore()
    for peer in (partner, across):
        pl.semaphore_signal(barrier, inc=1, device_id=peer, device_id_type=MESH)
    for n in range(kcols // HEAD):
        vx[n, :, HEAD:] = jnp.ones((tokens, HEAD), BF16)
    for i in range(2):
        tables[i].wait()
        wide = gain_in[i].astype(F32)
        for r in range(depth // LANES):
            gains[i : i + 1, r * LANES : (r + 1) * LANES] = wide[r : r + 1]

    def normed(p, _):
        rows = pl.ds(pl.multiple_of(p * PIECE, PIECE), PIECE)
        fetched(p).wait()
        scaled(rows, 0, lambda j, new: lhs[rows, j * NB : (j + 1) * NB].astype(F32))

        for g in range(RING - 1):

            @pl.when(p == 3 + 4 * g)
            def _():
                start(jnp.int32(g), (Q, KV))

        return 0

    lax.fori_loop(0, 2 * np_, normed, 0)
    pl.semaphore_wait(barrier, 2)
    for copy in tables[2:]:
        copy.wait()
    lax.fori_loop(0, seqs, first, 0)
    lax.fori_loop(0, seqs - 1, share, 0)
    last_share()

    def left(j):
        near, far = puts(seqs - 1, j, j)
        near.wait()
        far.wait_send()

    over = (seqs - 1) * (big - half)

    def blocks(j):
        at, row0 = lax.rem(j, YB), (seqs - 1) * half
        return [pltpu.make_async_copy(src.at[j, pl.ds(row0, n), :], yin.at[at, i, pl.ds(0, n), :], yin_sem.at[at, i])
                for i, (src, n) in enumerate(((h_all, half), (q_all.at[1], over), (r_all.at[1], over)))]

    for j in range(YB - 1):
        for copy in blocks(jnp.int32(j)):
            copy.start()

    def piece(j, _):
        at = lax.rem(j, YB)

        @pl.when(j + YB - 1 < nj)
        def _():
            for copy in blocks(j + YB - 1):
                copy.start()

        @pl.when(j >= YB)
        def _():
            left(j - YB)

        for copy in blocks(j):
            copy.wait()
        crossed_last(j).wait_recv()
        here, there = lhs[:small, block_cols(j)].astype(F32), lhs[small : 2 * small, block_cols(j)].astype(F32)
        yout[at, :over] = (yin[at, 0, :over].astype(F32) + (yin[at, 1, :over].astype(F32) + yin[at, 2, :over].astype(F32))).astype(BF16)
        yout[at, over:] = (yin[at, 0, over:].astype(F32) + (here + there)).astype(BF16)
        for copy in puts(seqs - 1, j, j):
            copy.start()
        return 0

    lax.fori_loop(0, nj, piece, 0)
    for j in range(nj - YB, nj):
        left(jnp.int32(j))
    final.sent()

    def arrived(c, _):
        where = y.at[pl.ds(pl.multiple_of(c * tokens + (1 - core) * half, half), half), :]
        pltpu.make_async_copy(where, where, yr_sem.at[c]).wait()
        return 0

    lax.fori_loop(0, seqs, arrived, 0)


def layer(x, gain_a, wq, wk, wv, wo, gain_m, w_gate, w_up, w_down):
    seqs, tokens, depth = x.shape
    half, nj = tokens // 2, depth // NB
    big, _ = _shares(seqs, half)
    i = np.arange(HEAD // 2, dtype=np.float32)
    angle = np.arange(tokens, dtype=np.float32)[:, None] * np.float32(THETA) ** (-i / np.float32(HEAD // 2))
    cos, sin = np.cos(angle), np.sin(angle)
    cos, sin = np.concatenate([cos, cos], 1).astype(np.float32), np.concatenate([-sin, sin], 1).astype(np.float32)
    hbm = pl.BlockSpec(memory_space=pl.ANY)
    dma, regular = pltpu.SemaphoreType.DMA, pltpu.SemaphoreType.REGULAR
    out = [
        jax.ShapeDtypeStruct((seqs * tokens, depth), BF16),
        jax.ShapeDtypeStruct((nj, seqs * half, NB), BF16),
        jax.ShapeDtypeStruct((2, nj, seqs * half, NB), BF16),
        jax.ShapeDtypeStruct((2, nj, seqs * half, NB), BF16),
    ]
    kv = wk.shape[1]
    scratch = [
        pltpu.VMEM((2 * big, depth), BF16),
        pltpu.VMEM((RING, depth, NB), BF16),
        pltpu.VMEM((tokens, wq.shape[1]), BF16),
        pltpu.VMEM((tokens, 2 * kv), BF16),
        pltpu.VMEM((kv // HEAD, tokens, 2 * HEAD), BF16),
        pltpu.VMEM((2 * big, w_down.shape[0]), BF16),
        pltpu.VMEM((OWN, big, NB), F32),
        pltpu.VMEM((OWN, big, NB), BF16),
        pltpu.VMEM((FAR, big, NB), BF16),
        pltpu.VMEM((STG, big, NB), BF16),
        pltpu.VMEM((AHEAD, PIECE, depth), BF16),
        pltpu.VMEM((AHEAD, nj, PIECE, NB), BF16),
        pltpu.VMEM((AHEAD, nj, PIECE, NB), BF16),
        pltpu.VMEM((2, nj, PIECE, NB), BF16),
        pltpu.VMEM((YB, 3, half, NB), BF16),
        pltpu.VMEM((YB, half, NB), BF16),
        pltpu.VMEM((tokens, HEAD), F32),
        pltpu.VMEM((tokens, HEAD), F32),
        pltpu.VMEM((2, depth // LANES, LANES), BF16),
        pltpu.VMEM((2, depth), F32),
        dma((RING,)), dma((OWN,)), dma((FAR,)), dma((STG,)), dma((2 * seqs,)), dma((2 * seqs - 1,)),
        dma, dma, regular, regular,
        dma((AHEAD, 3)), dma((2,)), dma((YB, 3)), dma((YB,)), dma((YB,)), dma((seqs,)),
        dma((tokens // PIECE,)), dma((4,)), dma, dma((nj,)),
    ]
    y, *_ = pl.pallas_call(
        functools.partial(layer_kernel, seqs=seqs),
        out_shape=out,
        in_specs=[hbm] * 12,
        out_specs=[hbm] * 4,
        scratch_shapes=scratch,
        compiler_params=pltpu.CompilerParams(collective_id=0, has_side_effects=True, vmem_limit_bytes=67043328),
        name="layer",
    )(x.reshape(seqs * tokens, depth), wq, wk, wv, wo, w_gate, w_up, w_down, cos, sin,
      gain_a.reshape(-1, LANES), gain_m.reshape(-1, LANES))
    return y.reshape(x.shape)


def solution(mesh):
    def step(*args):
        return layer(*args)

    tokens, whole, columns, rows_of = P("dp", None, None), P(None), P(None, "tp"), P("tp", None)
    return jax.shard_map(
        step,
        mesh=mesh,
        in_specs=(tokens, whole, columns, columns, columns, rows_of, whole, columns, columns, rows_of),
        out_specs=tokens,
        check_vma=False,
    )
```

```python
import functools

import jax
import jax.numpy as jnp
import numpy as np
from jax import lax
from jax.experimental import pallas as pl
from jax.experimental.pallas import tpu as pltpu
from jax.sharding import PartitionSpec as P

HEAD = 128
THETA = 10000
LOG2E = 1.4426950408889634
HIDDEN = -jnp.inf
MESH = pl.DeviceIdType.MESH
NB = 512
FB = 256
NEXT = 3
EARLY = 1
RING = 3
Q, KV, O, GU, REST, DOWN = range(6)
LANES = 128
PIECE = 32
AHEAD = 4
LAG = 3
OWN, FAR = LAG + 1, 2 * LAG
STG = 4
YB = 4
QB = 128
HEADS = 8
F32, BF16 = jnp.float32, jnp.bfloat16


def _dot(a, b, ca=1, cb=0):
    return lax.dot_general(a, b, (((ca,), (cb,)), ((), ())), preferred_element_type=F32)


def _if(cond):
    if isinstance(cond, bool):
        return (lambda act: act()) if cond else (lambda act: None)
    return pl.when(cond)


def _either(cond, yes, no):
    def run(act):
        def branch():
            act()
            return 0

        return branch

    lax.cond(cond, run(yes), run(no))


def _and(*conds):
    known = [c for c in conds if isinstance(c, bool)]
    rest = [c for c in conds if not isinstance(c, bool)]
    return functools.reduce(jnp.logical_and, rest) if all(known) and rest else all(known)


def _shares(seqs, half):
    big = half + PIECE
    return big, seqs * half - (seqs - 1) * big


def layer_kernel(
    x, wq, wk, wv, wo, wg, wu, wd, cos_in, sin_in, gain_a, gain_m,
    y, h_all, q_all, r_all,
    lhs, slots, qs, kvs, vx, hid, own, snd, rcv, stg, xin, qin, rin, hst, yin, yout, cos, sin, gain_in, gains,
    wsem, rs_send, rs_recv, st_sem, xs_sem, xr_sem, l_send, l_recv, l_free, x_free, in_sem, h_sem, yin_sem, yl_sem, ys_sem, yr_sem,
    first_sem, table_sem, xh_sem, xl_sem,
    *, seqs,
):
    tokens, depth = qs.shape[0], x.shape[1]
    half = tokens // 2
    big, small = _shares(seqs, half)
    qcols, kcols, ff = wq.shape[1], wk.shape[1], wd.shape[0]
    nj = depth // NB
    nq = qcols // NB
    per = depth // qcols
    nwo = nj // per
    na = nq + 1 + nwo
    ngu = ff // FB
    tail = ff - ngu * FB
    nm = ngu + (1 if tail else 0) + nj
    first_d = nm - nj
    all_a = seqs * na
    total = all_a + seqs * nm
    heads = qcols // HEAD
    group = heads // (kcols // HEAD)
    np_ = half // PIECE
    last = 2 * seqs - 1

    me = lax.axis_index("tp")
    core, chip = lax.rem(me, 2), lax.div(me, 2)
    partner = {"tp": chip * 2 + (1 - core)}
    across = {"tp": (1 - chip) * 2 + core}

    def start(g, kinds):
        slot = lax.rem(g, RING)

        def when(kind, cond):
            if kind not in kinds:
                return lambda act: None
            return (lambda act: act()) if len(kinds) == 1 else pl.when(cond)

        sem = wsem.at[slot]
        in_a = g < all_a
        a, m = lax.rem(g, na), lax.rem(g + (nm - all_a % nm), nm)

        @when(Q, in_a & (a < nq))
        def _():
            pltpu.make_async_copy(wq.at[:, pl.ds(pl.multiple_of(a * NB, NB), NB)], slots.at[slot], sem).start()

        @when(KV, in_a & (a == nq))
        def _():
            pltpu.make_async_copy(wk, slots.at[slot, :, pl.ds(0, kcols)], sem).start()
            pltpu.make_async_copy(wv, slots.at[slot, :, pl.ds(kcols, kcols)], sem).start()

        @when(O, in_a & (a > nq))
        def _():
            for k in range(per):
                at = pl.multiple_of(((a - nq - 1) * per + k) * NB, NB)
                pltpu.make_async_copy(wo.at[:, pl.ds(at, NB)], slots.at[slot, pl.ds(k * qcols, qcols), :], sem).start()

        in_m = jnp.logical_not(in_a) & (g < total)

        @when(GU, in_m & (m < ngu))
        def _():
            at = pl.multiple_of(m * FB, FB)
            pltpu.make_async_copy(wg.at[:, pl.ds(at, FB)], slots.at[slot, :, pl.ds(0, FB)], sem).start()
            pltpu.make_async_copy(wu.at[:, pl.ds(at, FB)], slots.at[slot, :, pl.ds(FB, FB)], sem).start()

        if tail:

            @when(REST, in_m & (m == ngu))
            def _():
                pltpu.make_async_copy(wg.at[:, pl.ds(ngu * FB, tail)], slots.at[slot, :, pl.ds(0, tail)], sem).start()
                pltpu.make_async_copy(wu.at[:, pl.ds(ngu * FB, tail)], slots.at[slot, :, pl.ds(tail, tail)], sem).start()

        @when(DOWN, in_m & (m >= first_d))
        def _():
            at = pl.multiple_of((m - first_d) * NB, NB)
            pltpu.make_async_copy(wd.at[:, pl.ds(at, NB)], slots.at[slot, pl.ds(0, ff), :], sem).start()

    def ready(g, kinds, rows=None, cols=NB):
        to = g + RING - 1
        a, m = lax.rem(to, na), lax.rem(to + (nm - all_a % nm), nm)

        def follow():
            if kinds == (GU, REST, DOWN):
                _either(m < ngu, lambda: start(to, (GU,)), lambda: start(to, (REST, DOWN)))
            elif kinds == (GU, DOWN):

                def gates():
                    @pl.when(to < total)
                    def _():
                        start(to, (GU,))

                _either(m >= first_d, lambda: start(to, (DOWN,)), gates)
            elif kinds == (Q, KV, O):
                _either(a < nq, lambda: start(to, (Q,)), lambda: start(to, (KV, O)))
            else:
                start(to, kinds)

        slot = lax.rem(g, RING)
        rows = depth if rows is None else rows
        where = slots.at[slot, pl.ds(0, rows), pl.ds(0, cols)]
        pltpu.make_async_copy(where, where, wsem.at[slot]).wait()
        follow()
        return slot

    class Sum:
        def __init__(self, ar, which, row0, n):
            self.ar, self.which, self.row0, self.n = ar, which, row0, n

        def far(self, j, at, n, sem):
            rows = pl.ds(pl.multiple_of(self.row0 + at, PIECE), n)
            return pltpu.make_async_remote_copy(q_all.at[self.which, j, rows, :], r_all.at[self.which, j, rows, :], xs_sem.at[self.ar], sem,
                                                device_id=across, device_id_type=MESH)

        def crossed(self, j):
            return self.far(j, 0, self.n, xr_sem.at[self.ar])

        def head(self, j):
            return self.far(j, 0, PIECE, xh_sem)

        def rest(self, j):
            return self.far(j, PIECE, self.n - PIECE, xr_sem.at[self.ar])

        def cross(self, j):
            if self.which:
                self.crossed(j).start()
            else:

                _either(self.ar == EARLY, lambda: self.head(j).start(), lambda: self.crossed(j).start())

        def each(self, act):
            def one(j, _):
                act(j)
                return 0

            lax.fori_loop(0, nj, one, 0)

        def all_blocks(self, sem, at=0, n=None):
            rows = pl.ds(pl.multiple_of(self.row0 + at, PIECE), n or self.n)
            whole = r_all.at[self.which, :, rows, :]
            pltpu.make_async_copy(whole, whole, sem).wait()

        def sent(self):
            self.all_blocks(xs_sem.at[self.ar])

        def have(self):
            self.all_blocks(xr_sem.at[self.ar])

        def have_head(self):
            self.all_blocks(xh_sem, 0, PIECE)

        def have_rest(self):
            self.all_blocks(xr_sem.at[self.ar], PIECE, self.n - PIECE)

        def kept(self, j):
            at = lax.rem(j, STG)
            rows = pl.ds(pl.multiple_of(self.row0, PIECE), self.n)
            return pltpu.make_async_copy(stg.at[at, pl.ds(0, self.n), :], q_all.at[self.which, j, rows, :], st_sem.at[at])

        def shared(self, j):
            i = self.ar * nj + j
            near, far = lax.rem(i, OWN), lax.rem(i, FAR)
            return pltpu.make_async_remote_copy(snd.at[near, pl.ds(0, self.n), :], rcv.at[far, pl.ds(0, self.n), :], rs_send.at[near],
                                                rs_recv.at[far], device_id=partner, device_id_type=MESH)

        def of_chip(self, j):
            i = self.ar * nj + j
            return (own[lax.rem(i, OWN), : self.n] + rcv[lax.rem(i, FAR), : self.n].astype(F32)).astype(BF16)

        def keep_term(self, j, t):
            i = self.ar * nj + j
            snd[lax.rem(i, OWN), : self.n] = t[: self.n].astype(BF16)
            own[lax.rem(i, OWN), : self.n] = t[self.n :]

    def sum_a(c):
        return Sum(c, 0, c * half, half)

    def sum_m(m):
        return Sum(seqs + m, 1, m * big, big)

    final = Sum(jnp.int32(last), 1, (seqs - 1) * big, small)

    def block(s, j, term, *sides):
        @pl.when(j >= LAG)
        def _():
            s.shared(j - LAG).wait()

        for side in sides:
            side.before(j)
        for side in sides:
            side.work(j)
        stg[lax.rem(j + 12 - LAG, STG), : s.n] = s.of_chip(j + 12 - LAG)
        s.keep_term(j, term())

        @pl.when(j >= LAG)
        def _():
            @pl.when(j > LAG)
            def _():
                s.kept(j - LAG - 1).wait()
                s.cross(j - LAG - 1)

            s.kept(j - LAG).start()

        s.shared(j).start()
        for side in sides:
            side.after(j)

    def drain(s):
        for j in range(nj - LAG, nj):
            s.shared(jnp.int32(j)).wait_recv()
            stg[j % STG, : s.n] = s.of_chip(jnp.int32(j))
            s.kept(jnp.int32(j)).start()

    def drained(s):
        for j in range(nj - LAG - 1, nj):
            s.kept(jnp.int32(j)).wait()
            s.cross(jnp.int32(j))
        for j in range(nj - LAG, nj):
            s.shared(jnp.int32(j)).wait_send()
        if not s.which:

            @pl.when(s.ar == EARLY)
            def _():
                s.each(lambda j: s.rest(j).start())

    def block_cols(j):
        return pl.ds(pl.multiple_of(j * NB, NB), NB)

    def crossed_last(j):
        return pltpu.make_async_remote_copy(lhs.at[pl.ds(0, small), block_cols(j)], lhs.at[pl.ds(small, small), block_cols(j)],
                                            xs_sem.at[last], xl_sem.at[j], device_id=across, device_id_type=MESH)

    def finish_last(j):
        final.shared(j).wait_recv()
        lhs[:small, block_cols(j)] = final.of_chip(j)
        crossed_last(j).start()

    def block_last(j, term, side):
        @pl.when(j >= OWN)
        def _():
            final.shared(j - OWN).wait_send()

        final.keep_term(j, term())
        final.shared(j).start()
        side.beside(j)

        @pl.when(j == 0)
        def _():
            pl.semaphore_wait(x_free, 1)

        finish_last(j)

    def exchanged(n):
        pltpu.make_async_remote_copy(lhs.at[pl.ds(n, n), :], lhs.at[pl.ds(0, n), :], l_send, l_recv,
                                     device_id=partner, device_id_type=MESH).wait()

    def free():
        pl.semaphore_signal(l_free, inc=1, device_id=partner, device_id_type=MESH)

    def scaled(rows, which, part):
        squares = jnp.zeros((PIECE, NB), F32)
        for j in range(nj):
            v = part(j, True)
            squares += v * v
        scale = lax.rsqrt(jnp.sum(squares, axis=1, keepdims=True) * (1 / depth) + 1e-6)
        for j in range(nj):
            cols = slice(j * NB, (j + 1) * NB)
            lhs[rows, cols] = (part(j, False) * scale * gains[pl.ds(which, 1), cols]).astype(BF16)

    class Operand:
        def __init__(self, piece0, pieces, base, second):
            self.piece0, self.pieces, self.base, self.second = piece0, pieces, base, second

        def here(self, p):
            return pl.ds(pl.multiple_of((self.piece0 + p) * PIECE, PIECE), PIECE)

        def loads(self, p):
            at, i = lax.rem(p, AHEAD), self.piece0 + p
            row = lax.div(i, np_) * tokens + core * half + lax.rem(i, np_) * PIECE
            return (pltpu.make_async_copy(x.at[pl.ds(pl.multiple_of(row, PIECE), PIECE), :], xin.at[at], in_sem.at[at, 0]),
                    pltpu.make_async_copy(q_all.at[0, :, self.here(p), :], qin.at[at], in_sem.at[at, 1]),
                    pltpu.make_async_copy(r_all.at[0, :, self.here(p), :], rin.at[at], in_sem.at[at, 2]))[: 3 if self.second else 1]

        def put(self, p):
            at = lax.rem(p, 2)
            return pltpu.make_async_copy(hst.at[at], h_all.at[:, self.here(p), :], h_sem.at[at])

        def give(self, p):
            here = pl.ds(pl.multiple_of(self.base + p * PIECE, PIECE), PIECE)
            there = pl.ds(pl.multiple_of(p * PIECE, PIECE), PIECE)
            return pltpu.make_async_remote_copy(lhs.at[here, :], lhs.at[there, :], l_send, l_recv, device_id=partner, device_id_type=MESH)

        def begin(self):
            for p in range(AHEAD - 1):
                for copy in self.loads(jnp.int32(p)):
                    copy.start()

        def before(self, p):
            @pl.when(p + AHEAD - 1 < self.pieces)
            def _():
                for copy in self.loads(p + AHEAD - 1):
                    copy.start()

            for copy in self.loads(p):
                copy.wait()

            @pl.when(p == 1)
            def _():
                pl.semaphore_wait(l_free, 1)
                self.give(jnp.int32(0)).start()

            @pl.when(p >= 2)
            def _():
                if self.second:
                    self.put(p - 2).wait()
                self.give(p - 1).start()

        def work(self, p):
            at, to = lax.rem(p, AHEAD), lax.rem(p, 2)
            rows = pl.ds(pl.multiple_of(self.base + p * PIECE, PIECE), PIECE)

            def plain(j, new):
                return xin[at, :, j * NB : (j + 1) * NB].astype(F32)

            def part(j, new):
                if new:
                    v = xin[at, :, j * NB : (j + 1) * NB].astype(F32) + (qin[at, j].astype(F32) + rin[at, j].astype(F32))
                    hst[to, j] = v.astype(BF16)
                return hst[to, j].astype(F32)

            scaled(rows, int(self.second), part if self.second else plain)

        def after(self, p):
            if self.second:
                self.put(p).start()

        def last(self):
            self.give(jnp.int32(self.pieces - 1)).start()

        def end(self):
            if self.second:
                for p in (2, 1):
                    self.put(jnp.int32(self.pieces - p)).wait()

    def with_operand(side, step):
        lax.fori_loop(0, side.pieces, lambda j, _: step(j, side), 0)
        side.last()
        lax.fori_loop(side.pieces, nj, lambda j, _: step(j), 0)
        side.end()

    early = pl.multiple_of((1 - core) * half, half)
    late = pl.multiple_of(core * half, half)

    def turned(t):
        t = t.astype(F32)
        r = pltpu.roll(t, HEAD // 2, 1)
        out = []
        for rows, place in ((slice(0, half), (1 - core) * half), (slice(half, tokens), core * half)):
            place = pl.ds(pl.multiple_of(place, half), half)
            out.append((t[rows] * cos[place, :] + r[rows] * sin[place, :]).astype(BF16))
        return jnp.concatenate(out, 0)

    def turn(s):
        for n in range(NB // HEAD):
            cols = pl.ds(pl.multiple_of(s * NB + n * HEAD, HEAD), HEAD)
            qs[:, cols] = turned(qs[:, cols])

    def attention():
        e = HEAD**-0.5 * LOG2E
        for n in range(kcols // HEAD):
            vx[n, :, :HEAD] = kvs[:, kcols + n * HEAD : kcols + (n + 1) * HEAD]
        seen = lax.broadcasted_iota(jnp.int32, (QB, QB), 1) <= lax.broadcasted_iota(jnp.int32, (QB, QB), 0)
        many = min(HEADS, group)

        def rows(b):
            at = b * QB
            return pl.ds(pl.multiple_of(early + at if at < half else late + at - half, QB), QB)

        def some(i, _):
            n = lax.div(i * many, group)
            kc = pl.ds(pl.multiple_of(n * HEAD, HEAD), HEAD)
            cols = [pl.ds(pl.multiple_of((i * many + t) * HEAD, HEAD), HEAD) for t in range(many)]
            keys = [kvs[rows(b), kc] for b in range(tokens // QB)]
            values = [vx[n, rows(b), :] for b in range(tokens // QB)]
            for b in range(tokens // QB):
                q = jnp.concatenate([qs[rows(b), c] for c in cols], 0)
                scores = _dot(q, jnp.concatenate(keys[: b + 1], 0), 1, 1)
                weights = []
                for t in range(many):
                    of = scores[t * QB : (t + 1) * QB]
                    parts = [of[:, u * QB : (u + 1) * QB] for u in range(b)] + [jnp.where(seen, of[:, b * QB :], HIDDEN)]
                    top = functools.reduce(jnp.maximum, parts).max(axis=1, keepdims=True)
                    weights.append(jnp.concatenate([jnp.exp2((u - top) * e).astype(BF16) for u in parts], 1))
                o = _dot(jnp.concatenate(weights, 0), jnp.concatenate(values[: b + 1], 0))
                for t, c in enumerate(cols):
                    of = o[t * QB : (t + 1) * QB]
                    hid[rows(b), c] = (of[:, :HEAD] / of[:, HEAD:]).astype(BF16)
            return 0

        lax.fori_loop(0, heads // many, some, 0)

    def first(c, _):
        g0 = c * na

        def queries(s, _):
            slot = ready(g0 + s, (Q, KV, O))
            turn(jnp.maximum(s - 1, 0))
            qs[:, pl.ds(pl.multiple_of(s * NB, NB), NB)] = _dot(lhs[:tokens], slots[slot]).astype(BF16)

            @pl.when((c >= 1) & (s == min(1, nq - 1)))
            def _():
                drain(sum_a(c - 1))

            return 0

        lax.fori_loop(0, nq, queries, 0)

        slot = ready(g0 + nq, (O,) if nwo > 1 else (O, Q, GU))
        turn(nq - 1)
        t = _dot(lhs[:tokens], slots[slot, :, : 2 * kcols])
        for n in range(kcols // HEAD):
            cols = slice(n * HEAD, (n + 1) * HEAD)
            kvs[:, cols] = turned(t[:, cols].astype(BF16))
        kvs[:, kcols:] = t[:, kcols:].astype(BF16)
        free()

        @pl.when(c >= 1)
        def _():
            drained(sum_a(c - 1))

        rows = Operand((c + 1) * np_, np_, half, False)
        shares = Operand(jnp.int32(0), big // PIECE, big, True)

        @pl.when(c + 1 < seqs)
        def _():
            rows.begin()

        @pl.when(c + 1 == seqs)
        def _():
            s = sum_a(jnp.int32(0))
            s.have()
            s.sent()
            sum_a(jnp.int32(EARLY)).have_head()
            shares.begin()

        attention()

        def project(j, *sides):
            k = lax.rem(j, per)
            g = g0 + nq + 1 + lax.div(j, per)

            @pl.when(k == 0)
            def _():
                ready(g, (O, Q, KV, GU, DOWN))

            w = slots.at[lax.rem(g, RING), pl.ds(pl.multiple_of(k * qcols, qcols), qcols), :]
            block(sum_a(c), j, lambda: _dot(hid[:tokens, :qcols], w[...]), *sides)
            return 0

        @pl.when(c + 1 < seqs)
        def _():
            with_operand(rows, project)
            exchanged(half)

        @pl.when(c + 1 == seqs)
        def _():
            with_operand(shares, project)
            exchanged(big)

        return 0

    def puts(c, j, t):
        at = lax.rem(t, YB)
        where = y.at[pl.ds(pl.multiple_of(c * tokens + core * half, half), half), block_cols(j)]
        return (pltpu.make_async_copy(yout.at[at], where, yl_sem.at[at]),
                pltpu.make_async_remote_copy(yout.at[at], where, ys_sem.at[at], yr_sem.at[c], device_id=partner, device_id_type=MESH))

    class Results:
        def __init__(self):
            self.count = seqs - 1

        def of(self, t):
            return lax.div(t, nj), lax.rem(t, nj)

        def loads(self, t):
            c, j = self.of(t)
            at = lax.rem(t, YB)
            rows = pl.ds(pl.multiple_of(c * half, half), half)
            return [pltpu.make_async_copy(src, yin.at[at, i], yin_sem.at[at, i])
                    for i, src in enumerate((h_all.at[j, rows, :], q_all.at[1, j, rows, :], r_all.at[1, j, rows, :]))]

        def fetch(self, t):
            c, j = self.of(t)

            @pl.when(j == 0)
            def _():
                sum_m(c).have()

            for copy in self.loads(t):
                copy.start()

        def begin(self):
            for t in range(YB - 1):
                self.fetch(jnp.int32(t))

        def left(self, t):
            near, far = puts(*self.of(t), t)
            near.wait()
            far.wait_send()

        def item(self, t):
            at = lax.rem(t, YB)

            @pl.when(t + YB - 1 < self.count * nj)
            def _():
                self.fetch(t + YB - 1)

            for copy in self.loads(t):
                copy.wait()

            @pl.when(t >= YB)
            def _():
                self.left(t - YB)

            yout[at] = (yin[at, 0].astype(F32) + (yin[at, 1].astype(F32) + yin[at, 2].astype(F32))).astype(BF16)
            for copy in puts(*self.of(t), t):
                copy.start()

        def beside(self, j):
            for k in range(self.count):
                self.item(j * self.count + k)

        def end(self):
            for t in range(self.count * nj - YB, self.count * nj):
                self.left(jnp.int32(t))
            for c in range(self.count):
                sum_m(jnp.int32(c)).sent()

    def gated(gate, up):
        return (gate * jax.nn.sigmoid(gate) * up).astype(BF16)

    def second(m, n, ahead):
        g0 = all_a + m * nm

        def before(act):
            if n == small:
                act(sum_m(m - 1))
            else:

                @pl.when(m == 0)
                def _():
                    act(sum_a(jnp.int32(seqs - 1)))

                @pl.when(m > 0)
                def _():
                    act(sum_m(m - 1))

        def gates(s, _):
            slot = ready(g0 + s, (GU, REST, DOWN))
            t = _dot(lhs[: 2 * n], slots[slot])
            hid[: 2 * n, pl.ds(pl.multiple_of(s * FB, FB), FB)] = gated(t[:, :FB], t[:, FB:])

            @pl.when((s == 1) | (s == 3))
            def _():
                @pl.when(s == 1)
                def _():
                    before(drain)

                @pl.when(s == 3)
                def _():
                    before(drained)

            return 0

        lax.fori_loop(0, ngu, gates, 0)
        ahead()
        if tail:
            slot = ready(g0 + ngu, (DOWN,), None, 2 * tail)
            t = _dot(lhs[: 2 * n], slots[slot, :, : 2 * tail])
            hid[: 2 * n, ngu * FB :] = gated(t[:, :tail], t[:, tail:])

        def down(j):
            slot = ready(g0 + first_d + j, (GU, DOWN), ff)
            return lambda: _dot(hid[: 2 * n], slots[slot, :ff, :])

        return down

    def share(m, _):
        ends = m == seqs - 2
        next_n = jnp.where(ends, small, big)
        side = Operand((m + 1) * (big // PIECE), lax.div(next_n, PIECE), next_n, True)

        def ahead():
            @pl.when(m == 0)
            def _():
                s = sum_a(jnp.int32(EARLY))
                s.have_rest()
                s.sent()

            side.begin()

        down = second(m, big, ahead)
        free()

        def step(j, *sides):
            if sides:

                @pl.when((j == NEXT) & (m + 2 < seqs))
                def _():
                    s = sum_a(m + 2)
                    s.have()
                    s.sent()

            block(sum_m(m), j, down(j), *sides)
            return 0

        with_operand(side, step)

        @pl.when(ends)
        def _():
            exchanged(small)

        @pl.when(jnp.logical_not(ends))
        def _():
            exchanged(big)

        return 0

    def last_share():
        done = Results()
        down = second(seqs - 1, small, done.begin)
        pl.semaphore_signal(x_free, inc=1, device_id=across, device_id_type=MESH)

        def step(j, _):
            block_last(j, down(j), done)
            return 0

        lax.fori_loop(0, nj, step, 0)
        for j in range(nj - OWN, nj):
            final.shared(jnp.int32(j)).wait_send()
        done.end()

    def fetched(p):
        owner = jnp.where(p < np_, 1 - core, core)
        rows = pl.ds(pl.multiple_of(owner * half + lax.rem(p, np_) * PIECE, PIECE), PIECE)
        return pltpu.make_async_copy(x.at[rows, :], lhs.at[pl.ds(pl.multiple_of(p * PIECE, PIECE), PIECE), :], first_sem.at[p])

    tables = [pltpu.make_async_copy(src, dst, table_sem.at[i]) for i, (src, dst) in
              enumerate(((gain_a, gain_in.at[0]), (gain_m, gain_in.at[1]), (cos_in, cos), (sin_in, sin)))]
    for p in range(2 * np_):
        fetched(jnp.int32(p)).start()
    for copy in tables:
        copy.start()
    barrier = pltpu.get_barrier_semaphore()
    for peer in (partner, across):
        pl.semaphore_signal(barrier, inc=1, device_id=peer, device_id_type=MESH)
    for n in range(kcols // HEAD):
        vx[n, :, HEAD:] = jnp.ones((tokens, HEAD), BF16)
    for i in range(2):
        tables[i].wait()
        wide = gain_in[i].astype(F32)
        for r in range(depth // LANES):
            gains[i : i + 1, r * LANES : (r + 1) * LANES] = wide[r : r + 1]

    def normed(p, _):
        rows = pl.ds(pl.multiple_of(p * PIECE, PIECE), PIECE)
        fetched(p).wait()
        scaled(rows, 0, lambda j, new: lhs[rows, j * NB : (j + 1) * NB].astype(F32))

        for g in range(RING - 1):

            @pl.when(p == 3 + 4 * g)
            def _():
                start(jnp.int32(g), (Q, KV))

        return 0

    lax.fori_loop(0, 2 * np_, normed, 0)
    pl.semaphore_wait(barrier, 2)
    for copy in tables[2:]:
        copy.wait()
    lax.fori_loop(0, seqs, first, 0)
    lax.fori_loop(0, seqs - 1, share, 0)
    last_share()

    def left(j):
        near, far = puts(seqs - 1, j, j)
        near.wait()
        far.wait_send()

    over = (seqs - 1) * (big - half)

    def blocks(j):
        at, row0 = lax.rem(j, YB), (seqs - 1) * half
        return [pltpu.make_async_copy(src.at[j, pl.ds(row0, n), :], yin.at[at, i, pl.ds(0, n), :], yin_sem.at[at, i])
                for i, (src, n) in enumerate(((h_all, half), (q_all.at[1], over), (r_all.at[1], over)))]

    for j in range(YB - 1):
        for copy in blocks(jnp.int32(j)):
            copy.start()

    def piece(j, _):
        at = lax.rem(j, YB)

        @pl.when(j + YB - 1 < nj)
        def _():
            for copy in blocks(j + YB - 1):
                copy.start()

        @pl.when(j >= YB)
        def _():
            left(j - YB)

        for copy in blocks(j):
            copy.wait()
        crossed_last(j).wait_recv()
        here, there = lhs[:small, block_cols(j)].astype(F32), lhs[small : 2 * small, block_cols(j)].astype(F32)
        yout[at, :over] = (yin[at, 0, :over].astype(F32) + (yin[at, 1, :over].astype(F32) + yin[at, 2, :over].astype(F32))).astype(BF16)
        yout[at, over:] = (yin[at, 0, over:].astype(F32) + (here + there)).astype(BF16)
        for copy in puts(seqs - 1, j, j):
            copy.start()
        return 0

    lax.fori_loop(0, nj, piece, 0)
    for j in range(nj - YB, nj):
        left(jnp.int32(j))
    final.sent()

    def arrived(c, _):
        where = y.at[pl.ds(pl.multiple_of(c * tokens + (1 - core) * half, half), half), :]
        pltpu.make_async_copy(where, where, yr_sem.at[c]).wait()
        return 0

    lax.fori_loop(0, seqs, arrived, 0)


def layer(x, gain_a, wq, wk, wv, wo, gain_m, w_gate, w_up, w_down):
    seqs, tokens, depth = x.shape
    half, nj = tokens // 2, depth // NB
    big, _ = _shares(seqs, half)
    i = np.arange(HEAD // 2, dtype=np.float32)
    angle = np.arange(tokens, dtype=np.float32)[:, None] * np.float32(THETA) ** (-i / np.float32(HEAD // 2))
    cos, sin = np.cos(angle), np.sin(angle)
    cos, sin = np.concatenate([cos, cos], 1).astype(np.float32), np.concatenate([-sin, sin], 1).astype(np.float32)
    hbm = pl.BlockSpec(memory_space=pl.ANY)
    dma, regular = pltpu.SemaphoreType.DMA, pltpu.SemaphoreType.REGULAR
    out = [
        jax.ShapeDtypeStruct((seqs * tokens, depth), BF16),
        jax.ShapeDtypeStruct((nj, seqs * half, NB), BF16),
        jax.ShapeDtypeStruct((2, nj, seqs * half, NB), BF16),
        jax.ShapeDtypeStruct((2, nj, seqs * half, NB), BF16),
    ]
    kv = wk.shape[1]
    scratch = [
        pltpu.VMEM((2 * big, depth), BF16),
        pltpu.VMEM((RING, depth, NB), BF16),
        pltpu.VMEM((tokens, wq.shape[1]), BF16),
        pltpu.VMEM((tokens, 2 * kv), BF16),
        pltpu.VMEM((kv // HEAD, tokens, 2 * HEAD), BF16),
        pltpu.VMEM((2 * big, w_down.shape[0]), BF16),
        pltpu.VMEM((OWN, big, NB), F32),
        pltpu.VMEM((OWN, big, NB), BF16),
        pltpu.VMEM((FAR, big, NB), BF16),
        pltpu.VMEM((STG, big, NB), BF16),
        pltpu.VMEM((AHEAD, PIECE, depth), BF16),
        pltpu.VMEM((AHEAD, nj, PIECE, NB), BF16),
        pltpu.VMEM((AHEAD, nj, PIECE, NB), BF16),
        pltpu.VMEM((2, nj, PIECE, NB), BF16),
        pltpu.VMEM((YB, 3, half, NB), BF16),
        pltpu.VMEM((YB, half, NB), BF16),
        pltpu.VMEM((tokens, HEAD), F32),
        pltpu.VMEM((tokens, HEAD), F32),
        pltpu.VMEM((2, depth // LANES, LANES), BF16),
        pltpu.VMEM((2, depth), F32),
        dma((RING,)), dma((OWN,)), dma((FAR,)), dma((STG,)), dma((2 * seqs,)), dma((2 * seqs - 1,)),
        dma, dma, regular, regular,
        dma((AHEAD, 3)), dma((2,)), dma((YB, 3)), dma((YB,)), dma((YB,)), dma((seqs,)),
        dma((tokens // PIECE,)), dma((4,)), dma, dma((nj,)),
    ]
    y, *_ = pl.pallas_call(
        functools.partial(layer_kernel, seqs=seqs),
        out_shape=out,
        in_specs=[hbm] * 12,
        out_specs=[hbm] * 4,
        scratch_shapes=scratch,
        compiler_params=pltpu.CompilerParams(collective_id=0, has_side_effects=True, vmem_limit_bytes=67043328),
        name="layer",
    )(x.reshape(seqs * tokens, depth), wq, wk, wv, wo, w_gate, w_up, w_down, cos, sin,
      gain_a.reshape(-1, LANES), gain_m.reshape(-1, LANES))
    return y.reshape(x.shape)


def solution(mesh):
    def step(*args):
        return layer(*args)

    tokens, whole, columns, rows_of = P("dp", None, None), P(None), P(None, "tp"), P("tp", None)
    return jax.shard_map(
        step,
        mesh=mesh,
        in_specs=(tokens, whole, columns, columns, columns, rows_of, whole, columns, columns, rows_of),
        out_specs=tokens,
        check_vma=False,
    )
```
